32 devices in a mesh: section: 4 (over x, core), obs: 8 (over z, y).
Axes of the slice: x: 2, y: 2, z: 4, core: 2. Of those that a mesh axis runs over, the one named last changes fastest.
Arguments:
- predictors: bfloat16 [4, 4, 20, 32768], P('section', None, None, 'obs'), may hold values from -5 to 5
- departures: float32 [4, 4, 32768], P('section', None, 'obs'), may hold values from -30 to 30
- obs_precision: float32 [4, 4, 32768], P('section', None, 'obs'), may hold values from 0.3 to 3
- qc_pass: int32 [4, 4, 32768], P('section', None, 'obs'), may hold values 0 or 1
- block_channel: int32 [4, 4, 256], P('section', None, 'obs'), may hold values from 0 to 2047, as said below
- stream_order: int32 [4], replicated, may hold values from 0 to 3, each once
- prior_coeffs: float32 [4, 20, 2048], P(None, None, 'obs'), may hold values from -1 to 1
- prior_info: float32 [4, 210, 2048], P(None, None, 'obs'), may hold values from -1 to 32, as said below
- memory_factor: float32 [2048], P('obs'), may hold values from 0.5 to 0.98
Outputs:
- coeffs: float32 [4, 4, 20, 2048], P('section', None, None, 'obs')
- information: float32 [4, 4, 210, 2048], P('section', None, None, 'obs')
The draws below stay inside these ranges and needn't reach their ends.
Inputs may be any that keep to these rules, and one draw needn't show every extreme that they name: `block_channel`: among the 32 row blocks of one index of obs, at most 8 have channels in any one range of the 256 channels from a multiple of 256; in every window and stream one such range holds exactly 8 blocks of every index of obs. `stream_order`: each stream appears once. `prior_info`: for every stream and channel the 210 entries are the upper triangle, row by row, of a symmetric positive definite matrix of order 20.
All inputs are finite; a program needn't handle non-finite values. No bound on the sum of `qc_pass` on one device may be relied on, other than what follows from the above.
Results may differ from the reference program's by a relative error of at most 0.0038.
Values sent between devices are 32-bit elements; how exact they have to be, the bound alone decides.
A program may use at most 64 MiB of HBM per device.

```python
import math
import jax
import jax.numpy as jnp
import numpy as np
from jax import lax

NPRED = 20
CH = 2048
BLOCK_ROWS = 128
STREAMS = 4
WINDOWS = 4
ROWS = 32768
NB_DEV = 32
NBLK = 256
CH_DEV = 256
CAP = 8


def observation_fields(base_key):
    pred_key, truth_key, noise_key = jax.random.split(jax.random.fold_in(base_key, 11), 3)
    values = jax.random.truncated_normal(pred_key, -5.0, 5.0, (WINDOWS, STREAMS, NPRED, ROWS), jnp.float32)
    true_coeffs = 0.25 * jax.random.truncated_normal(truth_key, -4.0, 4.0, (WINDOWS, STREAMS, NPRED, NBLK), jnp.float32)
    signal = jnp.einsum('wspbr,wspb->wsbr', values.reshape(WINDOWS, STREAMS, NPRED, NBLK, BLOCK_ROWS), true_coeffs).reshape(WINDOWS, STREAMS, ROWS)
    position = jnp.arange(ROWS, dtype=jnp.float32) / ROWS
    spread = 1.0 + 2.0 * position
    noise_draw = jax.random.truncated_normal(noise_key, -5.0, 5.0, (WINDOWS, STREAMS, ROWS), jnp.float32)
    return (values, jnp.clip(signal + spread * noise_draw, -30.0, 30.0))


def draw_predictors(key, part):
    return observation_fields(key)[0].astype(jnp.bfloat16)


def draw_departures(key, part):
    return observation_fields(key)[1]


def draw_block_channel(key, part):
    owner_count = NBLK // NB_DEV

    def one_group(group_key):
        pick_key, device_key = jax.random.split(group_key)
        special = jax.random.randint(pick_key, (), 0, owner_count)

        def one_device(own_key):
            list_key, shuffle_key, inner_key = jax.random.split(own_key, 3)
            others = jax.random.permutation(list_key, (owner_count - 1) * CAP)[:NB_DEV - CAP]
            other_owner = (others // CAP + special + 1) % owner_count
            owners = jnp.concatenate([jnp.full((CAP,), special, jnp.int32), other_owner.astype(jnp.int32)])
            owners = jax.random.permutation(shuffle_key, owners)
            inner_channel = jax.random.randint(inner_key, (NB_DEV,), 0, CH_DEV)
            return (owners * CH_DEV + inner_channel).astype(jnp.int32)
        return jax.vmap(one_device)(jax.random.split(device_key, owner_count)).reshape(NBLK)
    groups = jax.vmap(one_group)(jax.random.split(jax.random.fold_in(key, 31), WINDOWS * STREAMS))
    return groups.reshape(WINDOWS, STREAMS, NBLK)


def draw_prior_info(key, part):
    raw_key, margin_key = jax.random.split(jax.random.fold_in(key, 23))
    raw = jax.random.uniform(raw_key, (STREAMS, CH, NPRED, NPRED), jnp.float32, -1.0, 1.0)
    identity = jnp.eye(NPRED, dtype=jnp.float32)
    coupling = 0.5 * (raw + jnp.swapaxes(raw, 2, 3)) * (1.0 - identity)
    margin = jnp.exp(jax.random.uniform(margin_key, (STREAMS, CH, NPRED), jnp.float32, math.log(2.0), math.log(12.0)))
    leading = jnp.sum(jnp.abs(coupling), axis=3) + margin
    matrix = coupling + leading[..., None] * identity
    upper_index = np.array([i * NPRED + j for i in range(NPRED) for j in range(i, NPRED)], dtype=np.int32)
    packed = matrix.reshape(STREAMS, CH, NPRED * NPRED)[:, :, upper_index]
    return jnp.swapaxes(packed, 1, 2)


def place_ends(drawn, key, smallest, top_value):
    longest = drawn.shape.index(max(drawn.shape))
    spots = []
    for shift in (0, 1):
        where = [jax.random.randint(jax.random.fold_in(key, axis), (), 0, length) for axis, length in enumerate(drawn.shape)]
        where[longest] = (where[longest] + shift) % drawn.shape[longest]
        spots.append(tuple(where))
    return drawn.at[spots[0]].set(smallest).at[spots[1]].set(top_value)


def levels(stream_key, dims, pieces, least, top_value):
    factor_of = 1.0
    for axis_at, parts in pieces:
        heights = jax.random.uniform(jax.random.fold_in(jax.random.fold_in(stream_key, 6), axis_at), (parts,), jnp.float32, least / len(pieces), top_value / len(pieces))
        factor_of = factor_of * jnp.repeat(jnp.exp(heights), dims[axis_at] // parts).reshape((-1,) + (1,) * (len(dims) - 1 - axis_at))
    return factor_of


def scatter_about(key, extent, scale, reach, cuts=(), held_as=jnp.bfloat16):
    drawn = scale * jax.random.normal(key, extent, jnp.float32)
    if cuts:
        drawn = drawn * levels(key, extent, cuts, -0.22, 0.18)
    return jnp.clip(drawn, -reach, reach).astype(held_as)


def setup_inputs(seed: int = 0) -> dict:
    splits = jax.random.split(jax.random.key(seed), 10)
    predictors = draw_predictors(jax.random.fold_in(splits[9], 71), 0)
    departures = draw_departures(jax.random.fold_in(splits[9], 71), 0)
    obs_precision = jnp.clip(jnp.exp(math.log(3.0) - 2.3025851 * jax.random.uniform(splits[2], (WINDOWS, STREAMS, ROWS), jnp.float32) ** levels(splits[2], (WINDOWS, STREAMS, ROWS), ((0, 4), (2, 8)), -0.2, 0.2)), 0.3, 3.0)
    qc_pass = place_ends((jax.random.randint(splits[3], (WINDOWS, STREAMS, ROWS), 0, 4) < 3).astype(jnp.int32), jax.random.fold_in(splits[3], 1), 0, 1)
    block_channel = draw_block_channel(jax.random.fold_in(splits[9], 71), 0)
    stream_order = jax.random.permutation(splits[5], STREAMS).astype(jnp.int32)
    prior_coeffs = scatter_about(splits[6], (STREAMS, NPRED, CH), 0.25, 1.0, ((2, 8),), jnp.float32)
    prior_info = draw_prior_info(jax.random.fold_in(splits[9], 71), 0)
    memory_factor = jnp.clip(jnp.exp(math.log(0.98) - 0.6729445 * jax.random.uniform(splits[8], (CH,), jnp.float32) ** levels(splits[8], (CH,), ((0, 8),), -0.2, 0.2)), 0.5, 0.98)
    return {"predictors": predictors, "departures": departures, "obs_precision": obs_precision, "qc_pass": qc_pass, "block_channel": block_channel, "stream_order": stream_order, "prior_coeffs": prior_coeffs, "prior_info": prior_info, "memory_factor": memory_factor}


HUBER_SQ = 9.0
PRIOR_WEIGHT = 64.0

def upper_positions(dimension):
    return np.array([i * dimension + j for i in range(dimension) for j in range(i, dimension)], dtype=np.int32)

def solve_packed(packed, target):
    dimension = target.shape[0]
    placing = {}
    counter = 0
    for i in range(dimension):
        for j in range(i, dimension):
            placing[i, j] = counter
            counter += 1
    factor = [[None] * dimension for i in range(dimension)]
    for j in range(dimension):
        pivot_root = jnp.sqrt(packed[placing[j, j]] - sum((factor[j][k] * factor[j][k] for k in range(j))))
        factor[j][j] = pivot_root
        for i in range(j + 1, dimension):
            factor[i][j] = (packed[placing[j, i]] - sum((factor[i][k] * factor[j][k] for k in range(j)))) / pivot_root
    forward = []
    for i in range(dimension):
        forward.append((target[i] - sum((factor[i][k] * forward[k] for k in range(i)))) / factor[i][i])
    backward = [None] * dimension
    for i in reversed(range(dimension)):
        backward[i] = (forward[i] - sum((factor[k][i] * backward[k] for k in range(i + 1, dimension)))) / factor[i][i]
    return jnp.stack(backward)

def stream_update(beta_prior, info_prior, predicted, departed, precision, passed, channel):
    pred_count = predicted.shape[0]
    block_count = channel.shape[0]
    block_width = departed.shape[0] // block_count
    shaped = predicted.astype(jnp.float32).reshape(pred_count, block_count, block_width)
    block_coeffs = jnp.take(beta_prior, channel, axis=1)
    offset = lax.optimization_barrier(jnp.sum(shaped * block_coeffs[:, :, None], axis=0))
    residual = departed.reshape(block_count, block_width) - offset
    scale_row = precision.reshape(block_count, block_width)
    weight = passed.reshape(block_count, block_width).astype(jnp.float32) * scale_row / (1.0 + scale_row * residual * residual / HUBER_SQ)
    weighted = lax.optimization_barrier((weight[None] * shaped).astype(jnp.bfloat16)).astype(jnp.float32)
    chi_square = jnp.sum(weight * residual * residual)
    passed_count = jnp.sum(passed.astype(jnp.float32))
    inflation = (chi_square + PRIOR_WEIGHT) / (passed_count + PRIOR_WEIGHT)
    gram_upper = jnp.einsum('ibr,jbr->bij', weighted, shaped).reshape(block_count, pred_count * pred_count)[:, upper_positions(pred_count)]
    gradient = jnp.einsum('ibr,br->bi', weighted, residual)
    block_sums = jnp.concatenate([gram_upper, gradient], axis=1)
    normal = jax.ops.segment_sum(block_sums, channel, num_segments=CH).T
    tri_count = gram_upper.shape[1]
    info_post = info_prior + normal[:tri_count] / inflation
    beta_post = beta_prior + solve_packed(info_post, normal[tri_count:] / inflation)
    return (beta_post, info_post)

def reference(predictors, departures, obs_precision, qc_pass, block_channel, stream_order, prior_coeffs, prior_info, memory_factor):

    def window_step(state_pair, window):
        beta_prior, info_prior = state_pair

        def select_window(source):
            return jnp.take(lax.dynamic_index_in_dim(source, window, 0, keepdims=False), stream_order, axis=0)
        beta_post, info_post = jax.vmap(stream_update)(beta_prior, info_prior, select_window(predictors), select_window(departures), select_window(obs_precision), select_window(qc_pass), select_window(block_channel))
        return ((beta_post, memory_factor[None, None, :] * info_post), (beta_post, info_post))
    initial = (jnp.take(prior_coeffs, stream_order, axis=0), jnp.take(prior_info, stream_order, axis=0))
    final_state, outputs = lax.scan(window_step, initial, jnp.arange(WINDOWS, dtype=jnp.int32))
    return (outputs[0], outputs[1])
```

```python
import functools

import jax
import jax.numpy as jnp
import numpy as np
from jax import lax
from jax.experimental import pallas as pl
from jax.experimental.pallas import tpu as pltpu
from jax.sharding import PartitionSpec as P

HUBER_SQ = 9.0
PRIOR_WEIGHT = 64.0
F32 = jnp.float32
BF16 = jnp.bfloat16
NN = (((1,), (0,)), ((), ()))
NT = (((1,), (1,)), ((), ()))
TN = (((0,), (0,)), ((), ()))


def round_up(n, m):
    return -(-n // m) * m


def split3(x):
    hi = x.astype(BF16)
    rest = x - hi.astype(F32)
    mid = rest.astype(BF16)
    low = (rest - mid.astype(F32)).astype(BF16)
    return hi, mid, low


def dot(a, b, dims):
    return lax.dot_general(a, b, dims, preferred_element_type=F32)


def each(low, high, body):
    n = high - low

    def step(i, _):
        body(i)
        return 0

    lax.fori_loop(low, high, step, 0, unroll=n if n <= 8 else 1)


def iota(shape, axis):
    return lax.broadcasted_iota(jnp.int32, shape, axis)


def kernel(
    cfg,
    order_hbm,
    x_hbm,
    dep_hbm,
    prec_hbm,
    qc_hbm,
    bc_hbm,
    pc_hbm,
    pi_hbm,
    mf_hbm,
    ee_hbm,
    co_out,
    io_out,
    order_s,
    x_v,
    dep_v,
    prec_v,
    qc_v,
    bc_v,
    pc_v,
    pi_v,
    mf_v,
    ee_v,
    lists,
    bcr,
    pcs,
    pcr,
    cs,
    cr,
    ts,
    tr,
    xs,
    xh,
    pt,
    chcol,
    place,
    place_t,
    coef_v,
    hots,
    state,
    betas,
    beta_in,
    work,
    cob,
    iob,
    load_sem,
    bc_send,
    bc_recv,
    p_send,
    p_recv,
    c_send,
    c_recv,
    t_send,
    t_recv,
    f_send,
    f_recv,
    b_send,
    b_recv,
    o_send,
    o_recv,
):
    S, O, K, N, NP, T, C, NB, SL, TL = cfg
    G = S // 2
    Q = O * SL
    sec = lax.axis_index("section")
    ob = lax.axis_index("obs")
    odd = lax.rem(sec, 2) == 1
    g = sec // 2

    def remote(src, dst, send_sem, recv_sem, s, o):
        pltpu.make_async_remote_copy(
            src_ref=src,
            dst_ref=dst,
            send_sem=send_sem,
            recv_sem=recv_sem,
            device_id={"section": s, "obs": o},
            device_id_type=pl.DeviceIdType.MESH,
        ).start()

    def got(ref, sem):
        pltpu.make_async_copy(ref, ref, sem).wait()

    def fan(src, dst, send_sem, recv_sem, s):
        def one(j):
            o = lax.rem(ob + j, O)
            remote(src(o), dst, send_sem, recv_sem, s, o)

        each(1, O, one)

        @pl.when(s != sec)
        def _():
            remote(src(ob), dst, send_sem, recv_sem, s, ob)

        @pl.when(s == sec)
        def _():
            pltpu.make_async_copy(src(ob), dst, recv_sem).start()

    def fanned(like, send_sem, s):
        @pl.when(s != sec)
        def _():
            got(like, send_sem)

        @pl.when(s == sec)
        def _():
            got(like.at[0 : O - 1], send_sem)

    loads = [
        (order_hbm, order_s),
        (bc_hbm, bc_v),
        (pc_hbm, pc_v),
        (x_hbm, x_v),
        (ee_hbm, ee_v),
        (dep_hbm, dep_v),
        (prec_hbm, prec_v),
        (qc_hbm, qc_v),
        (mf_hbm, mf_v),
        (pi_hbm, pi_v),
    ]
    loads = [pltpu.make_async_copy(a, b, load_sem.at[i]) for i, (a, b) in enumerate(loads)]
    for copy in loads:
        copy.start()
    order_in, bc_in, pc_in, x_in, ee_in, dep_in, prec_in, qc_in, mf_in, pi_in = loads

    barrier = pltpu.get_barrier_semaphore()

    def greet(s):
        def one(o):
            @pl.when(jnp.logical_not((s == sec) & (o == ob)))
            def _():
                pl.semaphore_signal(
                    barrier,
                    inc=1,
                    device_id={"section": s, "obs": o},
                    device_id_type=pl.DeviceIdType.MESH,
                )

        each(0, O, one)

    lax.fori_loop(0, S, lambda s, c: (greet(s), c)[1], 0)

    bc_in.wait()
    line = bc_v[...]
    if NB < 128:
        line = jnp.concatenate([line, jnp.full((K, 128 - NB), -1, jnp.int32)], axis=1)
    lists[...] = jnp.full((8, 128), -1, jnp.int32)
    lists[0:K, :] = line
    pc_in.wait()
    for m in range(K):
        pcs[m] = jnp.zeros((NP, C), F32)
        pcs[m, 0:N, :] = pc_v[:, m, :]
        betas[m] = pcs[m]
    pl.semaphore_wait(barrier, S * O - 1)

    @pl.when(sec == 1)
    def _():
        def one(m):
            fan(lambda o: pcs.at[m], pcr.at[m, ob], p_send.at[m], p_recv.at[m], 0)

        lax.fori_loop(0, K, lambda m, c: (one(m), c)[1], 0)

    def send_lists(q):
        fan(lambda o: lists, bcr.at[sec, ob], bc_send.at[q], bc_recv.at[sec], 2 * q + 1)

    lax.fori_loop(0, G, lambda q, c: (send_lists(q), c)[1], 0)

    cs[...] = jnp.zeros_like(cs)

    eye = iota((128, 128), 0) == iota((128, 128), 1)
    upto = iota((128, 128), 0) <= iota((128, 128), 1)
    for m in range(K):
        row = jnp.broadcast_to(lists[m : m + 1, :].astype(F32), (128, 128))
        col = jnp.sum(jnp.where(eye, row, 0.0), axis=1, keepdims=True)
        range_row = jnp.floor((row + 0.5) * (1.0 / C))
        range_col = jnp.floor((col + 0.5) * (1.0 / C))
        same = range_row == range_col
        rank_row = jnp.sum(jnp.where(same & upto, 1.0, 0.0), axis=0, keepdims=True)
        back = jnp.where(same & (iota((128, 128), 0) >= iota((128, 128), 1)), 1.0, 0.0)
        rank_col = jnp.sum(back, axis=1, keepdims=True)
        chcol[m] = jnp.broadcast_to(col[0:NB], (NB, 128))
        slot = iota((Q, 128), 0)
        hit = (range_row[0:1] == (slot // SL).astype(F32)) & (rank_row == (slot % SL + 1).astype(F32))
        place[m] = jnp.where(hit, 1.0, 0.0).astype(BF16)
        slot = iota((NB, Q), 1)
        hit = (range_col[0:NB] == (slot // SL).astype(F32)) & (rank_col[0:NB] == (slot % SL + 1).astype(F32))
        place_t[m] = jnp.where(hit, 1.0, 0.0).astype(BF16)

    x_in.wait()
    ee_in.wait()

    def products(b):
        lanes = pl.ds(pl.multiple_of(b * 128, 128), 128)
        for i in range(N):
            xs[b, i * K : (i + 1) * K, :] = x_v[i, :, lanes].astype(F32)
        xs[b, N * K : (N + 1) * K, :] = jnp.ones((K, 128), F32)
        xs[b, (N + 1) * K :, :] = jnp.zeros(((NP - N - 1) * K, 128), F32)
        for m in range(K):
            xb = xs[b, pl.ds(m, NP, stride=K), :].astype(BF16)
            xh[m, :, lanes] = xb
            both = dot(xb, ee_v[...], TN)
            pt[m, lanes, :] = (both[:, 0:TL] * both[:, TL:]).astype(BF16)

    lax.fori_loop(0, NB, lambda b, c: (products(b), c)[1], 0)
    dep_in.wait()
    prec_in.wait()
    qc_in.wait()

    def split_f32(x):
        return [p.astype(F32) for p in split3(x)]

    def row_entry(m):
        @pl.when(sec == 0)
        def _():
            got(pcr.at[m], p_recv.at[m])
            channel = chcol[m]
            coef = jnp.zeros((NB, NP), F32)
            lane = iota((NB, C), 1).astype(F32)
            for o in range(O):
                wide = jnp.broadcast_to(channel[:, 0:1], (NB, C)) - float(o * C)
                hot = jnp.where(lane == wide, 1.0, 0.0).astype(BF16)
                for part in split3(pcr[m, o]):
                    coef = coef + dot(hot, part, NT)
            coef_v[...] = coef

        @pl.when(sec != 0)
        def _():
            got(cr.at[m], c_recv.at[m])
            slots = cr[m].reshape(Q, 128)[:, 0:NP]
            coef_v[...] = sum(dot(place_t[m], part, NN) for part in split3(slots))

        pieces = split_f32(coef_v[...])
        sub = iota((8, 128), 0)
        tiles = []
        for q in range(NB // 8):
            stack = jnp.concatenate([p[8 * q : 8 * q + 8] for p in pieces], axis=0).astype(BF16)
            tile = jnp.zeros((8, 128), F32)
            for c in range(4):
                at = (8 * q + 2 * c) * 128
                full = dot(stack, xh[m, :, at : at + 256], NN)
                full = full[0:8] + full[8:16] + full[16:24]
                tile = jnp.where(sub == 2 * c, full[:, 0:128], tile)
                tile = jnp.where(sub == 2 * c + 1, full[:, 128:256], tile)
            tiles.append(tile)
        offset = jnp.concatenate(tiles, axis=0)
        rows = pl.ds(m, NB, stride=K)
        residual = dep_v[rows, :] - offset
        precision = prec_v[rows, :]
        passed = qc_v[rows, :].astype(F32)
        weight = passed * precision / (1.0 + precision * residual * residual / HUBER_SQ)
        pull = weight * residual
        total = jnp.sum(jnp.sum(pull * residual, axis=0, keepdims=True), axis=1, keepdims=True)
        count = jnp.sum(jnp.sum(passed, axis=0, keepdims=True), axis=1, keepdims=True)
        weight_hi = weight.astype(BF16).astype(F32)
        weight_lo = weight - weight_hi
        pull_hi = pull.astype(BF16).astype(F32)
        pull_lo = pull - pull_hi
        group = iota((32, 128), 0) % 8
        lane = iota((8, TL), 1)
        sums = []
        for q in range(NB // 8):
            stack = jnp.concatenate(
                [v[8 * q : 8 * q + 8] for v in (weight_hi, weight_lo, pull_hi, pull_lo)], axis=0
            )
            acc = jnp.zeros((32, TL), F32)
            for c in range(4):
                at = (8 * q + 2 * c) * 128
                left = jnp.concatenate(
                    [jnp.where(group == 2 * c, stack, 0.0), jnp.where(group == 2 * c + 1, stack, 0.0)], axis=1
                )
                acc = acc + dot(left.astype(BF16), pt[m, at : at + 256, :], NN)
            sums.append(jnp.where(lane < T, acc[0:8] + acc[8:16], acc[16:24] + acc[24:32]))
        packed = jnp.concatenate(sums, axis=0)
        place_m = place[m][:, 0:NB]
        out = sum(dot(place_m, part, NN) for part in split3(packed))
        lane = iota((Q, TL), 1)
        out = jnp.where(lane == T + N, total, jnp.where(lane == T + N + 1, count, out))
        ts[m] = out.reshape(O, SL, TL)
        fan(lambda o: ts.at[m, o], tr.at[sec, m, ob], t_send.at[m], t_recv.at[sec, m], sec + 1 - lax.rem(sec, 2))

    def normal_terms(w, m):
        terms = tr[w, m].reshape(Q, TL)
        row = iota((Q, TL), 0)
        sums = jnp.sum(jnp.where(row % SL == 0, terms, 0.0), axis=0, keepdims=True)
        inverse = (sums[:, T + N + 1 : T + N + 2] + PRIOR_WEIGHT) / (sums[:, T + N : T + N + 1] + PRIOR_WEIGHT)
        return sum(dot(part, hots[w, m], TN) for part in split3(terms)) * inverse

    def solve(target_at):
        H = NP // 8
        sub = iota((8, C), 0)
        cols = []
        for k in range(N):
            at = k * N - k * (k - 1) // 2 - k
            cols.append([work[at + 8 * h : at + 8 * h + 8, :] for h in range(H)])
        right = [work[target_at + 8 * h : target_at + 8 * h + 8, :] for h in range(H)]
        scale = [jnp.ones((8, C), F32) for _ in range(H)]
        for j in range(N):
            h, r = j // 8, j % 8
            col = cols[j]
            root = lax.rsqrt(jnp.broadcast_to(col[h][r : r + 1], (8, C)))
            inverse = root * root
            factor = [v * inverse for v in col]
            factor[h] = jnp.where(sub == r, 0.0, factor[h])
            scale[h] = jnp.where(sub == r, inverse, scale[h])
            step = jnp.broadcast_to(right[h][r : r + 1], (8, C))
            right = [right[i] - factor[i] * step for i in range(H)]
            for k in range(j + 1, N):
                kh, kr = k // 8, k % 8
                pivot = jnp.broadcast_to(col[kh][kr : kr + 1], (8, C))
                for i in range(H):
                    if i >= kh or i < h or (i == h and r > 0):
                        cols[k][i] = cols[k][i] - factor[i] * pivot
                cols[k][h] = jnp.where(sub == r, pivot, cols[k][h])
        return jnp.concatenate([right[i] * scale[i] for i in range(H)], axis=0)

    def hub_entry(w, par, m):
        got(tr.at[w, m], t_recv.at[w, m])
        for q in range(1, G):

            @pl.when(q > g)
            def _():
                remote(tr.at[w, m], tr.at[w, m], f_send.at[par, m, q], f_recv.at[w, m], 2 * q + 1, ob)

        @pl.when((par == 0) & (g > 0))
        def _():
            got(beta_in.at[m], b_recv.at[m])
            betas[m] = beta_in[m]

        normal = normal_terms(w, m)
        post = state[m] + normal[0:T]
        work[0:T, :] = post
        work[T:TL, :] = normal[T:TL]
        state[m] = post * mf_v[...]
        iob[par, m] = post
        fresh = betas[m] + jnp.where(iota((NP, C), 0) < N, solve(T), 0.0)
        betas[m] = fresh
        cob[par, m] = fresh

        @pl.when(w + 1 < S)
        def _():
            hot = hots[w + 1, m]
            slots = sum(dot(hot, part, NT) for part in split3(fresh))
            cs[par, m, :, :, 0:NP] = slots.reshape(O, SL, NP)
            fan(lambda o: cs.at[par, m, o], cr.at[m, ob], c_send.at[par, m], c_recv.at[m], w + 1)

        @pl.when(par == 0)
        def _():
            remote(iob.at[0, m], iob.at[1, m], o_send.at[m, 0], o_recv.at[m, 0], sec - 1, ob)
            remote(cob.at[0, m], cob.at[1, m], o_send.at[m, 1], o_recv.at[m, 1], sec - 1, ob)

        @pl.when((par == 1) & (g + 1 < G))
        def _():
            remote(cob.at[1, m], beta_in.at[m], b_send.at[m], b_recv.at[m], sec + 2, ob)

    def hub_begin():
        pi_in.wait()
        mf_in.wait()
        for m in range(K):
            state[m] = pi_v[:, m, :]
        low = ob * C
        prefix = jnp.where(iota((128, 128), 0) <= iota((128, 128), 1), 1.0, 0.0).astype(BF16)
        rank_of_row = (iota((Q, 128), 0) % SL + 1).astype(F32)
        lane = iota((Q, C), 1).astype(F32)

        def window_hots(w):
            got(bcr.at[w], bc_recv.at[w])
            for m in range(K):
                channel = jnp.concatenate(
                    [jnp.broadcast_to(bcr[w, o, m : m + 1, :], (SL, 128)) for o in range(O)], axis=0
                )
                inside = (channel >= low) & (channel < low + C)
                rank = dot(jnp.where(inside, 1.0, 0.0).astype(BF16), prefix, NN)
                hit = inside & (rank == rank_of_row)
                value = jnp.sum(jnp.where(hit, (channel - low + 1).astype(F32), 0.0), axis=1, keepdims=True)
                hots[w, m] = jnp.where(lane == value - 1.0, 1.0, 0.0).astype(BF16)

        lax.fori_loop(0, S, lambda w, c: (window_hots(w), c)[1], 0)

        def earlier(w):
            def one(m):
                got(tr.at[w, m], f_recv.at[w, m])
                state[m] = (state[m] + normal_terms(w, m)[0:T]) * mf_v[...]

            lax.fori_loop(0, K, lambda m, c: (one(m), c)[1], 0)

        lax.fori_loop(0, 2 * g, lambda w, c: (earlier(w), c)[1], 0)

    @pl.when(odd)
    def _():
        hub_begin()

    @pl.when(jnp.logical_not(odd))
    def _():
        pi_in.wait()
        mf_in.wait()

    def turn(par):
        @pl.when(odd)
        def _():
            lax.fori_loop(0, K, lambda m, c: (hub_entry(2 * g + par, par, m), c)[1], 0)

        @pl.when(par == 0)
        def _():
            lax.fori_loop(0, K, lambda m, c: (row_entry(m), c)[1], 0)

    lax.fori_loop(0, 2, lambda par, c: (turn(par), c)[1], 0)

    @pl.when(jnp.logical_not(odd))
    def _():
        for m in range(K):
            got(iob.at[1, m], o_recv.at[m, 0])
            got(cob.at[1, m], o_recv.at[m, 1])

    order_in.wait()
    for k in range(K):
        m = order_s[k]
        io_out[:, k, :] = iob[1, m]
        co_out[:, k, :] = cob[1, m, 0:N, :]

    def drain(m):
        @pl.when(sec == 1)
        def _():
            got(pcr.at[m], p_send.at[m])

        fanned(ts.at[m], t_send.at[m], sec + 1 - lax.rem(sec, 2))

        @pl.when(odd)
        def _():
            fanned(cr.at[m], c_send.at[0, m], sec)

            @pl.when(sec + 1 < S)
            def _():
                fanned(cr.at[m], c_send.at[1, m], sec + 1)
                got(betas.at[m], b_send.at[m])

            for par in range(2):
                for q in range(1, G):

                    @pl.when(q > g)
                    def _():
                        got(ts.at[m], f_send.at[par, m, q])

            got(iob.at[0, m], o_send.at[m, 0])
            got(cob.at[0, m], o_send.at[m, 1])

    lax.fori_loop(0, K, lambda m, c: (drain(m), c)[1], 0)
    for q in range(G):
        fanned(bcr.at[0], bc_send.at[q], 2 * q + 1)


def local(
    predictors,
    departures,
    obs_precision,
    qc_pass,
    block_channel,
    stream_order,
    prior_coeffs,
    prior_info,
    memory_factor,
):
    S, O = lax.axis_size("section"), lax.axis_size("obs")
    K, N, C = prior_coeffs.shape
    T = prior_info.shape[1]
    NB = block_channel.shape[2]
    R = predictors.shape[3]
    width = R // NB
    assert width == 128 and S % 2 == 0 and K <= 8 and NB <= 128 and NB % 8 == 0
    NP = round_up(N + 1, 8)
    SL = round_up(max(2 * NB // O, 1), 8)
    TL = round_up(T + NP + 2, 128)
    G, Q = S // 2, O * SL
    pairs = [(i, j) for i in range(N) for j in range(i, N)]
    expand = np.zeros((NP, 2 * TL), np.float32)
    for t, (i, j) in enumerate(pairs):
        expand[i, t] = 1.0
        expand[j, TL + t] = 1.0
    for i in range(N):
        expand[i, T + i] = 1.0
        expand[N, TL + T + i] = 1.0
    cfg = (S, O, K, N, NP, T, C, NB, SL, TL)

    def by_block(array):
        return array[0].reshape(K, NB, width).transpose(1, 0, 2).reshape(NB * K, width)

    vm = pl.BlockSpec(memory_space=pltpu.VMEM)
    hbm = pl.BlockSpec(memory_space=pltpu.HBM)
    dma = pltpu.SemaphoreType.DMA
    coeffs, info = pl.pallas_call(
        functools.partial(kernel, cfg),
        out_shape=(
            jax.ShapeDtypeStruct((N, K, C), F32),
            jax.ShapeDtypeStruct((T, K, C), F32),
        ),
        in_specs=[hbm] * 10,
        out_specs=(vm, vm),
        scratch_shapes=[
            pltpu.SMEM((K,), jnp.int32),
            pltpu.VMEM((N, K, R), BF16),
            pltpu.VMEM((NB * K, 128), F32),
            pltpu.VMEM((NB * K, 128), F32),
            pltpu.VMEM((NB * K, 128), jnp.int32),
            pltpu.VMEM((K, NB), jnp.int32),
            pltpu.VMEM((N, K, C), F32),
            pltpu.VMEM((T, K, C), F32),
            pltpu.VMEM((1, C), F32),
            pltpu.VMEM((NP, 2 * TL), BF16),
            pltpu.VMEM((8, 128), jnp.int32),
            pltpu.VMEM((S, O, 8, 128), jnp.int32),
            pltpu.VMEM((K, NP, C), F32),
            pltpu.VMEM((K, O, NP, C), F32),
            pltpu.VMEM((2, K, O, SL, 128), F32),
            pltpu.VMEM((K, O, SL, 128), F32),
            pltpu.VMEM((K, O, SL, TL), F32),
            pltpu.VMEM((S, K, O, SL, TL), F32),
            pltpu.VMEM((NB, NP * K, 128), F32),
            pltpu.VMEM((K, NP, R), BF16),
            pltpu.VMEM((K, R, TL), BF16),
            pltpu.VMEM((K, NB, 128), F32),
            pltpu.VMEM((K, Q, 128), BF16),
            pltpu.VMEM((K, NB, Q), BF16),
            pltpu.VMEM((NB, NP), F32),
            pltpu.VMEM((S, K, Q, C), BF16),
            pltpu.VMEM((K, T, C), F32),
            pltpu.VMEM((K, NP, C), F32),
            pltpu.VMEM((K, NP, C), F32),
            pltpu.VMEM((TL, C), F32),
            pltpu.VMEM((2, K, NP, C), F32),
            pltpu.VMEM((2, K, T, C), F32),
            dma((10,)),
            dma((G,)),
            dma((S,)),
            dma((K,)),
            dma((K,)),
            dma((2, K)),
            dma((K,)),
            dma((K,)),
            dma((S, K)),
            dma((2, K, G)),
            dma((S, K)),
            dma((K,)),
            dma((K,)),
            dma((K, 2)),
            dma((K, 2)),
        ],
        compiler_params=pltpu.CompilerParams(
            has_side_effects=True, collective_id=0, vmem_limit_bytes=48 * 1024 * 1024
        ),
    )(*(pltpu.with_memory_space_constraint(a, pltpu.HBM) for a in (
        stream_order,
        predictors[0].transpose(1, 0, 2),
        by_block(departures),
        by_block(obs_precision),
        by_block(qc_pass),
        block_channel[0],
        prior_coeffs.transpose(1, 0, 2),
        prior_info.transpose(1, 0, 2),
        memory_factor[None],
        jnp.asarray(expand, BF16),
    )))
    return coeffs.transpose(1, 0, 2)[None], info.transpose(1, 0, 2)[None]


def solution(mesh):
    in_specs = (
        P("section", None, None, "obs"),
        P("section", None, "obs"),
        P("section", None, "obs"),
        P("section", None, "obs"),
        P("section", None, "obs"),
        P(),
        P(None, None, "obs"),
        P(None, None, "obs"),
        P("obs"),
    )
    out_specs = (P("section", None, None, "obs"), P("section", None, None, "obs"))
    return jax.shard_map(local, mesh=mesh, in_specs=in_specs, out_specs=out_specs, check_vma=False)
```

```python
import functools

import jax
import jax.numpy as jnp
import numpy as np
from jax import lax
from jax.experimental import pallas as pl
from jax.experimental.pallas import tpu as pltpu
from jax.sharding import PartitionSpec as P

HUBER_SQ = 9.0
PRIOR_WEIGHT = 64.0
F32 = jnp.float32
BF16 = jnp.bfloat16
NN = (((1,), (0,)), ((), ()))
NT = (((1,), (1,)), ((), ()))
TN = (((0,), (0,)), ((), ()))


def round_up(n, m):
    return -(-n // m) * m


def split3(x):
    hi = x.astype(BF16)
    rest = x - hi.astype(F32)
    mid = rest.astype(BF16)
    low = (rest - mid.astype(F32)).astype(BF16)
    return hi, mid, low


def dot(a, b, dims):
    return lax.dot_general(a, b, dims, preferred_element_type=F32)


def each(low, high, body):
    n = high - low

    def step(i, _):
        body(i)
        return 0

    lax.fori_loop(low, high, step, 0, unroll=n if n <= 8 else 1)


def iota(shape, axis):
    return lax.broadcasted_iota(jnp.int32, shape, axis)


def kernel(
    cfg,
    order_hbm,
    x_hbm,
    dep_hbm,
    prec_hbm,
    qc_hbm,
    bc_hbm,
    pc_hbm,
    pi_hbm,
    mf_hbm,
    ee_hbm,
    co_out,
    io_out,
    order_s,
    x_v,
    dep_v,
    prec_v,
    qc_v,
    bc_v,
    pc_v,
    pi_v,
    mf_v,
    ee_v,
    lists,
    bcr,
    pcs,
    pcr,
    cs,
    cr,
    ts,
    tr,
    xs,
    xh,
    pt,
    chcol,
    place,
    place_t,
    coef_v,
    hots,
    state,
    betas,
    beta_in,
    beta_pass,
    base,
    held,
    match,
    first,
    follow,
    work,
    cob,
    iob,
    load_sem,
    bc_send,
    bc_recv,
    p_send,
    p_recv,
    c_send,
    c_recv,
    t_send,
    t_recv,
    f_send,
    f_recv,
    b_send,
    b_recv,
    o_send,
    o_recv,
):
    S, O, K, N, NP, T, C, NB, SL, TL = cfg
    G = S // 2
    Q = O * SL
    sec = lax.axis_index("section")
    ob = lax.axis_index("obs")
    core = lax.rem(sec, 2)
    odd = core == 1
    g = sec // 2
    mine = K // 2

    def hub_of(m):
        return 2 * g + 1 - lax.rem(m, 2)

    def remote(src, dst, send_sem, recv_sem, s, o):
        pltpu.make_async_remote_copy(
            src_ref=src,
            dst_ref=dst,
            send_sem=send_sem,
            recv_sem=recv_sem,
            device_id={"section": s, "obs": o},
            device_id_type=pl.DeviceIdType.MESH,
        ).start()

    def got(ref, sem):
        pltpu.make_async_copy(ref, ref, sem).wait()

    def fan(src, dst, send_sem, recv_sem, s):
        def one(j):
            o = lax.rem(ob + j, O)
            remote(src(o), dst, send_sem, recv_sem, s, o)

        each(1, O, one)

        @pl.when(s != sec)
        def _():
            remote(src(ob), dst, send_sem, recv_sem, s, ob)

        @pl.when(s == sec)
        def _():
            pltpu.make_async_copy(src(ob), dst, recv_sem).start()

    def fanned(like, send_sem, s):
        @pl.when(s != sec)
        def _():
            got(like, send_sem)

        @pl.when(s == sec)
        def _():
            got(like.at[0 : O - 1], send_sem)

    loads = [
        (order_hbm, order_s),
        (bc_hbm, bc_v),
        (pc_hbm, pc_v),
        (x_hbm, x_v),
        (ee_hbm, ee_v),
        (dep_hbm, dep_v),
        (prec_hbm, prec_v),
        (qc_hbm, qc_v),
        (mf_hbm, mf_v),
        (pi_hbm, pi_v),
    ]
    loads = [pltpu.make_async_copy(a, b, load_sem.at[i]) for i, (a, b) in enumerate(loads)]
    for copy in loads:
        copy.start()
    order_in, bc_in, pc_in, x_in, ee_in, dep_in, prec_in, qc_in, mf_in, pi_in = loads

    barrier = pltpu.get_barrier_semaphore()

    def greet(s):
        def one(o):
            @pl.when(jnp.logical_not((s == sec) & (o == ob)))
            def _():
                pl.semaphore_signal(
                    barrier,
                    inc=1,
                    device_id={"section": s, "obs": o},
                    device_id_type=pl.DeviceIdType.MESH,
                )

        each(0, O, one)

    lax.fori_loop(0, S, lambda s, c: (greet(s), c)[1], 0)

    bc_in.wait()
    line = [bc_v[m : m + 1, :] for m in range(K)]
    if K * NB < 128:
        line.append(jnp.full((1, 128 - K * NB), -1, jnp.int32))
    lists[...] = jnp.concatenate(line, axis=1)
    pc_in.wait()
    for m in range(K):
        pcs[m] = jnp.zeros((NP, C), F32)
        pcs[m, 0:N, :] = pc_v[:, m, :]
        betas[m] = pcs[m]
    def unpack():
        x_in.wait()
        ee_in.wait()
        for b in range(NB):
            for i in range(N):
                xs[b, i * K : (i + 1) * K, :] = x_v[i, :, b * 128 : (b + 1) * 128].astype(F32)
            xs[b, N * K : (N + 1) * K, :] = jnp.ones((K, 128), F32)
            xs[b, (N + 1) * K :, :] = jnp.zeros(((NP - N - 1) * K, 128), F32)

    def products(low, high):
        def one(b):
            lanes = pl.ds(pl.multiple_of(b * 128, 128), 128)
            for m in range(low, high):
                xb = xs[b, pl.ds(m, NP, stride=K), :].astype(BF16)
                xh[m, :, lanes] = xb
                both = dot(xb, ee_v[...], TN)
                pt[m, lanes, :] = (both[:, 0:TL] * both[:, TL:]).astype(BF16)

        lax.fori_loop(0, NB, lambda b, c: (one(b), c)[1], 0, unroll=4)

    @pl.when(jnp.logical_not(odd))
    def _():
        unpack()
        products(0, K // 2)

    pl.semaphore_wait(barrier, S * O - 1)

    def send_lists(s):
        fan(lambda o: lists, bcr.at[sec, ob], bc_send.at[s], bc_recv.at[sec], s)

    lax.fori_loop(0, S, lambda s, c: (send_lists(s), c)[1], 0)

    def send_prior(m):
        @pl.when(sec == 2 * lax.rem(m, G) + 1)
        def _():
            fan(lambda o: pcs.at[m], pcr.at[m, ob], p_send.at[m], p_recv.at[m], 0)

    lax.fori_loop(0, K, lambda m, c: (send_prior(m), c)[1], 0)

    cs[...] = jnp.zeros_like(cs)

    eye = iota((128, 128), 0) == iota((128, 128), 1)
    upto = iota((128, 128), 0) <= iota((128, 128), 1)
    for m in range(K):
        row = bc_v[m : m + 1, :].astype(F32)
        if NB < 128:
            row = jnp.concatenate([row, jnp.full((1, 128 - NB), -1.0, F32)], axis=1)
        row = jnp.broadcast_to(row, (128, 128))
        col = jnp.sum(jnp.where(eye, row, 0.0), axis=1, keepdims=True)
        range_row = jnp.floor((row + 0.5) * (1.0 / C))
        range_col = jnp.floor((col + 0.5) * (1.0 / C))
        same = range_row == range_col
        rank_row = jnp.sum(jnp.where(same & upto, 1.0, 0.0), axis=0, keepdims=True)
        back = jnp.where(same & (iota((128, 128), 0) >= iota((128, 128), 1)), 1.0, 0.0)
        rank_col = jnp.sum(back, axis=1, keepdims=True)
        chcol[m] = jnp.broadcast_to(col[0:NB], (NB, 128))
        slot = iota((Q, 128), 0)
        hit = (range_row[0:1] == (slot // SL).astype(F32)) & (rank_row == (slot % SL + 1).astype(F32))
        place[m] = jnp.where(hit, 1.0, 0.0).astype(BF16)
        slot = iota((NB, Q), 1)
        hit = (range_col[0:NB] == (slot // SL).astype(F32)) & (rank_col[0:NB] == (slot % SL + 1).astype(F32))
        place_t[m] = jnp.where(hit, 1.0, 0.0).astype(BF16)

    @pl.when(odd)
    def _():
        unpack()
        products(0, K // 2)

    products(K // 2, K)

    dep_in.wait()
    prec_in.wait()
    qc_in.wait()

    def split_f32(x):
        return [p.astype(F32) for p in split3(x)]

    def row_entry(m):
        @pl.when(sec == 0)
        def _():
            got(pcr.at[m], p_recv.at[m])
            channel = chcol[m]
            coef = jnp.zeros((NB, NP), F32)
            lane = iota((NB, C), 1).astype(F32)
            for o in range(O):
                wide = jnp.broadcast_to(channel[:, 0:1], (NB, C)) - float(o * C)
                hot = jnp.where(lane == wide, 1.0, 0.0).astype(BF16)
                for part in split3(pcr[m, o]):
                    coef = coef + dot(hot, part, NT)
            coef_v[...] = coef

        @pl.when(sec != 0)
        def _():
            got(cr.at[m], c_recv.at[m])
            slots = cr[m].reshape(Q, 128)[:, 0:NP]
            coef_v[...] = sum(dot(place_t[m], part, NN) for part in split3(slots))

        pieces = split_f32(coef_v[...])
        sub = iota((8, 128), 0)
        tiles = []
        for q in range(NB // 8):
            stack = jnp.concatenate([p[8 * q : 8 * q + 8] for p in pieces], axis=0).astype(BF16)
            tile = jnp.zeros((8, 128), F32)
            for c in range(4):
                at = (8 * q + 2 * c) * 128
                full = dot(stack, xh[m, :, at : at + 256], NN)
                full = full[0:8] + full[8:16] + full[16:24]
                tile = jnp.where(sub == 2 * c, full[:, 0:128], tile)
                tile = jnp.where(sub == 2 * c + 1, full[:, 128:256], tile)
            tiles.append(tile)
        offset = jnp.concatenate(tiles, axis=0)
        rows = pl.ds(m, NB, stride=K)
        residual = dep_v[rows, :] - offset
        precision = prec_v[rows, :]
        passed = qc_v[rows, :].astype(F32)
        weight = passed * precision / (1.0 + precision * residual * residual / HUBER_SQ)
        pull = weight * residual
        total = jnp.sum(jnp.sum(pull * residual, axis=0, keepdims=True), axis=1, keepdims=True)
        count = jnp.sum(jnp.sum(passed, axis=0, keepdims=True), axis=1, keepdims=True)
        weight_hi = weight.astype(BF16).astype(F32)
        weight_lo = weight - weight_hi
        pull_hi = pull.astype(BF16).astype(F32)
        pull_lo = pull - pull_hi
        group = iota((32, 128), 0) % 8
        lane = iota((8, TL), 1)
        sums = []
        for q in range(NB // 8):
            stack = jnp.concatenate(
                [v[8 * q : 8 * q + 8] for v in (weight_hi, weight_lo, pull_hi, pull_lo)], axis=0
            )
            acc = jnp.zeros((32, TL), F32)
            for c in range(4):
                at = (8 * q + 2 * c) * 128
                left = jnp.concatenate(
                    [jnp.where(group == 2 * c, stack, 0.0), jnp.where(group == 2 * c + 1, stack, 0.0)], axis=1
                )
                acc = acc + dot(left.astype(BF16), pt[m, at : at + 256, :], NN)
            sums.append(jnp.where(lane < T, acc[0:8] + acc[8:16], acc[16:24] + acc[24:32]))
        packed = jnp.concatenate(sums, axis=0)
        place_m = place[m][:, 0:NB]
        out = sum(dot(place_m, part, NN) for part in split3(packed))
        lane = iota((Q, TL), 1)
        out = jnp.where(lane == T + N, total, jnp.where(lane == T + N + 1, count, out))
        ts[m] = out.reshape(O, SL, TL)
        fan(lambda o: ts.at[m, o], tr.at[sec, m, ob], t_send.at[m], t_recv.at[sec, m], hub_of(m))

    def scale_of(terms):
        row = iota((Q, TL), 0)
        sums = jnp.sum(jnp.where(row % SL == 0, terms, 0.0), axis=0, keepdims=True)
        return (sums[:, T + N + 1 : T + N + 2] + PRIOR_WEIGHT) / (sums[:, T + N : T + N + 1] + PRIOR_WEIGHT)

    def solve():
        H = NP // 8
        sub = iota((8, Q), 0)
        cols = []
        for k in range(N):
            at = k * N - k * (k - 1) // 2 - k
            cols.append([work[at + 8 * h : at + 8 * h + 8, :] for h in range(H)])
        right = [work[T + 8 * h : T + 8 * h + 8, :] for h in range(H)]
        scale = [jnp.ones((8, Q), F32) for _ in range(H)]
        for j in range(N):
            h, r = j // 8, j % 8
            col = cols[j]
            root = lax.rsqrt(jnp.broadcast_to(col[h][r : r + 1], (8, Q)))
            inverse = root * root
            factor = [v * inverse for v in col]
            factor[h] = jnp.where(sub == r, 0.0, factor[h])
            scale[h] = jnp.where(sub == r, inverse, scale[h])
            step = jnp.broadcast_to(right[h][r : r + 1], (8, Q))
            right = [right[i] - factor[i] * step for i in range(H)]
            for k in range(j + 1, N):
                kh, kr = k // 8, k % 8
                pivot = jnp.broadcast_to(col[kh][kr : kr + 1], (8, Q))
                for i in range(H):
                    if i >= kh or i < h or (i == h and r > 0):
                        cols[k][i] = cols[k][i] - factor[i] * pivot
                cols[k][h] = jnp.where(sub == r, pivot, cols[k][h])
        return jnp.concatenate([right[i] * scale[i] for i in range(H)], axis=0)

    def hub_ready(par, m):
        w = 2 * g + par

        @pl.when(w + 1 < S)
        def _():
            base[m] = sum(dot(hots[w + 1, m], part, NT) for part in split3(betas[m]))

        held[m] = sum(dot(part, hots[w, m], NT) for part in split3(state[m]))

    def hub_entry(par, m):
        w = 2 * g + par
        hot = hots[w, m]
        got(tr.at[w, m], t_recv.at[w, m])
        for q in range(1, G):

            @pl.when(q > g)
            def _():
                remote(tr.at[w, m], tr.at[w, m], f_send.at[par, m, q], f_recv.at[w, m], 2 * q + core, ob)

        terms = tr[w, m].reshape(Q, TL)
        parts = split3(terms)
        inverse = scale_of(terms)
        normal = sum(dot(part, match[par, m], TN) for part in parts) * inverse
        work[0:T, :] = held[m] + normal[0:T]
        work[T:TL, :] = normal[T:TL]
        filled = work[0:1, :] > 0.0
        delta = jnp.where((iota((NP, Q), 0) < N) & filled, solve(), 0.0)
        deltas = split3(delta)

        @pl.when(w + 1 < S)
        def _():
            slots = base[m] + sum(dot(follow[par, m], part, NT) for part in deltas)
            cs[par, m, :, :, 0:NP] = slots.reshape(O, SL, NP)
            fan(lambda o: cs.at[par, m, o], cr.at[m, ob], c_send.at[par, m], c_recv.at[m], w + 1)

        here = jnp.where(w == sec, 1, 0)
        fresh = betas[m] + sum(dot(part, first[par, m], NN) for part in deltas)
        betas[m] = fresh
        cob[here, m] = fresh
        post = state[m] + sum(dot(part, hot, TN) for part in parts)[0:T] * inverse
        iob[here, m] = post
        state[m] = post * mf_v[...]

        @pl.when(w != sec)
        def _():
            remote(iob.at[0, m], iob.at[1, m], o_send.at[m, 0], o_recv.at[m, 0], w, ob)
            remote(cob.at[0, m], cob.at[1, m], o_send.at[m, 1], o_recv.at[m, 1], w, ob)

        @pl.when((par == 1) & (g + 1 < G))
        def _():
            beta_pass[m] = fresh
            remote(beta_pass.at[m], beta_in.at[m], b_send.at[m], b_recv.at[m], sec + 2, ob)

    def stream(i):
        return 2 * i + 1 - core

    def hub_begin():
        pi_in.wait()
        mf_in.wait()
        for m in range(K):
            state[m] = pi_v[:, m, :]
        low = ob * C
        prefix = jnp.where(iota((128, 128), 0) <= iota((128, 128), 1), 1.0, 0.0).astype(BF16)
        rank_of_row = (iota((Q, 128), 0) % SL + 1).astype(F32)
        lane = iota((Q, C), 1).astype(F32)

        for w in range(S):
            got(bcr.at[w], bc_recv.at[w])
        owner_lane = iota((Q, 128), 1) // NB

        def window_hots(w):
            channel = jnp.concatenate([jnp.broadcast_to(bcr[w, o], (SL, 128)) for o in range(O)], axis=0)
            inside = (channel >= low) & (channel < low + C)
            for i in range(mine):
                ours = inside & (owner_lane == stream(i))
                rank = dot(jnp.where(ours, 1.0, 0.0).astype(BF16), prefix, NN)
                hit = ours & (rank == rank_of_row)
                value = jnp.sum(jnp.where(hit, (channel - low + 1).astype(F32), 0.0), axis=1, keepdims=True)
                hots[w, stream(i)] = jnp.where(lane == value - 1.0, 1.0, 0.0).astype(BF16)

        each(0, S, window_hots)
        earlier_slot = iota((Q, Q), 1) < iota((Q, Q), 0)

        def links(par, i):
            m = stream(i)
            w = 2 * g + par
            hot = hots[w, m]
            same = dot(hot, hot, NT)
            match[par, m] = same.astype(BF16)
            copies = jnp.sum(jnp.where(earlier_slot, same, 0.0), axis=1, keepdims=True)
            lead = jnp.where(copies == 0.0, hot.astype(F32), 0.0).astype(BF16)
            first[par, m] = lead

            after = jnp.minimum(w + 1, S - 1)
            follow[par, m] = dot(hots[after, m], lead, NT).astype(BF16)

        for i in range(mine):
            for par in range(2):
                links(par, i)

        def earlier(w):
            def one(i):
                m = stream(i)
                got(tr.at[w, m], f_recv.at[w, m])
                terms = tr[w, m].reshape(Q, TL)
                normal = sum(dot(part, hots[w, m], TN) for part in split3(terms))[0:T] * scale_of(terms)
                state[m] = (state[m] + normal) * mf_v[...]

            lax.fori_loop(0, mine, lambda i, c: (one(i), c)[1], 0)

        lax.fori_loop(0, 2 * g, lambda w, c: (earlier(w), c)[1], 0)

        @pl.when(g > 0)
        def _():
            def take(i):
                m = stream(i)
                got(beta_in.at[m], b_recv.at[m])
                betas[m] = beta_in[m]

            lax.fori_loop(0, mine, lambda i, c: (take(i), c)[1], 0)

    def turn(par):
        @pl.when(par == core)
        def _():
            lax.fori_loop(0, K, lambda m, c: (row_entry(m), c)[1], 0)

        @pl.when(par == 0)
        def _():
            hub_begin()

        lax.fori_loop(0, mine, lambda i, c: (hub_ready(par, stream(i)), c)[1], 0)
        lax.fori_loop(0, mine, lambda i, c: (hub_entry(par, stream(i)), c)[1], 0)

    lax.fori_loop(0, 2, lambda par, c: (turn(par), c)[1], 0)

    def arrive(i):
        m = 2 * i + core
        got(iob.at[1, m], o_recv.at[m, 0])
        got(cob.at[1, m], o_recv.at[m, 1])

    lax.fori_loop(0, K - mine, lambda i, c: (arrive(i), c)[1], 0)
    order_in.wait()
    for k in range(K):
        m = order_s[k]
        io_out[:, k, :] = iob[1, m]
        co_out[:, k, :] = cob[1, m, 0:N, :]

    def drain(m):
        @pl.when(sec == 2 * lax.rem(m, G) + 1)
        def _():
            got(pcr.at[m], p_send.at[m])

        fanned(ts.at[m], t_send.at[m], hub_of(m))

    def drain_hub(i):
        m = stream(i)
        fanned(cr.at[m], c_send.at[0, m], 2 * g + 1)

        @pl.when(g + 1 < G)
        def _():
            fanned(cr.at[m], c_send.at[1, m], 2 * g + 2)
            got(betas.at[m], b_send.at[m])

        for par in range(2):
            for q in range(1, G):

                @pl.when(q > g)
                def _():
                    got(ts.at[m], f_send.at[par, m, q])

        got(iob.at[0, m], o_send.at[m, 0])
        got(cob.at[0, m], o_send.at[m, 1])

    lax.fori_loop(0, mine, lambda i, c: (drain_hub(i), c)[1], 0)
    lax.fori_loop(0, K, lambda m, c: (drain(m), c)[1], 0)
    lax.fori_loop(0, S, lambda s, c: (fanned(bcr.at[0], bc_send.at[s], s), c)[1], 0)


def local(
    predictors,
    departures,
    obs_precision,
    qc_pass,
    block_channel,
    stream_order,
    prior_coeffs,
    prior_info,
    memory_factor,
):
    S, O = lax.axis_size("section"), lax.axis_size("obs")
    K, N, C = prior_coeffs.shape
    T = prior_info.shape[1]
    NB = block_channel.shape[2]
    R = predictors.shape[3]
    width = R // NB
    assert width == 128 and S % 2 == 0 and K % 2 == 0 and K * NB <= 128 and NB % 8 == 0
    NP = round_up(N + 1, 8)
    SL = round_up(max(2 * NB // O, 1), 8)
    TL = round_up(T + NP + 2, 128)
    G, Q = S // 2, O * SL
    pairs = [(i, j) for i in range(N) for j in range(i, N)]
    expand = np.zeros((NP, 2 * TL), np.float32)
    for t, (i, j) in enumerate(pairs):
        expand[i, t] = 1.0
        expand[j, TL + t] = 1.0
    for i in range(N):
        expand[i, T + i] = 1.0
        expand[N, TL + T + i] = 1.0
    cfg = (S, O, K, N, NP, T, C, NB, SL, TL)

    def by_block(array):
        return array[0].reshape(K, NB, width).transpose(1, 0, 2).reshape(NB * K, width)

    vm = pl.BlockSpec(memory_space=pltpu.VMEM)
    hbm = pl.BlockSpec(memory_space=pltpu.HBM)
    dma = pltpu.SemaphoreType.DMA
    coeffs, info = pl.pallas_call(
        functools.partial(kernel, cfg),
        out_shape=(
            jax.ShapeDtypeStruct((N, K, C), F32),
            jax.ShapeDtypeStruct((T, K, C), F32),
        ),
        in_specs=[hbm] * 10,
        out_specs=(vm, vm),
        scratch_shapes=[
            pltpu.SMEM((K,), jnp.int32),
            pltpu.VMEM((N, K, R), BF16),
            pltpu.VMEM((NB * K, 128), F32),
            pltpu.VMEM((NB * K, 128), F32),
            pltpu.VMEM((NB * K, 128), jnp.int32),
            pltpu.VMEM((K, NB), jnp.int32),
            pltpu.VMEM((N, K, C), F32),
            pltpu.VMEM((T, K, C), F32),
            pltpu.VMEM((1, C), F32),
            pltpu.VMEM((NP, 2 * TL), BF16),
            pltpu.VMEM((1, 128), jnp.int32),
            pltpu.VMEM((S, O, 1, 128), jnp.int32),
            pltpu.VMEM((K, NP, C), F32),
            pltpu.VMEM((K, O, NP, C), F32),
            pltpu.VMEM((2, K, O, SL, 128), F32),
            pltpu.VMEM((K, O, SL, 128), F32),
            pltpu.VMEM((K, O, SL, TL), F32),
            pltpu.VMEM((S, K, O, SL, TL), F32),
            pltpu.VMEM((NB, NP * K, 128), F32),
            pltpu.VMEM((K, NP, R), BF16),
            pltpu.VMEM((K, R, TL), BF16),
            pltpu.VMEM((K, NB, 128), F32),
            pltpu.VMEM((K, Q, 128), BF16),
            pltpu.VMEM((K, NB, Q), BF16),
            pltpu.VMEM((NB, NP), F32),
            pltpu.VMEM((S, K, Q, C), BF16),
            pltpu.VMEM((K, T, C), F32),
            pltpu.VMEM((K, NP, C), F32),
            pltpu.VMEM((K, NP, C), F32),
            pltpu.VMEM((K, NP, C), F32),
            pltpu.VMEM((K, Q, NP), F32),
            pltpu.VMEM((K, T, Q), F32),
            pltpu.VMEM((2, K, Q, Q), BF16),
            pltpu.VMEM((2, K, Q, C), BF16),
            pltpu.VMEM((2, K, Q, Q), BF16),
            pltpu.VMEM((TL, Q), F32),
            pltpu.VMEM((2, K, NP, C), F32),
            pltpu.VMEM((2, K, T, C), F32),
            dma((10,)),
            dma((S,)),
            dma((S,)),
            dma((K,)),
            dma((K,)),
            dma((2, K)),
            dma((K,)),
            dma((K,)),
            dma((S, K)),
            dma((2, K, G)),
            dma((S, K)),
            dma((K,)),
            dma((K,)),
            dma((K, 2)),
            dma((K, 2)),
        ],
        compiler_params=pltpu.CompilerParams(
            has_side_effects=True, collective_id=0, vmem_limit_bytes=48 * 1024 * 1024
        ),
    )(*(pltpu.with_memory_space_constraint(a, pltpu.HBM) for a in (
        stream_order,
        predictors[0].transpose(1, 0, 2),
        by_block(departures),
        by_block(obs_precision),
        by_block(qc_pass),
        block_channel[0],
        prior_coeffs.transpose(1, 0, 2),
        prior_info.transpose(1, 0, 2),
        memory_factor[None],
        jnp.asarray(expand, BF16),
    )))
    return coeffs.transpose(1, 0, 2)[None], info.transpose(1, 0, 2)[None]


def solution(mesh):
    in_specs = (
        P("section", None, None, "obs"),
        P("section", None, "obs"),
        P("section", None, "obs"),
        P("section", None, "obs"),
        P("section", None, "obs"),
        P(),
        P(None, None, "obs"),
        P(None, None, "obs"),
        P("obs"),
    )
    out_specs = (P("section", None, None, "obs"), P("section", None, None, "obs"))
    return jax.shard_map(local, mesh=mesh, in_specs=in_specs, out_specs=out_specs, check_vma=False)
```

```python
import functools

import jax
import jax.numpy as jnp
import numpy as np
from jax import lax
from jax.experimental import pallas as pl
from jax.experimental.pallas import tpu as pltpu
from jax.sharding import PartitionSpec as P

HUBER_SQ = 9.0
PRIOR_WEIGHT = 64.0
F32 = jnp.float32
BF16 = jnp.bfloat16
NN = (((1,), (0,)), ((), ()))
NT = (((1,), (1,)), ((), ()))
TN = (((0,), (0,)), ((), ()))


def round_up(n, m):
    return -(-n // m) * m


def split3(x):
    hi = x.astype(BF16)
    rest = x - hi.astype(F32)
    mid = rest.astype(BF16)
    low = (rest - mid.astype(F32)).astype(BF16)
    return hi, mid, low


def dot(a, b, dims):
    return lax.dot_general(a, b, dims, preferred_element_type=F32)


def each(low, high, body):
    n = high - low

    def step(i, _):
        body(i)
        return 0

    lax.fori_loop(low, high, step, 0, unroll=n if n <= 8 else 1)


def iota(shape, axis):
    return lax.broadcasted_iota(jnp.int32, shape, axis)


def kernel(
    cfg,
    order_hbm,
    x_hbm,
    dep_hbm,
    prec_hbm,
    qc_hbm,
    bc_hbm,
    pc_hbm,
    pi_hbm,
    mf_hbm,
    ee_hbm,
    co_out,
    io_out,
    order_s,
    x_v,
    dep_v,
    prec_v,
    qc_v,
    bc_v,
    pc_v,
    pi_v,
    mf_v,
    ee_v,
    lists,
    bcr,
    pcs,
    pcr,
    cs,
    cr,
    ts,
    tr,
    xs,
    xh,
    pt,
    chcol,
    place,
    place_t,
    coef_v,
    hots,
    state,
    betas,
    beta_in,
    beta_mid,
    state_in,
    base,
    held,
    match,
    first,
    follow,
    work,
    cob,
    iob,
    load_sem,
    bc_send,
    bc_recv,
    p_send,
    p_recv,
    c_send,
    c_recv,
    t_send,
    t_recv,
    f_send,
    f_recv,
    b_send,
    b_recv,
    s_send,
    h_send,
    h_recv,
    o_send,
    o_recv,
):
    S, O, K, N, NP, T, C, NB, SL, TL = cfg
    G = S // 2
    Q = O * SL
    sec = lax.axis_index("section")
    ob = lax.axis_index("obs")
    core = lax.rem(sec, 2)
    odd = core == 1
    g = sec // 2
    hub = 2 * g + 1

    def remote(src, dst, send_sem, recv_sem, s, o):
        pltpu.make_async_remote_copy(
            src_ref=src,
            dst_ref=dst,
            send_sem=send_sem,
            recv_sem=recv_sem,
            device_id={"section": s, "obs": o},
            device_id_type=pl.DeviceIdType.MESH,
        ).start()

    def got(ref, sem):
        pltpu.make_async_copy(ref, ref, sem).wait()

    def fan(src, dst, send_sem, recv_sem, s):
        def one(j):
            o = lax.rem(ob + j, O)
            remote(src(o), dst, send_sem, recv_sem, s, o)

        each(1, O, one)

        @pl.when(s != sec)
        def _():
            remote(src(ob), dst, send_sem, recv_sem, s, ob)

        @pl.when(s == sec)
        def _():
            pltpu.make_async_copy(src(ob), dst, recv_sem).start()

    def fanned(like, send_sem, s):
        @pl.when(s != sec)
        def _():
            got(like, send_sem)

        @pl.when(s == sec)
        def _():
            got(like.at[:, 0 : O - 1], send_sem)

    loads = [
        (order_hbm, order_s),
        (bc_hbm, bc_v),
        (pc_hbm, pc_v),
        (x_hbm, x_v),
        (ee_hbm, ee_v),
        (dep_hbm, dep_v),
        (prec_hbm, prec_v),
        (qc_hbm, qc_v),
        (mf_hbm, mf_v),
        (pi_hbm, pi_v),
    ]
    loads = [pltpu.make_async_copy(a, b, load_sem.at[i]) for i, (a, b) in enumerate(loads)]
    for copy in loads:
        copy.start()
    order_in, bc_in, pc_in, x_in, ee_in, dep_in, prec_in, qc_in, mf_in, pi_in = loads

    barrier = pltpu.get_barrier_semaphore()

    def greet(s):
        def one(o):
            @pl.when(jnp.logical_not((s == sec) & (o == ob)))
            def _():
                pl.semaphore_signal(
                    barrier,
                    inc=1,
                    device_id={"section": s, "obs": o},
                    device_id_type=pl.DeviceIdType.MESH,
                )

        each(0, O, one)

    lax.fori_loop(0, S, lambda s, c: (greet(s), c)[1], 0)

    bc_in.wait()
    line = [bc_v[m : m + 1, :] for m in range(K)]
    if K * NB < 128:
        line.append(jnp.full((1, 128 - K * NB), -1, jnp.int32))
    lists[...] = jnp.concatenate(line, axis=1)
    pc_in.wait()
    for m in range(K):
        pcs[m] = jnp.zeros((NP, C), F32)
        pcs[m, 0:N, :] = pc_v[:, m, :]
        betas[m] = pcs[m]
    def unpack():
        x_in.wait()
        ee_in.wait()
        for b in range(NB):
            for i in range(N):
                xs[b, i * K : (i + 1) * K, :] = x_v[i, :, b * 128 : (b + 1) * 128].astype(F32)
            xs[b, N * K : (N + 1) * K, :] = jnp.ones((K, 128), F32)
            xs[b, (N + 1) * K :, :] = jnp.zeros(((NP - N - 1) * K, 128), F32)

    def products(low, high):
        def one(b):
            lanes = pl.ds(pl.multiple_of(b * 128, 128), 128)
            for m in range(low, high):
                xb = xs[b, pl.ds(m, NP, stride=K), :].astype(BF16)
                xh[m, :, lanes] = xb
                both = dot(xb, ee_v[...], TN)
                pt[m, lanes, :] = (both[:, 0:TL] * both[:, TL:]).astype(BF16)

        lax.fori_loop(0, NB, lambda b, c: (one(b), c)[1], 0, unroll=8)

    @pl.when(jnp.logical_not(odd))
    def _():
        unpack()
        products(0, K // 2)

    pl.semaphore_wait(barrier, S * O - 1)

    def send_lists(s):
        fan(lambda o: lists, bcr.at[sec * O + ob], bc_send, bc_recv.at[sec], s)

    lax.fori_loop(0, S, lambda s, c: (send_lists(s), c)[1], 0)

    def send_prior(m):
        def one(i):
            o = lax.rem(m + g, G) + G * i
            remote(pcs.at[m], pcr.at[m, ob], p_send, p_recv.at[m], 0, o)

        each(0, O // G, one)

    @pl.when(odd)
    def _():
        lax.fori_loop(0, K, lambda m, c: (send_prior(m), c)[1], 0)

    cs[...] = jnp.zeros_like(cs)

    eye = iota((128, 128), 0) == iota((128, 128), 1)
    upto = iota((128, 128), 0) <= iota((128, 128), 1)
    for m in range(K):
        row = bc_v[m : m + 1, :].astype(F32)
        if NB < 128:
            row = jnp.concatenate([row, jnp.full((1, 128 - NB), -1.0, F32)], axis=1)
        row = jnp.broadcast_to(row, (128, 128))
        col = jnp.sum(jnp.where(eye, row, 0.0), axis=1, keepdims=True)
        range_row = jnp.floor((row + 0.5) * (1.0 / C))
        range_col = jnp.floor((col + 0.5) * (1.0 / C))
        same = range_row == range_col
        rank_row = jnp.sum(jnp.where(same & upto, 1.0, 0.0), axis=0, keepdims=True)
        back = jnp.where(same & (iota((128, 128), 0) >= iota((128, 128), 1)), 1.0, 0.0)
        rank_col = jnp.sum(back, axis=1, keepdims=True)
        chcol[m] = jnp.broadcast_to(col[0:NB], (NB, 128))
        slot = iota((Q, 128), 0)
        hit = (range_row[0:1] == (slot // SL).astype(F32)) & (rank_row == (slot % SL + 1).astype(F32))
        place[m] = jnp.where(hit, 1.0, 0.0).astype(BF16)
        slot = iota((NB, Q), 1)
        hit = (range_col[0:NB] == (slot // SL).astype(F32)) & (rank_col[0:NB] == (slot % SL + 1).astype(F32))
        place_t[m] = jnp.where(hit, 1.0, 0.0).astype(BF16)

    @pl.when(odd)
    def _():
        unpack()
        products(0, K // 2)

    products(K // 2, K)

    dep_in.wait()
    prec_in.wait()
    qc_in.wait()

    def split_f32(x):
        return [p.astype(F32) for p in split3(x)]

    def row_entry(m):
        @pl.when(sec == 0)
        def _():
            got(pcr.at[m], p_recv.at[m])
            channel = chcol[m]
            coef = jnp.zeros((NB, NP), F32)
            lane = iota((NB, C), 1).astype(F32)
            for o in range(O):
                wide = jnp.broadcast_to(channel[:, 0:1], (NB, C)) - float(o * C)
                hot = jnp.where(lane == wide, 1.0, 0.0).astype(BF16)
                for part in split3(pcr[m, o]):
                    coef = coef + dot(hot, part, NT)
            coef_v[...] = coef

        @pl.when(sec != 0)
        def _():
            got(cr.at[m], c_recv.at[m])
            slots = cr[m].reshape(Q, 128)[:, 0:NP]
            coef_v[...] = sum(dot(place_t[m], part, NN) for part in split3(slots))

        pieces = split_f32(coef_v[...])
        sub = iota((8, 128), 0)
        tiles = []
        for q in range(NB // 8):
            stack = jnp.concatenate([p[8 * q : 8 * q + 8] for p in pieces], axis=0).astype(BF16)
            tile = jnp.zeros((8, 128), F32)
            for c in range(4):
                at = (8 * q + 2 * c) * 128
                full = dot(stack, xh[m, :, at : at + 256], NN)
                full = full[0:8] + full[8:16] + full[16:24]
                tile = jnp.where(sub == 2 * c, full[:, 0:128], tile)
                tile = jnp.where(sub == 2 * c + 1, full[:, 128:256], tile)
            tiles.append(tile)
        offset = jnp.concatenate(tiles, axis=0)
        rows = pl.ds(m, NB, stride=K)
        residual = dep_v[rows, :] - offset
        precision = prec_v[rows, :]
        passed = qc_v[rows, :].astype(F32)
        weight = passed * precision / (1.0 + precision * residual * residual / HUBER_SQ)
        pull = weight * residual
        total = jnp.sum(jnp.sum(pull * residual, axis=0, keepdims=True), axis=1, keepdims=True)
        count = jnp.sum(jnp.sum(passed, axis=0, keepdims=True), axis=1, keepdims=True)
        weight_hi = weight.astype(BF16).astype(F32)
        weight_lo = weight - weight_hi
        pull_hi = pull.astype(BF16).astype(F32)
        pull_lo = pull - pull_hi
        group = iota((32, 128), 0) % 8
        lane = iota((8, TL), 1)
        sums = []
        for q in range(NB // 8):
            stack = jnp.concatenate(
                [v[8 * q : 8 * q + 8] for v in (weight_hi, weight_lo, pull_hi, pull_lo)], axis=0
            )
            acc = jnp.zeros((32, TL), F32)
            for c in range(4):
                at = (8 * q + 2 * c) * 128
                left = jnp.concatenate(
                    [jnp.where(group == 2 * c, stack, 0.0), jnp.where(group == 2 * c + 1, stack, 0.0)], axis=1
                )
                acc = acc + dot(left.astype(BF16), pt[m, at : at + 256, :], NN)
            sums.append(jnp.where(lane < T, acc[0:8] + acc[8:16], acc[16:24] + acc[24:32]))
        packed = jnp.concatenate(sums, axis=0)
        place_m = place[m][:, 0:NB]
        out = sum(dot(place_m, part, NN) for part in split3(packed))
        lane = iota((Q, TL), 1)
        out = jnp.where(lane == T + N, total, jnp.where(lane == T + N + 1, count, out))
        ts[m] = out.reshape(O, SL, TL)
        fan(lambda o: ts.at[m, o], tr.at[sec, m, ob], t_send, t_recv.at[sec, m], hub)

    def scale_of(terms):
        row = iota((Q, TL), 0)
        sums = jnp.sum(jnp.where(row % SL == 0, terms, 0.0), axis=0, keepdims=True)
        return (sums[:, T + N + 1 : T + N + 2] + PRIOR_WEIGHT) / (sums[:, T + N : T + N + 1] + PRIOR_WEIGHT)

    def solve():
        H = NP // 8
        sub = iota((8, Q), 0)
        cols = []
        for k in range(N):
            at = k * N - k * (k - 1) // 2 - k
            cols.append([work[at + 8 * h : at + 8 * h + 8, :] for h in range(H)])
        right = [work[T + 8 * h : T + 8 * h + 8, :] for h in range(H)]
        scale = [jnp.ones((8, Q), F32) for _ in range(H)]
        pivot_now = jnp.broadcast_to(cols[0][0][0:1], (8, Q))
        for j in range(N):
            h, r = j // 8, j % 8
            col = cols[j]
            root = lax.rsqrt(pivot_now)
            inverse = root * root
            if j + 1 < N:
                kh, kr = (j + 1) // 8, (j + 1) % 8
                side = jnp.broadcast_to(col[kh][kr : kr + 1], (8, Q))
                pivot_now = jnp.broadcast_to(cols[j + 1][kh][kr : kr + 1], (8, Q)) - side * side * inverse
            factor = [v * inverse for v in col]
            factor[h] = jnp.where(sub == r, 0.0, factor[h])
            scale[h] = jnp.where(sub == r, inverse, scale[h])
            step = jnp.broadcast_to(right[h][r : r + 1], (8, Q))
            right = [right[i] - factor[i] * step for i in range(H)]
            for k in range(j + 1, N):
                kh, kr = k // 8, k % 8
                pivot = jnp.broadcast_to(col[kh][kr : kr + 1], (8, Q))
                for i in range(H):
                    if i >= kh or i < h or (i == h and r > 0):
                        cols[k][i] = cols[k][i] - factor[i] * pivot
                cols[k][h] = jnp.where(sub == r, pivot, cols[k][h])
        return jnp.concatenate([right[i] * scale[i] for i in range(H)], axis=0)

    def base_ready(par, m):
        after = jnp.minimum(2 * g + par + 1, S - 1)
        base[m] = sum(dot(hots[after, m], part, NT) for part in split3(betas[m]))

    def at_slots(w, m):
        return sum(dot(part, hots[w, m], NT) for part in split3(state[m]))

    def full_normal(w, m):
        terms = tr[w, m].reshape(Q, TL)
        return sum(dot(part, hots[w, m], TN) for part in split3(terms))[0:T] * scale_of(terms)

    def finish(m):
        got(state_in.at[m], h_recv.at[m, 0])
        iob[m] = state_in[m] + full_normal(hub, m)

    def hub_entry(par, m):
        w = 2 * g + par
        got(tr.at[w, m], t_recv.at[w, m])

        @pl.when(par == 0)
        def _():
            remote(tr.at[w, m], tr.at[w, m], s_send.at[w], f_recv.at[w, m], sec - 1, ob)

        for q in range(1, G):

            @pl.when(q > g)
            def _():
                remote(tr.at[w, m], tr.at[w, m], f_send.at[par, q], f_recv.at[w, m], 2 * q + 1, ob)

        @pl.when(par == 1)
        def _():
            got(held.at[1, m], h_recv.at[m, 1])

        terms = tr[w, m].reshape(Q, TL)
        parts = split3(terms)
        inverse = scale_of(terms)
        normal = sum(dot(part, match[par, m], TN) for part in parts) * inverse
        work[0:T, :] = held[par, m] + normal[0:T]
        work[T:TL, :] = normal[T:TL]
        filled = work[0:1, :] > 0.0
        delta = jnp.where((iota((NP, Q), 0) < N) & filled, solve(), 0.0)
        deltas = split3(delta)

        @pl.when(w + 1 < S)
        def _():
            slots = base[m] + sum(dot(follow[par, m], part, NT) for part in deltas)
            cs[par, m, :, :, 0:NP] = slots.reshape(O, SL, NP)
            fan(lambda o: cs.at[par, m, o], cr.at[m, ob], c_send.at[par], c_recv.at[m], w + 1)

        fresh = betas[m] + sum(dot(part, first[par, m], NN) for part in deltas)
        betas[m] = fresh

        @pl.when(par == 0)
        def _():
            beta_mid[m] = fresh
            remote(beta_mid.at[m], cob.at[m], o_send, o_recv.at[m], sec - 1, ob)
            base_ready(1, m)

        @pl.when(par == 1)
        def _():
            cob[m] = fresh

            @pl.when(g + 1 < G)
            def _():
                remote(cob.at[m], beta_in.at[m], b_send, b_recv.at[m], sec + 2, ob)

            @pl.when(g + 1 == G)
            def _():
                finish(m)

    def streams(body):
        lax.fori_loop(0, K, lambda m, c: (body(m), c)[1], 0)

    def begin():
        pi_in.wait()
        mf_in.wait()
        for m in range(K):
            state[m] = pi_v[:, m, :]
        low = ob * C
        prefix = jnp.where(iota((128, 128), 0) <= iota((128, 128), 1), 1.0, 0.0).astype(BF16)
        rank_of_row = (iota((Q, 128), 0) % SL + 1).astype(F32)
        lane = iota((Q, C), 1).astype(F32)
        for w in range(S):
            got(bcr.at[w * O : (w + 1) * O], bc_recv.at[w])
        owner_lane = iota((Q, 128), 1) // NB

        def window_hots(w):
            channel = jnp.concatenate([jnp.broadcast_to(bcr[w * O + o], (SL, 128)) for o in range(O)], axis=0)
            inside = (channel >= low) & (channel < low + C)
            for m in range(K):
                ours = inside & (owner_lane == m)
                rank = dot(jnp.where(ours, 1.0, 0.0).astype(BF16), prefix, NN)
                hit = ours & (rank == rank_of_row)
                value = jnp.sum(jnp.where(hit, (channel - low + 1).astype(F32), 0.0), axis=1, keepdims=True)
                hots[w, m] = jnp.where(lane == value - 1.0, 1.0, 0.0).astype(BF16)

        each(0, S, window_hots)

    def links():
        earlier_slot = iota((Q, Q), 1) < iota((Q, Q), 0)
        for m in range(K):
            for par in range(2):
                w = 2 * g + par
                hot = hots[w, m]
                same = dot(hot, hot, NT)
                match[par, m] = same.astype(BF16)
                copies = jnp.sum(jnp.where(earlier_slot, same, 0.0), axis=1, keepdims=True)
                lead = jnp.where(copies == 0.0, hot.astype(F32), 0.0).astype(BF16)
                first[par, m] = lead
                after = jnp.minimum(w + 1, S - 1)
                follow[par, m] = dot(hots[after, m], lead, NT).astype(BF16)

    def catch_up():
        def one(w, m):
            got(tr.at[w, m], f_recv.at[w, m])

            @pl.when(odd)
            def _():
                remote(tr.at[w, m], tr.at[w, m], s_send.at[w], f_recv.at[w, m], sec - 1, ob)

            state[m] = (state[m] + full_normal(w, m)) * mf_v[...]

        lax.fori_loop(0, 2 * g, lambda w, c: (streams(lambda m: one(w, m)), c)[1], 0)

    def first_ready():
        def take(m):
            got(beta_in.at[m], b_recv.at[m])
            betas[m] = beta_in[m]

        @pl.when(g > 0)
        def _():
            streams(take)

        def one(m):
            base_ready(0, m)
            held[0, m] = at_slots(2 * g, m)

        streams(one)

    @pl.when(odd | (g > 0))
    def _():
        begin()

    @pl.when(odd)
    def _():
        links()
        catch_up()
        first_ready()

    def turn(par):
        @pl.when(par == core)
        def _():
            streams(row_entry)

        @pl.when(odd)
        def _():
            streams(lambda m: hub_entry(par, m))

    lax.fori_loop(0, 2, lambda par, c: (turn(par), c)[1], 0)

    @pl.when(odd & (g + 1 < G))
    def _():
        streams(finish)

    @pl.when(jnp.logical_not(odd))
    def _():
        @pl.when(g == 0)
        def _():
            begin()

        catch_up()

        def update(m):
            got(tr.at[2 * g, m], f_recv.at[2 * g, m])
            post = state[m] + full_normal(2 * g, m)
            iob[m] = post
            state[m] = post * mf_v[...]
            remote(state.at[m], state_in.at[m], h_send.at[0], h_recv.at[m, 0], sec + 1, ob)
            held[1, m] = at_slots(2 * g + 1, m)
            remote(held.at[1, m], held.at[1, m], h_send.at[1], h_recv.at[m, 1], sec + 1, ob)

        streams(update)
        streams(lambda m: got(cob.at[m], o_recv.at[m]))

    order_in.wait()
    for k in range(K):
        m = order_s[k]
        io_out[:, k, :] = iob[m]
        co_out[:, k, :] = cob[m, 0:N, :]

    got(bcr.at[0 : S * O - 1], bc_send)
    fanned(ts, t_send, hub)

    @pl.when(odd)
    def _():
        got(pcr.at[:, 0 : O // G], p_send)
        fanned(cr, c_send.at[0], hub)
        got(beta_mid, o_send)
        lax.fori_loop(0, 2 * g + 1, lambda w, c: (got(tr.at[0], s_send.at[w]), c)[1], 0)

        @pl.when(g + 1 < G)
        def _():
            fanned(cr, c_send.at[1], hub + 1)
            got(cob, b_send)

        for q in range(1, G):

            @pl.when(q > g)
            def _():
                got(tr.at[0], f_send.at[0, q])
                got(tr.at[0], f_send.at[1, q])

    @pl.when(jnp.logical_not(odd))
    def _():
        got(state, h_send.at[0])
        got(held.at[1], h_send.at[1])


def local(
    predictors,
    departures,
    obs_precision,
    qc_pass,
    block_channel,
    stream_order,
    prior_coeffs,
    prior_info,
    memory_factor,
):
    S, O = lax.axis_size("section"), lax.axis_size("obs")
    K, N, C = prior_coeffs.shape
    T = prior_info.shape[1]
    NB = block_channel.shape[2]
    R = predictors.shape[3]
    width = R // NB
    assert width == 128 and S % 2 == 0 and O % (S // 2) == 0 and K * NB <= 128 and NB % 8 == 0
    NP = round_up(N + 1, 8)
    SL = round_up(max(2 * NB // O, 1), 8)
    TL = round_up(T + NP + 2, 128)
    G, Q = S // 2, O * SL
    pairs = [(i, j) for i in range(N) for j in range(i, N)]
    expand = np.zeros((NP, 2 * TL), np.float32)
    for t, (i, j) in enumerate(pairs):
        expand[i, t] = 1.0
        expand[j, TL + t] = 1.0
    for i in range(N):
        expand[i, T + i] = 1.0
        expand[N, TL + T + i] = 1.0
    cfg = (S, O, K, N, NP, T, C, NB, SL, TL)

    def by_block(array):
        return array[0].reshape(K, NB, width).transpose(1, 0, 2).reshape(NB * K, width)

    vm = pl.BlockSpec(memory_space=pltpu.VMEM)
    hbm = pl.BlockSpec(memory_space=pltpu.HBM)
    dma = pltpu.SemaphoreType.DMA
    coeffs, info = pl.pallas_call(
        functools.partial(kernel, cfg),
        out_shape=(
            jax.ShapeDtypeStruct((N, K, C), F32),
            jax.ShapeDtypeStruct((T, K, C), F32),
        ),
        in_specs=[hbm] * 10,
        out_specs=(vm, vm),
        scratch_shapes=[
            pltpu.SMEM((K,), jnp.int32),
            pltpu.VMEM((N, K, R), BF16),
            pltpu.VMEM((NB * K, 128), F32),
            pltpu.VMEM((NB * K, 128), F32),
            pltpu.VMEM((NB * K, 128), jnp.int32),
            pltpu.VMEM((K, NB), jnp.int32),
            pltpu.VMEM((N, K, C), F32),
            pltpu.VMEM((T, K, C), F32),
            pltpu.VMEM((1, C), F32),
            pltpu.VMEM((NP, 2 * TL), BF16),
            pltpu.VMEM((1, 128), jnp.int32),
            pltpu.VMEM((S * O, 1, 128), jnp.int32),
            pltpu.VMEM((K, NP, C), F32),
            pltpu.VMEM((K, O, NP, C), F32),
            pltpu.VMEM((2, K, O, SL, 128), F32),
            pltpu.VMEM((K, O, SL, 128), F32),
            pltpu.VMEM((K, O, SL, TL), F32),
            pltpu.VMEM((S, K, O, SL, TL), F32),
            pltpu.VMEM((NB, NP * K, 128), F32),
            pltpu.VMEM((K, NP, R), BF16),
            pltpu.VMEM((K, R, TL), BF16),
            pltpu.VMEM((K, NB, 128), F32),
            pltpu.VMEM((K, Q, 128), BF16),
            pltpu.VMEM((K, NB, Q), BF16),
            pltpu.VMEM((NB, NP), F32),
            pltpu.VMEM((S, K, Q, C), BF16),
            pltpu.VMEM((K, T, C), F32),
            pltpu.VMEM((K, NP, C), F32),
            pltpu.VMEM((K, NP, C), F32),
            pltpu.VMEM((K, NP, C), F32),
            pltpu.VMEM((K, T, C), F32),
            pltpu.VMEM((K, Q, NP), F32),
            pltpu.VMEM((2, K, T, Q), F32),
            pltpu.VMEM((2, K, Q, Q), BF16),
            pltpu.VMEM((2, K, Q, C), BF16),
            pltpu.VMEM((2, K, Q, Q), BF16),
            pltpu.VMEM((TL, Q), F32),
            pltpu.VMEM((K, NP, C), F32),
            pltpu.VMEM((K, T, C), F32),
            dma((10,)),
            dma,
            dma((S,)),
            dma,
            dma((K,)),
            dma((2,)),
            dma((K,)),
            dma,
            dma((S, K)),
            dma((2, G)),
            dma((S, K)),
            dma,
            dma((K,)),
            dma((S,)),
            dma((2,)),
            dma((K, 2)),
            dma,
            dma((K,)),
        ],
        compiler_params=pltpu.CompilerParams(
            has_side_effects=True, collective_id=0, vmem_limit_bytes=48 * 1024 * 1024
        ),
    )(*(pltpu.with_memory_space_constraint(a, pltpu.HBM) for a in (
        stream_order,
        predictors[0].transpose(1, 0, 2),
        by_block(departures),
        by_block(obs_precision),
        by_block(qc_pass),
        block_channel[0],
        prior_coeffs.transpose(1, 0, 2),
        prior_info.transpose(1, 0, 2),
        memory_factor[None],
        jnp.asarray(expand, BF16),
    )))
    return coeffs.transpose(1, 0, 2)[None], info.transpose(1, 0, 2)[None]


def solution(mesh):
    in_specs = (
        P("section", None, None, "obs"),
        P("section", None, "obs"),
        P("section", None, "obs"),
        P("section", None, "obs"),
        P("section", None, "obs"),
        P(),
        P(None, None, "obs"),
        P(None, None, "obs"),
        P("obs"),
    )
    out_specs = (P("section", None, None, "obs"), P("section", None, None, "obs"))
    return jax.shard_map(local, mesh=mesh, in_specs=in_specs, out_specs=out_specs, check_vma=False)
```

```python
import functools

import jax
import jax.numpy as jnp
import numpy as np
from jax import lax
from jax.experimental import pallas as pl
from jax.experimental.pallas import tpu as pltpu
from jax.sharding import PartitionSpec as P

HUBER_SQ = 9.0
PRIOR_WEIGHT = 64.0
F32 = jnp.float32
BF16 = jnp.bfloat16
NN = (((1,), (0,)), ((), ()))
NT = (((1,), (1,)), ((), ()))
TN = (((0,), (0,)), ((), ()))


def round_up(n, m):
    return -(-n // m) * m


def split3(x):
    hi = x.astype(BF16)
    rest = x - hi.astype(F32)
    mid = rest.astype(BF16)
    low = (rest - mid.astype(F32)).astype(BF16)
    return hi, mid, low


def dot(a, b, dims):
    return lax.dot_general(a, b, dims, preferred_element_type=F32)


def each(low, high, body):
    n = high - low

    def step(i, _):
        body(i)
        return 0

    lax.fori_loop(low, high, step, 0, unroll=n if n <= 8 else 1)


def iota(shape, axis):
    return lax.broadcasted_iota(jnp.int32, shape, axis)


def kernel(
    cfg,
    order_hbm,
    x_hbm,
    dep_hbm,
    prec_hbm,
    qc_hbm,
    bc_hbm,
    pc_hbm,
    pi_hbm,
    mf_hbm,
    ee_hbm,
    co_out,
    io_out,
    order_s,
    x_v,
    dep_v,
    prec_v,
    qc_v,
    bc_v,
    pc_v,
    pi_v,
    mf_v,
    ee_v,
    lists,
    bcr,
    pcs,
    pcr,
    cs,
    cr,
    ts,
    tr,
    xs,
    xh,
    pt,
    chcol,
    slots_v,
    slots_s,
    came,
    coef_v,
    hots,
    state,
    betas,
    beta_in,
    betas_out,
    state_in,
    base,
    held,
    match,
    first,
    follow,
    work,
    cob,
    iob,
    load_sem,
    slot_sem,
    bc_send,
    bc_recv,
    p_send,
    p_recv,
    c_send,
    c_recv,
    t_send,
    t_recv,
    f_send,
    f_recv,
    b_send,
    b_recv,
    s_send,
    h_send,
    h_recv,
    o_send,
    o_recv,
):
    S, O, K, N, NP, T, C, NB, SL, TL = cfg
    G = S // 2
    Q = O * SL
    sec = lax.axis_index("section")
    ob = lax.axis_index("obs")
    core = lax.rem(sec, 2)
    odd = core == 1
    g = sec // 2
    hub = 2 * g + 1

    def remote(src, dst, send_sem, recv_sem, s, o):
        pltpu.make_async_remote_copy(
            src_ref=src,
            dst_ref=dst,
            send_sem=send_sem,
            recv_sem=recv_sem,
            device_id={"section": s, "obs": o},
            device_id_type=pl.DeviceIdType.MESH,
        ).start()

    def got(ref, sem):
        pltpu.make_async_copy(ref, ref, sem).wait()

    def partner(j):
        if O & (O - 1):
            return lax.rem(ob + j, O)
        o = ob
        for bit in range(O.bit_length() - 1):
            if j >> bit & 1:
                step = 1 << bit
                o = o + step - 2 * step * lax.rem(ob // step, 2)
        return o

    def fan(src, dst, send_sem, recv_sem, s):
        for j in range(1, O):
            o = partner(O - j)
            remote(src(o), dst, send_sem, recv_sem, s, o)

        @pl.when(s != sec)
        def _():
            remote(src(ob), dst, send_sem, recv_sem, s, ob)

        @pl.when(s == sec)
        def _():
            pltpu.make_async_copy(src(ob), dst, recv_sem).start()

    def fanned(like, send_sem, s):
        @pl.when(s != sec)
        def _():
            got(like, send_sem)

        @pl.when(s == sec)
        def _():
            got(like.at[:, 0 : like.shape[1] // O * (O - 1)], send_sem)

    loads = [
        (order_hbm, order_s),
        (bc_hbm, bc_v),
        (pc_hbm, pc_v),
        (x_hbm, x_v),
        (ee_hbm, ee_v),
        (dep_hbm, dep_v),
        (prec_hbm, prec_v),
        (qc_hbm, qc_v),
        (mf_hbm, mf_v),
        (pi_hbm, pi_v),
    ]
    loads = [pltpu.make_async_copy(a, b, load_sem.at[i]) for i, (a, b) in enumerate(loads)]
    for copy in loads:
        copy.start()
    order_in, bc_in, pc_in, x_in, ee_in, dep_in, prec_in, qc_in, mf_in, pi_in = loads

    barrier = pltpu.get_barrier_semaphore()

    def greet(s):
        def one(o):
            @pl.when(jnp.logical_not((s == sec) & (o == ob)))
            def _():
                pl.semaphore_signal(
                    barrier,
                    inc=1,
                    device_id={"section": s, "obs": o},
                    device_id_type=pl.DeviceIdType.MESH,
                )

        each(0, O, one)

    lax.fori_loop(0, S, lambda s, c: (greet(s), c)[1], 0)

    bc_in.wait()
    line = [bc_v[m : m + 1, :] for m in range(K)]
    if K * NB < 128:
        line.append(jnp.full((1, 128 - K * NB), -1, jnp.int32))
    lists[...] = jnp.concatenate(line, axis=1)
    pc_in.wait()
    for m in range(K):
        pcs[m] = jnp.zeros((NP, C), F32)
        pcs[m, 0:N, :] = pc_v[:, m, :]
        betas[m] = pcs[m]
    def unpack():
        x_in.wait()
        ee_in.wait()
        for b in range(NB):
            for i in range(N):
                xs[b, i * K : (i + 1) * K, :] = x_v[i, :, b * 128 : (b + 1) * 128].astype(F32)
            xs[b, N * K : (N + 1) * K, :] = jnp.ones((K, 128), F32)
            xs[b, (N + 1) * K :, :] = jnp.zeros(((NP - N - 1) * K, 128), F32)

    def products(low, high):
        def one(b):
            lanes = pl.ds(pl.multiple_of(b * 128, 128), 128)
            for m in range(low, high):
                xb = xs[b, pl.ds(m, NP, stride=K), :].astype(BF16)
                xh[m, b] = xb
                both = dot(xb, ee_v[...], TN)
                product = (both[:, 0:TL] * both[:, TL:]).astype(BF16)
                for h in range(TL // 128):
                    pt[m, h, lanes, :] = product[:, 128 * h : 128 * h + 128]

        lax.fori_loop(0, NB, lambda b, c: (one(b), c)[1], 0, unroll=8)

    unpack()

    @pl.when(odd)
    def _():
        products(0, 1)

    @pl.when(jnp.logical_not(odd))
    def _():
        products(0, K // 2)

    pl.semaphore_wait(barrier, S * O - 1)

    def send_lists(s):
        fan(lambda o: lists, bcr.at[sec * O + ob], bc_send, bc_recv.at[sec], s)

    lax.fori_loop(0, S, lambda s, c: (send_lists(s), c)[1], 0)

    def send_prior(m):
        def one(i):
            o = lax.rem(m + g, G) + G * i
            remote(pcs.at[m], pcr.at[m, ob], p_send, p_recv.at[m], 0, o)

        each(0, O // G, one)

    @pl.when(odd)
    def _():
        lax.fori_loop(0, K, lambda m, c: (send_prior(m), c)[1], 0)

    cs[...] = jnp.zeros_like(cs)
    coef_v[...] = jnp.zeros_like(coef_v)
    came[...] = jnp.zeros_like(came)

    eye = iota((128, 128), 0) == iota((128, 128), 1)
    upto = iota((128, 128), 0) <= iota((128, 128), 1)
    for m in range(K):
        row = bc_v[m : m + 1, :].astype(F32)
        if NB < 128:
            row = jnp.concatenate([row, jnp.full((1, 128 - NB), -1.0, F32)], axis=1)
        row = jnp.broadcast_to(row, (128, 128))
        col = jnp.sum(jnp.where(eye, row, 0.0), axis=1, keepdims=True)
        range_row = jnp.floor((row + 0.5) * (1.0 / C))
        range_col = jnp.floor((col + 0.5) * (1.0 / C))
        same = range_row == range_col
        rank_row = jnp.sum(jnp.where(same & upto, 1.0, 0.0), axis=0, keepdims=True)
        chcol[m] = jnp.broadcast_to(col[0:NB], (NB, 128))
        slots_v[m : m + 1, :] = jnp.clip((range_row[0:1] * float(SL) + rank_row - 1.0).astype(jnp.int32), 0, Q - 1)
    to_scalars = pltpu.make_async_copy(slots_v, slots_s, slot_sem)
    to_scalars.start()

    @pl.when(odd)
    def _():
        products(1, K)

    @pl.when(jnp.logical_not(odd))
    def _():
        products(K // 2, K)

    dep_in.wait()
    prec_in.wait()
    qc_in.wait()
    to_scalars.wait()

    def split_f32(x):
        return [p.astype(F32) for p in split3(x)]

    def row_entry(m):
        @pl.when(sec == 0)
        def _():
            got(pcr.at[m], p_recv.at[m])
            channel = chcol[m]
            coef = jnp.zeros((NB, N), F32)
            lane = iota((NB, C), 1).astype(F32)
            for o in range(O):
                wide = jnp.broadcast_to(channel[:, 0:1], (NB, C)) - float(o * C)
                hot = jnp.where(lane == wide, 1.0, 0.0).astype(BF16)
                for part in split3(pcr[m, o, 0:N, :]):
                    coef = coef + dot(hot, part, NT)
            coef_v[:, 0:N] = coef

        @pl.when(sec != 0)
        def _():
            got(cr.at[m], c_recv.at[m])
            came[0:Q, :] = cr[m]
            sub = iota((8, 128), 0)
            for q in range(NB // 8):
                tile = jnp.zeros((8, 128), F32)
                for r in range(8):
                    row = jnp.broadcast_to(came[pl.ds(jnp.clip(slots_s[m, 8 * q + r], 0, Q - 1), 1), :], (8, 128))
                    tile = jnp.where(sub == r, row, tile)
                coef_v[8 * q : 8 * q + 8, :] = tile[:, 0:NP]

        pieces = split_f32(coef_v[...])
        sub = iota((8, 128), 0)
        tiles = []
        for q in range(NB // 8):
            stack = jnp.concatenate([p[8 * q : 8 * q + 8] for p in pieces], axis=0).astype(BF16)
            tile = jnp.zeros((8, 128), F32)
            for c in range(4):
                at = (8 * q + 2 * c) * 128
                pair = jnp.concatenate([xh[m, at // 128], xh[m, at // 128 + 1]], axis=1)
                full = dot(stack, pair, NN)
                full = full[0:8] + full[8:16] + full[16:24]
                tile = jnp.where(sub == 2 * c, full[:, 0:128], tile)
                tile = jnp.where(sub == 2 * c + 1, full[:, 128:256], tile)
            tiles.append(tile)
        offset = jnp.concatenate(tiles, axis=0)
        rows = pl.ds(m, NB, stride=K)
        residual = dep_v[rows, :] - offset
        precision = prec_v[rows, :]
        passed = qc_v[rows, :].astype(F32)
        weight = passed * precision / (1.0 + precision * residual * residual / HUBER_SQ)
        pull = weight * residual
        total = jnp.sum(jnp.sum(pull * residual, axis=0, keepdims=True), axis=1, keepdims=True)
        count = jnp.sum(jnp.sum(passed, axis=0, keepdims=True), axis=1, keepdims=True)
        slot = iota((Q, 128), 0)
        acc = jnp.zeros((2 * Q, TL), F32)
        for c in range(NB // 2):
            sides = []
            for b in (2 * c, 2 * c + 1):
                hit = slot == slots_s[m, b]
                sides.append(
                    jnp.concatenate(
                        [jnp.where(hit, jnp.broadcast_to(v[b : b + 1], (Q, 128)), 0.0) for v in (weight, pull)], axis=0
                    )
                )
            left = jnp.concatenate(sides, axis=1).astype(BF16)
            right = jnp.concatenate([pt[m, h, 256 * c : 256 * c + 256, :] for h in range(TL // 128)], axis=1)
            acc = acc + dot(left, right, NN)
        out = jnp.where(iota((Q, TL), 1) < T, acc[0:Q], acc[Q:])
        lane = iota((Q, TL), 1)
        out = jnp.where(lane == T + N, total, jnp.where(lane == T + N + 1, count, out))
        ts[m] = out.reshape(O, SL, TL)
        fan(lambda o: ts.at[m, o], tr.at[sec, m, ob], t_send, t_recv.at[sec, m], hub)

    def scale_of(terms):
        row = iota((Q, TL), 0)
        sums = jnp.sum(jnp.where(row % SL == 0, terms, 0.0), axis=0, keepdims=True)
        return (sums[:, T + N + 1 : T + N + 2] + PRIOR_WEIGHT) / (sums[:, T + N : T + N + 1] + PRIOR_WEIGHT)

    def solve():
        H = NP // 8
        sub = iota((8, Q), 0)
        cols = []
        for k in range(N):
            at = k * N - k * (k - 1) // 2 - k
            cols.append([work[at + 8 * h : at + 8 * h + 8, :] for h in range(H)])
        right = [work[T + 8 * h : T + 8 * h + 8, :] for h in range(H)]
        scale = [jnp.ones((8, Q), F32) for _ in range(H)]
        pivot_now = jnp.broadcast_to(cols[0][0][0:1], (8, Q))
        for j in range(N):
            h, r = j // 8, j % 8
            col = cols[j]
            root = lax.rsqrt(pivot_now)
            inverse = root * root
            if j + 1 < N:
                kh, kr = (j + 1) // 8, (j + 1) % 8
                side = jnp.broadcast_to(col[kh][kr : kr + 1], (8, Q))
                pivot_now = jnp.broadcast_to(cols[j + 1][kh][kr : kr + 1], (8, Q)) - side * side * inverse
            factor = [v * inverse for v in col]
            factor[h] = jnp.where(sub == r, 0.0, factor[h])
            scale[h] = jnp.where(sub == r, inverse, scale[h])
            step = jnp.broadcast_to(right[h][r : r + 1], (8, Q))
            right = [right[i] - factor[i] * step for i in range(H)]
            for k in range(j + 1, N):
                kh, kr = k // 8, k % 8
                pivot = jnp.broadcast_to(col[kh][kr : kr + 1], (8, Q))
                for i in range(H):
                    if i >= kh or i < h or (i == h and r > 0):
                        cols[k][i] = cols[k][i] - factor[i] * pivot
                cols[k][h] = jnp.where(sub == r, pivot, cols[k][h])
        return jnp.concatenate([right[i] * scale[i] for i in range(H)], axis=0)

    def base_ready(m):
        for par in range(2):
            after = jnp.minimum(2 * g + par + 1, S - 1)
            base[par, m] = sum(dot(hots[after, m], part, NT) for part in split3(betas[m]))

    def at_slots(w, m):
        return sum(dot(part, hots[w, m], NT) for part in split3(state[m]))

    def full_normal(w, m):
        terms = tr[w, m].reshape(Q, TL)
        return sum(dot(part, hots[w, m], TN) for part in split3(terms))[0:T] * scale_of(terms)

    def finish(m):
        got(state_in.at[m], h_recv.at[m, 0])
        iob[m] = state_in[m] + full_normal(hub, m)

    def change(par, m):
        w = 2 * g + par
        terms = tr[w, m].reshape(Q, TL)
        normal = sum(dot(part, match[par, m], TN) for part in split3(terms)) * scale_of(terms)
        work[0:T, :] = held[par, m] + normal[0:T]
        work[T:TL, :] = normal[T:TL]
        filled = work[0:1, :] > 0.0
        return split3(jnp.where((iota((NP, Q), 0) < N) & filled, solve(), 0.0))

    def hub_entry(par, m):
        w = 2 * g + par
        got(tr.at[w, m], t_recv.at[w, m])

        @pl.when(par == 0)
        def _():
            remote(tr.at[w, m], tr.at[w, m], s_send.at[w], f_recv.at[w, m], sec - 1, ob)

        for q in range(1, G):

            @pl.when(q > g)
            def _():
                remote(tr.at[w, m], tr.at[w, m], f_send.at[par, q], f_recv.at[w, m], 2 * q + 1, ob)

        @pl.when(par == 1)
        def _():
            got(held.at[1, m], h_recv.at[m, 1])

        @pl.when(w + 1 < S)
        def _():
            deltas = change(par, m)
            slots = base[par, m] + sum(dot(follow[par, m], part, NT) for part in deltas)
            later = base[1, m] + sum(dot(follow[2, m], part, NT) for part in deltas)
            fresh = betas[m] + sum(dot(part, first[par, m], NN) for part in deltas)
            cs[par, m, :, :, 0:NP] = slots.reshape(O, SL, NP)
            base[1, m] = later
            betas[m] = fresh
            betas_out[par, m] = fresh
            fan(lambda o: cs.at[par, m, o], cr.at[m, pl.ds(pl.multiple_of(ob * SL, SL), SL)], c_send.at[par], c_recv.at[m], w + 1)

            @pl.when(par == 0)
            def _():
                remote(betas_out.at[0, m], cob.at[m], o_send, o_recv.at[m], sec - 1, ob)

            @pl.when(par == 1)
            def _():
                cob[m] = betas_out[1, m]
                remote(betas_out.at[1, m], beta_in.at[m], b_send, b_recv.at[m], sec + 2, ob)

        @pl.when(w + 1 == S)
        def _():
            got(state_in.at[m], h_recv.at[m, 0])
            iob[m] = state_in[m] + full_normal(hub, m)
            cob[m] = betas[m] + sum(dot(part, first[par, m], NN) for part in change(par, m))

    def streams(body):
        lax.fori_loop(0, K, lambda m, c: (body(m), c)[1], 0)

    def begin():
        pi_in.wait()
        mf_in.wait()
        for m in range(K):
            state[m] = pi_v[:, m, :]
        low = ob * C
        prefix = jnp.where(iota((128, 128), 0) <= iota((128, 128), 1), 1.0, 0.0).astype(BF16)
        rank_of_row = (iota((Q, 128), 0) % SL + 1).astype(F32)
        lane = iota((Q, C), 1).astype(F32)
        for w in range(S):
            got(bcr.at[w * O : (w + 1) * O], bc_recv.at[w])
        owner_lane = iota((Q, 128), 1) // NB

        def window_hots(w):
            channel = jnp.concatenate([jnp.broadcast_to(bcr[w * O + o], (SL, 128)) for o in range(O)], axis=0)
            inside = (channel >= low) & (channel < low + C)
            for m in range(K):
                ours = inside & (owner_lane == m)
                rank = dot(jnp.where(ours, 1.0, 0.0).astype(BF16), prefix, NN)
                hit = ours & (rank == rank_of_row)
                value = jnp.sum(jnp.where(hit, (channel - low + 1).astype(F32), 0.0), axis=1, keepdims=True)
                hots[w, m] = jnp.where(lane == value - 1.0, 1.0, 0.0).astype(BF16)

        each(0, S, window_hots)

    def links():
        earlier_slot = iota((Q, Q), 1) < iota((Q, Q), 0)
        for m in range(K):
            for par in range(2):
                hot = hots[2 * g + par, m]
                same = dot(hot, hot, NT)
                match[par, m] = same.astype(BF16)
                copies = jnp.sum(jnp.where(earlier_slot, same, 0.0), axis=1, keepdims=True)
                first[par, m] = jnp.where(copies == 0.0, hot.astype(F32), 0.0).astype(BF16)
        after = jnp.minimum(2 * g + 2, S - 1)
        for m in range(K):
            follow[0, m] = dot(hots[2 * g + 1, m], first[0, m], NT).astype(BF16)
            follow[1, m] = dot(hots[after, m], first[1, m], NT).astype(BF16)
            follow[2, m] = dot(hots[after, m], first[0, m], NT).astype(BF16)

    def catch_up_one(w, m):
        got(tr.at[w, m], f_recv.at[w, m])

        @pl.when(odd)
        def _():
            remote(tr.at[w, m], tr.at[w, m], s_send.at[w], f_recv.at[w, m], sec - 1, ob)

        state[m] = (state[m] + full_normal(w, m)) * mf_v[...]

    def catch_up(windows):
        lax.fori_loop(0, windows, lambda w, c: (streams(lambda m: catch_up_one(w, m)), c)[1], 0)

    def first_ready():
        @pl.when(g == 0)
        def _():
            for m in range(K):
                base_ready(m)
                held[0, m] = at_slots(2 * g, m)

        def one(i):
            @pl.when(i < K)
            def _():
                m = jnp.minimum(i, K - 1)
                catch_up_one(2 * g - 1, m)
                held[0, m] = at_slots(2 * g, m)

            @pl.when(i >= 2)
            def _():
                m = jnp.maximum(i - 2, 0)
                got(beta_in.at[m], b_recv.at[m])
                betas[m] = beta_in[m]
                base_ready(m)

        @pl.when(g > 0)
        def _():
            lax.fori_loop(0, K + 2, lambda i, c: (one(i), c)[1], 0)

    @pl.when(odd | (g > 0))
    def _():
        begin()

    @pl.when(odd)
    def _():
        links()
        catch_up(2 * g - 1)
        first_ready()
        got(pcr.at[:, 0 : O // G], p_send)
        lax.fori_loop(0, 2 * g, lambda w, c: (got(tr.at[0], s_send.at[w]), c)[1], 0)

    def turn(par):
        @pl.when(par == core)
        def _():
            streams(row_entry)

        @pl.when(odd)
        def _():
            streams(lambda m: hub_entry(par, m))

    got(bcr.at[0 : S * O - 1], bc_send)
    lax.fori_loop(0, 2, lambda par, c: (turn(par), c)[1], 0)

    @pl.when(odd & (g + 1 < G))
    def _():
        streams(finish)

    @pl.when(jnp.logical_not(odd))
    def _():
        @pl.when(g == 0)
        def _():
            begin()

        catch_up(2 * g)

        def update(m):
            got(tr.at[2 * g, m], f_recv.at[2 * g, m])
            post = state[m] + full_normal(2 * g, m)
            iob[m] = post
            state[m] = post * mf_v[...]
            remote(state.at[m], state_in.at[m], h_send.at[0], h_recv.at[m, 0], sec + 1, ob)
            held[1, m] = at_slots(2 * g + 1, m)
            remote(held.at[1, m], held.at[1, m], h_send.at[1], h_recv.at[m, 1], sec + 1, ob)

        streams(update)
        streams(lambda m: got(cob.at[m], o_recv.at[m]))

    order_in.wait()
    for k in range(K):
        m = order_s[k]
        io_out[:, k, :] = iob[m]
        co_out[:, k, :] = cob[m, 0:N, :]

    fanned(ts, t_send, hub)

    @pl.when(odd)
    def _():
        fanned(cr, c_send.at[0], hub)
        got(betas_out.at[0], o_send)
        got(tr.at[0], s_send.at[2 * g])

        @pl.when(g + 1 < G)
        def _():
            fanned(cr, c_send.at[1], hub + 1)
            got(betas_out.at[1], b_send)

        for q in range(1, G):

            @pl.when(q > g)
            def _():
                got(tr.at[0], f_send.at[0, q])
                got(tr.at[0], f_send.at[1, q])

    @pl.when(jnp.logical_not(odd))
    def _():
        got(state, h_send.at[0])
        got(held.at[1], h_send.at[1])


def local(
    predictors,
    departures,
    obs_precision,
    qc_pass,
    block_channel,
    stream_order,
    prior_coeffs,
    prior_info,
    memory_factor,
):
    S, O = lax.axis_size("section"), lax.axis_size("obs")
    K, N, C = prior_coeffs.shape
    T = prior_info.shape[1]
    NB = block_channel.shape[2]
    R = predictors.shape[3]
    width = R // NB
    assert width == 128 and S % 2 == 0 and O % (S // 2) == 0 and K * NB <= 128 and NB % 8 == 0
    NP = round_up(N + 1, 8)
    SL = round_up(max(2 * NB // O, 1), 8)
    TL = round_up(T + NP + 2, 128)
    G, Q = S // 2, O * SL
    pairs = [(i, j) for i in range(N) for j in range(i, N)]
    expand = np.zeros((NP, 2 * TL), np.float32)
    for t, (i, j) in enumerate(pairs):
        expand[i, t] = 1.0
        expand[j, TL + t] = 1.0
    for i in range(N):
        expand[i, T + i] = 1.0
        expand[N, TL + T + i] = 1.0
    cfg = (S, O, K, N, NP, T, C, NB, SL, TL)

    def by_block(array):
        return array[0].reshape(K, NB, width).transpose(1, 0, 2).reshape(NB * K, width)

    vm = pl.BlockSpec(memory_space=pltpu.VMEM)
    hbm = pl.BlockSpec(memory_space=pltpu.HBM)
    dma = pltpu.SemaphoreType.DMA
    coeffs, info = pl.pallas_call(
        functools.partial(kernel, cfg),
        out_shape=(
            jax.ShapeDtypeStruct((N, K, C), F32),
            jax.ShapeDtypeStruct((T, K, C), F32),
        ),
        in_specs=[hbm] * 10,
        out_specs=(vm, vm),
        scratch_shapes=[
            pltpu.SMEM((K,), jnp.int32),
            pltpu.VMEM((N, K, R), BF16),
            pltpu.VMEM((NB * K, 128), F32),
            pltpu.VMEM((NB * K, 128), F32),
            pltpu.VMEM((NB * K, 128), jnp.int32),
            pltpu.VMEM((K, NB), jnp.int32),
            pltpu.VMEM((N, K, C), F32),
            pltpu.VMEM((T, K, C), F32),
            pltpu.VMEM((1, C), F32),
            pltpu.VMEM((NP, 2 * TL), BF16),
            pltpu.VMEM((1, 128), jnp.int32),
            pltpu.VMEM((S * O, 1, 128), jnp.int32),
            pltpu.VMEM((K, NP, C), F32),
            pltpu.VMEM((K, O, NP, C), F32),
            pltpu.VMEM((2, K, O, SL, 128), F32),
            pltpu.VMEM((K, Q, 128), F32),
            pltpu.VMEM((K, O, SL, TL), F32),
            pltpu.VMEM((S, K, O, SL, TL), F32),
            pltpu.VMEM((NB, NP * K, 128), F32),
            pltpu.VMEM((K, NB, NP, 128), BF16),
            pltpu.VMEM((K, TL // 128, R, 128), BF16),
            pltpu.VMEM((K, NB, 128), F32),
            pltpu.VMEM((K, 128), jnp.int32),
            pltpu.SMEM((K, 128), jnp.int32),
            pltpu.VMEM((Q + 8, 128), F32),
            pltpu.VMEM((NB, NP), F32),
            pltpu.VMEM((S, K, Q, C), BF16),
            pltpu.VMEM((K, T, C), F32),
            pltpu.VMEM((K, NP, C), F32),
            pltpu.VMEM((K, NP, C), F32),
            pltpu.VMEM((2, K, NP, C), F32),
            pltpu.VMEM((K, T, C), F32),
            pltpu.VMEM((2, K, Q, NP), F32),
            pltpu.VMEM((2, K, T, Q), F32),
            pltpu.VMEM((2, K, Q, Q), BF16),
            pltpu.VMEM((2, K, Q, C), BF16),
            pltpu.VMEM((3, K, Q, Q), BF16),
            pltpu.VMEM((TL, Q), F32),
            pltpu.VMEM((K, NP, C), F32),
            pltpu.VMEM((K, T, C), F32),
            dma((10,)),
            dma,
            dma,
            dma((S,)),
            dma,
            dma((K,)),
            dma((2,)),
            dma((K,)),
            dma,
            dma((S, K)),
            dma((2, G)),
            dma((S, K)),
            dma,
            dma((K,)),
            dma((S,)),
            dma((2,)),
            dma((K, 2)),
            dma,
            dma((K,)),
        ],
        compiler_params=pltpu.CompilerParams(
            has_side_effects=True, collective_id=0, vmem_limit_bytes=48 * 1024 * 1024
        ),
    )(*(pltpu.with_memory_space_constraint(a, pltpu.HBM) for a in (
        stream_order,
        predictors[0].transpose(1, 0, 2),
        by_block(departures),
        by_block(obs_precision),
        by_block(qc_pass),
        block_channel[0],
        prior_coeffs.transpose(1, 0, 2),
        prior_info.transpose(1, 0, 2),
        memory_factor[None],
        jnp.asarray(expand, BF16),
    )))
    return coeffs.transpose(1, 0, 2)[None], info.transpose(1, 0, 2)[None]


def solution(mesh):
    in_specs = (
        P("section", None, None, "obs"),
        P("section", None, "obs"),
        P("section", None, "obs"),
        P("section", None, "obs"),
        P("section", None, "obs"),
        P(),
        P(None, None, "obs"),
        P(None, None, "obs"),
        P("obs"),
    )
    out_specs = (P("section", None, None, "obs"), P("section", None, None, "obs"))
    return jax.shard_map(local, mesh=mesh, in_specs=in_specs, out_specs=out_specs, check_vma=False)
```

```python
import functools

import jax
import jax.numpy as jnp
import numpy as np
from jax import lax
from jax.experimental import pallas as pl
from jax.experimental.pallas import tpu as pltpu
from jax.sharding import PartitionSpec as P

HUBER_SQ = 9.0
PRIOR_WEIGHT = 64.0
F32 = jnp.float32
BF16 = jnp.bfloat16
NN = (((1,), (0,)), ((), ()))
NT = (((1,), (1,)), ((), ()))
TN = (((0,), (0,)), ((), ()))


def round_up(n, m):
    return -(-n // m) * m


def split3(x):
    hi = x.astype(BF16)
    rest = x - hi.astype(F32)
    mid = rest.astype(BF16)
    low = (rest - mid.astype(F32)).astype(BF16)
    return hi, mid, low


def split2(x):
    hi = x.astype(BF16)
    return hi, (x - hi.astype(F32)).astype(BF16)


def dot(a, b, dims):
    return lax.dot_general(a, b, dims, preferred_element_type=F32)


def each(low, high, body):
    n = high - low

    def step(i, _):
        body(i)
        return 0

    lax.fori_loop(low, high, step, 0, unroll=n if n <= 8 else 1)


def iota(shape, axis):
    return lax.broadcasted_iota(jnp.int32, shape, axis)


def kernel(
    cfg,
    order_hbm,
    x_hbm,
    dep_hbm,
    prec_hbm,
    qc_hbm,
    bc_hbm,
    pc_hbm,
    pi_hbm,
    mf_hbm,
    ee_hbm,
    co_out,
    io_out,
    order_s,
    x_v,
    dep_v,
    prec_v,
    qc_v,
    bc_v,
    pc_v,
    pi_v,
    mf_v,
    ee_v,
    lists,
    bcr,
    pcs,
    pcr,
    cs,
    cr,
    ts,
    tr,
    xs,
    xh,
    pt,
    chcol,
    slots_v,
    slots_s,
    came,
    coef_v,
    hots,
    state,
    betas,
    beta_in,
    betas_out,
    state_in,
    base,
    held,
    match,
    first,
    follow,
    work,
    cob,
    iob,
    load_sem,
    slot_sem,
    bc_send,
    bc_recv,
    p_send,
    p_recv,
    c_send,
    c_recv,
    t_send,
    t_recv,
    f_send,
    f_recv,
    b_send,
    b_recv,
    s_send,
    h_send,
    h_recv,
    o_send,
    o_recv,
):
    S, O, K, N, NP, T, C, NB, SL, TL = cfg
    G = S // 2
    Q = O * SL
    sec = lax.axis_index("section")
    ob = lax.axis_index("obs")
    core = lax.rem(sec, 2)
    odd = core == 1
    g = sec // 2
    hub = 2 * g + 1

    def remote(src, dst, send_sem, recv_sem, s, o):
        pltpu.make_async_remote_copy(
            src_ref=src,
            dst_ref=dst,
            send_sem=send_sem,
            recv_sem=recv_sem,
            device_id={"section": s, "obs": o},
            device_id_type=pl.DeviceIdType.MESH,
        ).start()

    def got(ref, sem):
        pltpu.make_async_copy(ref, ref, sem).wait()

    def partner(j):
        if O & (O - 1):
            return lax.rem(ob + j, O)
        o = ob
        for bit in range(O.bit_length() - 1):
            if j >> bit & 1:
                step = 1 << bit
                o = o + step - 2 * step * lax.rem(ob // step, 2)
        return o

    def fan(src, dst, send_sem, recv_sem, s):
        for j in range(1, O):
            o = partner(O - j)
            remote(src(o), dst, send_sem, recv_sem, s, o)

        @pl.when(s != sec)
        def _():
            remote(src(ob), dst, send_sem, recv_sem, s, ob)

        @pl.when(s == sec)
        def _():
            pltpu.make_async_copy(src(ob), dst, recv_sem).start()

    def fanned(like, send_sem, s):
        @pl.when(s != sec)
        def _():
            got(like, send_sem)

        @pl.when(s == sec)
        def _():
            got(like.at[:, 0 : like.shape[1] // O * (O - 1)], send_sem)

    loads = [
        (order_hbm, order_s),
        (bc_hbm, bc_v),
        (pc_hbm, pc_v),
        (x_hbm, x_v),
        (ee_hbm, ee_v),
        (dep_hbm, dep_v),
        (prec_hbm, prec_v),
        (qc_hbm, qc_v),
        (mf_hbm, mf_v),
        (pi_hbm, pi_v),
    ]
    loads = [pltpu.make_async_copy(a, b, load_sem.at[i]) for i, (a, b) in enumerate(loads)]
    for copy in loads:
        copy.start()
    order_in, bc_in, pc_in, x_in, ee_in, dep_in, prec_in, qc_in, mf_in, pi_in = loads

    barrier = pltpu.get_barrier_semaphore()

    def greet(s):
        def one(o):
            @pl.when(jnp.logical_not((s == sec) & (o == ob)))
            def _():
                pl.semaphore_signal(
                    barrier,
                    inc=1,
                    device_id={"section": s, "obs": o},
                    device_id_type=pl.DeviceIdType.MESH,
                )

        each(0, O, one)

    lax.fori_loop(0, S, lambda s, c: (greet(s), c)[1], 0)

    bc_in.wait()
    line = [bc_v[m : m + 1, :] for m in range(K)]
    if K * NB < 128:
        line.append(jnp.full((1, 128 - K * NB), -1, jnp.int32))
    lists[...] = jnp.concatenate(line, axis=1)
    pc_in.wait()
    for m in range(K):
        pcs[m] = jnp.zeros((NP, C), F32)
        pcs[m, 0:N, :] = pc_v[:, m, :]
        betas[m] = pcs[m]
    def unpack():
        x_in.wait()
        ee_in.wait()
        for b in range(NB):
            for i in range(N):
                xs[b, i * K : (i + 1) * K, :] = x_v[i, :, b * 128 : (b + 1) * 128].astype(F32)
            xs[b, N * K : (N + 1) * K, :] = jnp.ones((K, 128), F32)
            xs[b, (N + 1) * K :, :] = jnp.zeros(((NP - N - 1) * K, 128), F32)

    def products(low, high):
        def one(b):
            lanes = pl.ds(pl.multiple_of(b * 128, 128), 128)
            for m in range(low, high):
                xb = xs[b, pl.ds(m, NP, stride=K), :].astype(BF16)
                xh[m, b] = xb
                both = dot(xb, ee_v[...], TN)
                product = (both[:, 0:TL] * both[:, TL:]).astype(BF16)
                for h in range(TL // 128):
                    pt[m, h, lanes, :] = product[:, 128 * h : 128 * h + 128]

        lax.fori_loop(0, NB, lambda b, c: (one(b), c)[1], 0, unroll=8)

    unpack()

    @pl.when(odd)
    def _():
        products(0, 1)

    @pl.when(jnp.logical_not(odd))
    def _():
        products(0, K // 2)

    pl.semaphore_wait(barrier, S * O - 1)

    def send_lists(s):
        fan(lambda o: lists, bcr.at[sec * O + ob], bc_send, bc_recv.at[sec], s)

    def send_prior(m):
        def one(i):
            o = lax.rem(m + g, G) + G * i
            remote(pcs.at[m], pcr.at[m, ob], p_send, p_recv.at[m], 0, o)

        each(0, O // G, one)

    @pl.when(odd)
    def _():
        lax.fori_loop(0, K, lambda m, c: (send_prior(m), c)[1], 0)

    lax.fori_loop(0, S, lambda s, c: (send_lists(s), c)[1], 0)

    cs[...] = jnp.zeros_like(cs)
    coef_v[...] = jnp.zeros_like(coef_v)
    came[...] = jnp.zeros_like(came)

    eye = iota((128, 128), 0) == iota((128, 128), 1)
    upto = iota((128, 128), 0) <= iota((128, 128), 1)
    for m in range(K):
        row = bc_v[m : m + 1, :].astype(F32)
        if NB < 128:
            row = jnp.concatenate([row, jnp.full((1, 128 - NB), -1.0, F32)], axis=1)
        row = jnp.broadcast_to(row, (128, 128))
        col = jnp.sum(jnp.where(eye, row, 0.0), axis=1, keepdims=True)
        range_row = jnp.floor((row + 0.5) * (1.0 / C))
        range_col = jnp.floor((col + 0.5) * (1.0 / C))
        same = range_row == range_col
        rank_row = jnp.sum(jnp.where(same & upto, 1.0, 0.0), axis=0, keepdims=True)
        chcol[m] = jnp.broadcast_to(col[0:NB], (NB, 128))
        slots_v[m : m + 1, :] = jnp.clip((range_row[0:1] * float(SL) + rank_row - 1.0).astype(jnp.int32), 0, Q - 1)
    to_scalars = pltpu.make_async_copy(slots_v, slots_s, slot_sem)
    to_scalars.start()

    @pl.when(odd)
    def _():
        products(1, K)

    @pl.when(jnp.logical_not(odd))
    def _():
        products(K // 2, K)

    dep_in.wait()
    prec_in.wait()
    qc_in.wait()
    to_scalars.wait()

    def split_f32(x):
        return [p.astype(F32) for p in split2(x)]

    def row_entry(m):
        @pl.when(sec == 0)
        def _():
            got(pcr.at[m], p_recv.at[m])
            channel = chcol[m]
            coef = jnp.zeros((NB, N), F32)
            lane = iota((NB, C), 1).astype(F32)
            for o in range(O):
                wide = jnp.broadcast_to(channel[:, 0:1], (NB, C)) - float(o * C)
                hot = jnp.where(lane == wide, 1.0, 0.0).astype(BF16)
                for part in split2(pcr[m, o, 0:N, :]):
                    coef = coef + dot(hot, part, NT)
            coef_v[:, 0:N] = coef

        @pl.when(sec != 0)
        def _():
            got(cr.at[m], c_recv.at[m])
            came[0:Q, :] = cr[m]
            sub = iota((8, 128), 0)
            for q in range(NB // 8):
                tile = jnp.zeros((8, 128), F32)
                for r in range(8):
                    row = jnp.broadcast_to(came[pl.ds(jnp.clip(slots_s[m, 8 * q + r], 0, Q - 1), 1), :], (8, 128))
                    tile = jnp.where(sub == r, row, tile)
                coef_v[8 * q : 8 * q + 8, :] = tile[:, 0:NP]

        pieces = split_f32(coef_v[...])
        sub = iota((8, 128), 0)
        tiles = []
        for q in range(NB // 8):
            stack = jnp.concatenate([p[8 * q : 8 * q + 8] for p in pieces], axis=0).astype(BF16)
            tile = jnp.zeros((8, 128), F32)
            for c in range(4):
                at = (8 * q + 2 * c) * 128
                pair = jnp.concatenate([xh[m, at // 128], xh[m, at // 128 + 1]], axis=1)
                full = dot(stack, pair, NN)
                full = full[0:8] + full[8:16]
                tile = jnp.where(sub == 2 * c, full[:, 0:128], tile)
                tile = jnp.where(sub == 2 * c + 1, full[:, 128:256], tile)
            tiles.append(tile)
        offset = jnp.concatenate(tiles, axis=0)
        rows = pl.ds(m, NB, stride=K)
        residual = dep_v[rows, :] - offset
        precision = prec_v[rows, :]
        passed = qc_v[rows, :].astype(F32)
        weight = passed * precision / (1.0 + precision * residual * residual / HUBER_SQ)
        pull = weight * residual
        total = jnp.sum(jnp.sum(pull * residual, axis=0, keepdims=True), axis=1, keepdims=True)
        count = jnp.sum(jnp.sum(passed, axis=0, keepdims=True), axis=1, keepdims=True)
        slot = iota((Q, 128), 0)
        acc = jnp.zeros((2 * Q, TL), F32)
        for c in range(NB // 2):
            sides = []
            for b in (2 * c, 2 * c + 1):
                hit = slot == slots_s[m, b]
                sides.append(
                    jnp.concatenate(
                        [jnp.where(hit, jnp.broadcast_to(v[b : b + 1], (Q, 128)), 0.0) for v in (weight, pull)], axis=0
                    )
                )
            left = jnp.concatenate(sides, axis=1).astype(BF16)
            right = jnp.concatenate([pt[m, h, 256 * c : 256 * c + 256, :] for h in range(TL // 128)], axis=1)
            acc = acc + dot(left, right, NN)
        out = jnp.where(iota((Q, TL), 1) < T, acc[0:Q], acc[Q:])
        lane = iota((Q, TL), 1)
        out = jnp.where(lane == T + N, total, jnp.where(lane == T + N + 1, count, out))
        ts[m] = out.reshape(O, SL, TL)
        fan(lambda o: ts.at[m, o], tr.at[sec, m, ob], t_send, t_recv.at[sec, m], hub)

    def scale_of(terms):
        row = iota((Q, TL), 0)
        sums = jnp.sum(jnp.where(row % SL == 0, terms, 0.0), axis=0, keepdims=True)
        return (sums[:, T + N + 1 : T + N + 2] + PRIOR_WEIGHT) / (sums[:, T + N : T + N + 1] + PRIOR_WEIGHT)

    def solve():
        H = NP // 8
        sub = iota((8, Q), 0)
        cols = []
        for k in range(N):
            at = k * N - k * (k - 1) // 2 - k
            cols.append([work[at + 8 * h : at + 8 * h + 8, :] for h in range(H)])
        right = [work[T + 8 * h : T + 8 * h + 8, :] for h in range(H)]
        scale = [jnp.ones((8, Q), F32) for _ in range(H)]
        pivot_now = jnp.broadcast_to(cols[0][0][0:1], (8, Q))
        for j in range(N):
            h, r = j // 8, j % 8
            col = cols[j]
            root = lax.rsqrt(pivot_now)
            inverse = root * root
            if j + 1 < N:
                kh, kr = (j + 1) // 8, (j + 1) % 8
                side = jnp.broadcast_to(col[kh][kr : kr + 1], (8, Q))
                pivot_now = jnp.broadcast_to(cols[j + 1][kh][kr : kr + 1], (8, Q)) - side * side * inverse
            factor = [v * inverse for v in col]
            factor[h] = jnp.where(sub == r, 0.0, factor[h])
            scale[h] = jnp.where(sub == r, inverse, scale[h])
            step = jnp.broadcast_to(right[h][r : r + 1], (8, Q))
            right = [right[i] - factor[i] * step for i in range(H)]
            for k in range(j + 1, N):
                kh, kr = k // 8, k % 8
                pivot = jnp.broadcast_to(col[kh][kr : kr + 1], (8, Q))
                for i in range(H):
                    if i >= kh or i < h or (i == h and r > 0):
                        cols[k][i] = cols[k][i] - factor[i] * pivot
                cols[k][h] = jnp.where(sub == r, pivot, cols[k][h])
        return jnp.concatenate([right[i] * scale[i] for i in range(H)], axis=0)

    def base_ready(m):
        for par in range(2):
            after = jnp.minimum(2 * g + par + 1, S - 1)
            base[par, m] = sum(dot(hots[after, m], part, NT) for part in split3(betas[m]))

    def at_slots(w, m):
        return sum(dot(part, hots[w, m], NT) for part in split3(state[m]))

    def full_normal(w, m):
        terms = tr[w, m].reshape(Q, TL)
        return sum(dot(part, hots[w, m], TN) for part in split2(terms))[0:T] * scale_of(terms)

    def finish(m):
        got(state_in.at[m], h_recv.at[m, 0])
        iob[m] = state_in[m] + full_normal(hub, m)

    def change(par, m):
        w = 2 * g + par
        terms = tr[w, m].reshape(Q, TL)
        normal = sum(dot(part, match[par, m], TN) for part in split2(terms)) * scale_of(terms)
        work[0:T, :] = held[par, m] + normal[0:T]
        work[T:TL, :] = normal[T:TL]
        filled = work[0:1, :] > 0.0
        return split2(jnp.where((iota((NP, Q), 0) < N) & filled, solve(), 0.0))

    def hub_entry(par, m):
        w = 2 * g + par
        got(tr.at[w, m], t_recv.at[w, m])

        @pl.when(par == 0)
        def _():
            remote(tr.at[w, m], tr.at[w, m], s_send.at[w], f_recv.at[w, m], sec - 1, ob)

        for q in range(1, G):

            @pl.when(q > g)
            def _():
                remote(tr.at[w, m], tr.at[w, m], f_send.at[par, q], f_recv.at[w, m], 2 * q + 1, ob)

        @pl.when(par == 1)
        def _():
            got(held.at[1, m], h_recv.at[m, 1])

        @pl.when(w + 1 < S)
        def _():
            deltas = change(par, m)
            slots = base[par, m] + sum(dot(follow[par, m], part, NT) for part in deltas)
            later = base[1, m] + sum(dot(follow[2, m], part, NT) for part in deltas)
            fresh = betas[m] + sum(dot(part, first[par, m], NN) for part in deltas)
            cs[par, m, :, :, 0:NP] = slots.reshape(O, SL, NP)
            base[1, m] = later
            betas[m] = fresh
            betas_out[par, m] = fresh
            fan(lambda o: cs.at[par, m, o], cr.at[m, pl.ds(pl.multiple_of(ob * SL, SL), SL)], c_send.at[par], c_recv.at[m], w + 1)

            @pl.when(par == 0)
            def _():
                remote(betas_out.at[0, m], cob.at[m], o_send, o_recv.at[m], sec - 1, ob)

            @pl.when(par == 1)
            def _():
                cob[m] = betas_out[1, m]
                remote(betas_out.at[1, m], beta_in.at[m], b_send, b_recv.at[m], sec + 2, ob)

        @pl.when(w + 1 == S)
        def _():
            got(state_in.at[m], h_recv.at[m, 0])
            iob[m] = state_in[m] + full_normal(hub, m)
            cob[m] = betas[m] + sum(dot(part, first[par, m], NN) for part in change(par, m))

    def streams(body):
        lax.fori_loop(0, K, lambda m, c: (body(m), c)[1], 0)

    def begin():
        pi_in.wait()
        mf_in.wait()
        for m in range(K):
            state[m] = pi_v[:, m, :]
        low = ob * C
        prefix = jnp.where(iota((128, 128), 0) <= iota((128, 128), 1), 1.0, 0.0).astype(BF16)
        rank_of_row = (iota((Q, 128), 0) % SL + 1).astype(F32)
        lane = iota((Q, C), 1).astype(F32)
        for w in range(S):
            got(bcr.at[w * O : (w + 1) * O], bc_recv.at[w])
        owner_lane = iota((Q, 128), 1) // NB

        def window_hots(w):
            channel = jnp.concatenate([jnp.broadcast_to(bcr[w * O + o], (SL, 128)) for o in range(O)], axis=0)
            inside = (channel >= low) & (channel < low + C)
            for m in range(K):
                ours = inside & (owner_lane == m)
                rank = dot(jnp.where(ours, 1.0, 0.0).astype(BF16), prefix, NN)
                hit = ours & (rank == rank_of_row)
                value = jnp.sum(jnp.where(hit, (channel - low + 1).astype(F32), 0.0), axis=1, keepdims=True)
                hots[w, m] = jnp.where(lane == value - 1.0, 1.0, 0.0).astype(BF16)

        each(0, S, window_hots)

    def links():
        earlier_slot = iota((Q, Q), 1) < iota((Q, Q), 0)
        for m in range(K):
            for par in range(2):
                hot = hots[2 * g + par, m]
                same = dot(hot, hot, NT)
                match[par, m] = same.astype(BF16)
                copies = jnp.sum(jnp.where(earlier_slot, same, 0.0), axis=1, keepdims=True)
                first[par, m] = jnp.where(copies == 0.0, hot.astype(F32), 0.0).astype(BF16)
        after = jnp.minimum(2 * g + 2, S - 1)
        for m in range(K):
            follow[0, m] = dot(hots[2 * g + 1, m], first[0, m], NT).astype(BF16)
            follow[1, m] = dot(hots[after, m], first[1, m], NT).astype(BF16)
            follow[2, m] = dot(hots[after, m], first[0, m], NT).astype(BF16)

    def catch_up_one(w, m):
        got(tr.at[w, m], f_recv.at[w, m])

        @pl.when(odd)
        def _():
            remote(tr.at[w, m], tr.at[w, m], s_send.at[w], f_recv.at[w, m], sec - 1, ob)

        state[m] = (state[m] + full_normal(w, m)) * mf_v[...]

    def catch_up(windows):
        lax.fori_loop(0, windows, lambda w, c: (streams(lambda m: catch_up_one(w, m)), c)[1], 0)

    def first_ready():
        @pl.when(g == 0)
        def _():
            for m in range(K):
                base_ready(m)
                held[0, m] = at_slots(2 * g, m)

        def one(i):
            @pl.when(i < K)
            def _():
                m = jnp.minimum(i, K - 1)
                catch_up_one(2 * g - 1, m)
                held[0, m] = at_slots(2 * g, m)

            @pl.when(i >= 2)
            def _():
                m = jnp.maximum(i - 2, 0)
                got(beta_in.at[m], b_recv.at[m])
                betas[m] = beta_in[m]
                base_ready(m)

        @pl.when(g > 0)
        def _():
            lax.fori_loop(0, K + 2, lambda i, c: (one(i), c)[1], 0)

    @pl.when(odd | (g > 0))
    def _():
        begin()

    @pl.when(odd)
    def _():
        links()
        catch_up(2 * g - 1)
        first_ready()
        got(pcr.at[:, 0 : O // G], p_send)
        lax.fori_loop(0, 2 * g, lambda w, c: (got(tr.at[0], s_send.at[w]), c)[1], 0)

    def turn(par):
        @pl.when(par == core)
        def _():
            streams(row_entry)

        @pl.when(odd)
        def _():
            streams(lambda m: hub_entry(par, m))

    got(bcr.at[0 : S * O - 1], bc_send)
    lax.fori_loop(0, 2, lambda par, c: (turn(par), c)[1], 0)

    @pl.when(odd & (g + 1 < G))
    def _():
        streams(finish)

    @pl.when(jnp.logical_not(odd))
    def _():
        @pl.when(g == 0)
        def _():
            begin()

        catch_up(2 * g)

        def update(m):
            got(tr.at[2 * g, m], f_recv.at[2 * g, m])
            post = state[m] + full_normal(2 * g, m)
            iob[m] = post
            state[m] = post * mf_v[...]
            remote(state.at[m], state_in.at[m], h_send.at[0], h_recv.at[m, 0], sec + 1, ob)
            held[1, m] = at_slots(2 * g + 1, m)
            remote(held.at[1, m], held.at[1, m], h_send.at[1], h_recv.at[m, 1], sec + 1, ob)

        streams(update)
        streams(lambda m: got(cob.at[m], o_recv.at[m]))

    order_in.wait()
    for k in range(K):
        m = order_s[k]
        io_out[:, k, :] = iob[m]
        co_out[:, k, :] = cob[m, 0:N, :]

    fanned(ts, t_send, hub)

    @pl.when(odd)
    def _():
        fanned(cr, c_send.at[0], hub)
        got(betas_out.at[0], o_send)
        got(tr.at[0], s_send.at[2 * g])

        @pl.when(g + 1 < G)
        def _():
            fanned(cr, c_send.at[1], hub + 1)
            got(betas_out.at[1], b_send)

        for q in range(1, G):

            @pl.when(q > g)
            def _():
                got(tr.at[0], f_send.at[0, q])
                got(tr.at[0], f_send.at[1, q])

    @pl.when(jnp.logical_not(odd))
    def _():
        got(state, h_send.at[0])
        got(held.at[1], h_send.at[1])


def write_out(coeffs, info, coeffs_out, info_out, sems):
    copies = [
        pltpu.make_async_copy(info, info_out, sems.at[0]),
        pltpu.make_async_copy(coeffs, coeffs_out, sems.at[1]),
    ]
    for copy in copies:
        copy.start()
    for copy in copies:
        copy.wait()


def local(
    predictors,
    departures,
    obs_precision,
    qc_pass,
    block_channel,
    stream_order,
    prior_coeffs,
    prior_info,
    memory_factor,
):
    S, O = lax.axis_size("section"), lax.axis_size("obs")
    K, N, C = prior_coeffs.shape
    T = prior_info.shape[1]
    NB = block_channel.shape[2]
    R = predictors.shape[3]
    width = R // NB
    assert width == 128 and S % 2 == 0 and O % (S // 2) == 0 and K * NB <= 128 and NB % 8 == 0
    NP = round_up(N + 1, 8)
    SL = round_up(max(2 * NB // O, 1), 8)
    TL = round_up(T + NP + 2, 128)
    G, Q = S // 2, O * SL
    pairs = [(i, j) for i in range(N) for j in range(i, N)]
    expand = np.zeros((NP, 2 * TL), np.float32)
    for t, (i, j) in enumerate(pairs):
        expand[i, t] = 1.0
        expand[j, TL + t] = 1.0
    for i in range(N):
        expand[i, T + i] = 1.0
        expand[N, TL + T + i] = 1.0
    cfg = (S, O, K, N, NP, T, C, NB, SL, TL)

    def by_block(array):
        return array[0].reshape(K, NB, width).transpose(1, 0, 2).reshape(NB * K, width)

    vm = pl.BlockSpec(memory_space=pltpu.VMEM)
    hbm = pl.BlockSpec(memory_space=pltpu.HBM)
    dma = pltpu.SemaphoreType.DMA
    coeffs, info = pl.pallas_call(
        functools.partial(kernel, cfg),
        out_shape=(
            jax.ShapeDtypeStruct((N, K, C), F32),
            jax.ShapeDtypeStruct((T, K, C), F32),
        ),
        in_specs=[hbm] * 10,
        out_specs=(vm, vm),
        scratch_shapes=[
            pltpu.SMEM((K,), jnp.int32),
            pltpu.VMEM((N, K, R), BF16),
            pltpu.VMEM((NB * K, 128), F32),
            pltpu.VMEM((NB * K, 128), F32),
            pltpu.VMEM((NB * K, 128), jnp.int32),
            pltpu.VMEM((K, NB), jnp.int32),
            pltpu.VMEM((N, K, C), F32),
            pltpu.VMEM((T, K, C), F32),
            pltpu.VMEM((1, C), F32),
            pltpu.VMEM((NP, 2 * TL), BF16),
            pltpu.VMEM((1, 128), jnp.int32),
            pltpu.VMEM((S * O, 1, 128), jnp.int32),
            pltpu.VMEM((K, NP, C), F32),
            pltpu.VMEM((K, O, NP, C), F32),
            pltpu.VMEM((2, K, O, SL, 128), F32),
            pltpu.VMEM((K, Q, 128), F32),
            pltpu.VMEM((K, O, SL, TL), F32),
            pltpu.VMEM((S, K, O, SL, TL), F32),
            pltpu.VMEM((NB, NP * K, 128), F32),
            pltpu.VMEM((K, NB, NP, 128), BF16),
            pltpu.VMEM((K, TL // 128, R, 128), BF16),
            pltpu.VMEM((K, NB, 128), F32),
            pltpu.VMEM((K, 128), jnp.int32),
            pltpu.SMEM((K, 128), jnp.int32),
            pltpu.VMEM((Q + 8, 128), F32),
            pltpu.VMEM((NB, NP), F32),
            pltpu.VMEM((S, K, Q, C), BF16),
            pltpu.VMEM((K, T, C), F32),
            pltpu.VMEM((K, NP, C), F32),
            pltpu.VMEM((K, NP, C), F32),
            pltpu.VMEM((2, K, NP, C), F32),
            pltpu.VMEM((K, T, C), F32),
            pltpu.VMEM((2, K, Q, NP), F32),
            pltpu.VMEM((2, K, T, Q), F32),
            pltpu.VMEM((2, K, Q, Q), BF16),
            pltpu.VMEM((2, K, Q, C), BF16),
            pltpu.VMEM((3, K, Q, Q), BF16),
            pltpu.VMEM((TL, Q), F32),
            pltpu.VMEM((K, NP, C), F32),
            pltpu.VMEM((K, T, C), F32),
            dma((10,)),
            dma,
            dma,
            dma((S,)),
            dma,
            dma((K,)),
            dma((2,)),
            dma((K,)),
            dma,
            dma((S, K)),
            dma((2, G)),
            dma((S, K)),
            dma,
            dma((K,)),
            dma((S,)),
            dma((2,)),
            dma((K, 2)),
            dma,
            dma((K,)),
        ],
        compiler_params=pltpu.CompilerParams(
            has_side_effects=True, collective_id=0, vmem_limit_bytes=48 * 1024 * 1024
        ),
    )(*(pltpu.with_memory_space_constraint(a, pltpu.HBM) for a in (
        stream_order,
        predictors[0].transpose(1, 0, 2),
        by_block(departures),
        by_block(obs_precision),
        by_block(qc_pass),
        block_channel[0],
        prior_coeffs.transpose(1, 0, 2),
        prior_info.transpose(1, 0, 2),
        memory_factor[None],
        jnp.asarray(expand, BF16),
    )))
    coeffs, info = pl.pallas_call(
        write_out,
        out_shape=(
            jax.ShapeDtypeStruct((N, K, C), F32),
            jax.ShapeDtypeStruct((T, K, C), F32),
        ),
        in_specs=[vm, vm],
        out_specs=(hbm, hbm),
        scratch_shapes=[dma((2,))],
        compiler_params=pltpu.CompilerParams(vmem_limit_bytes=4 * 1024 * 1024),
    )(coeffs, info)
    return coeffs.transpose(1, 0, 2)[None], info.transpose(1, 0, 2)[None]


def solution(mesh):
    in_specs = (
        P("section", None, None, "obs"),
        P("section", None, "obs"),
        P("section", None, "obs"),
        P("section", None, "obs"),
        P("section", None, "obs"),
        P(),
        P(None, None, "obs"),
        P(None, None, "obs"),
        P("obs"),
    )
    out_specs = (P("section", None, None, "obs"), P("section", None, None, "obs"))
    return jax.shard_map(local, mesh=mesh, in_specs=in_specs, out_specs=out_specs, check_vma=False)
```

```python
import functools

import jax
import jax.numpy as jnp
import numpy as np
from jax import lax
from jax.experimental import pallas as pl
from jax.experimental.pallas import tpu as pltpu
from jax.sharding import PartitionSpec as P

HUBER_SQ = 9.0
PRIOR_WEIGHT = 64.0
F32 = jnp.float32
BF16 = jnp.bfloat16
NN = (((1,), (0,)), ((), ()))
NT = (((1,), (1,)), ((), ()))
TN = (((0,), (0,)), ((), ()))


def round_up(n, m):
    return -(-n // m) * m


def split3(x):
    hi = x.astype(BF16)
    rest = x - hi.astype(F32)
    mid = rest.astype(BF16)
    low = (rest - mid.astype(F32)).astype(BF16)
    return hi, mid, low


def split2(x):
    hi = x.astype(BF16)
    return hi, (x - hi.astype(F32)).astype(BF16)


def dot(a, b, dims):
    return lax.dot_general(a, b, dims, preferred_element_type=F32)


def each(low, high, body):
    n = high - low

    def step(i, _):
        body(i)
        return 0

    lax.fori_loop(low, high, step, 0, unroll=n if n <= 8 else 1)


def iota(shape, axis):
    return lax.broadcasted_iota(jnp.int32, shape, axis)


def kernel(
    cfg,
    order_hbm,
    x_hbm,
    dep_hbm,
    prec_hbm,
    qc_hbm,
    bc_hbm,
    pc_hbm,
    pi_hbm,
    mf_hbm,
    ee_hbm,
    co_out,
    io_out,
    order_s,
    x_v,
    dep_v,
    prec_v,
    qc_v,
    bc_v,
    pc_v,
    pi_v,
    mf_v,
    ee_v,
    lists,
    bcr,
    pcs,
    pcr,
    cs,
    cr,
    ts,
    tr,
    xs,
    xh,
    pt,
    chcol,
    slots_v,
    slots_s,
    came,
    coef_v,
    hots,
    state,
    betas,
    beta_in,
    betas_out,
    state_in,
    base,
    held,
    match,
    first,
    follow,
    work,
    cob,
    iob,
    load_sem,
    slot_sem,
    bc_send,
    bc_recv,
    p_send,
    p_recv,
    c_send,
    c_recv,
    t_send,
    t_recv,
    f_send,
    f_recv,
    b_send,
    b_recv,
    s_send,
    h_send,
    h_recv,
    o_send,
    o_recv,
):
    S, O, K, N, NP, T, C, NB, SL, TL = cfg
    G = S // 2
    Q = O * SL
    sec = lax.axis_index("section")
    ob = lax.axis_index("obs")
    core = lax.rem(sec, 2)
    odd = core == 1
    g = sec // 2
    hub = 2 * g + 1

    def remote(src, dst, send_sem, recv_sem, s, o):
        pltpu.make_async_remote_copy(
            src_ref=src,
            dst_ref=dst,
            send_sem=send_sem,
            recv_sem=recv_sem,
            device_id={"section": s, "obs": o},
            device_id_type=pl.DeviceIdType.MESH,
        ).start()

    def got(ref, sem):
        pltpu.make_async_copy(ref, ref, sem).wait()

    def flipped(at, j, n):
        if n & (n - 1):
            return lax.rem(at + j, n)
        o = at
        for bit in range(n.bit_length() - 1):
            if j >> bit & 1:
                step = 1 << bit
                o = o + step - 2 * step * lax.rem(at // step, 2)
        return o

    def partner(j):
        return flipped(ob, j, O)

    def fan(src, dst, send_sem, recv_sem, s):
        for j in range(1, O):
            o = partner(O - j)
            remote(src(o), dst, send_sem, recv_sem, s, o)

        @pl.when(s != sec)
        def _():
            remote(src(ob), dst, send_sem, recv_sem, s, ob)

        @pl.when(s == sec)
        def _():
            pltpu.make_async_copy(src(ob), dst, recv_sem).start()

    def fanned(like, send_sem, s):
        @pl.when(s != sec)
        def _():
            got(like, send_sem)

        @pl.when(s == sec)
        def _():
            got(like.at[:, 0 : like.shape[1] // O * (O - 1)], send_sem)

    loads = [
        (order_hbm, order_s),
        (bc_hbm, bc_v),
        (pc_hbm, pc_v),
        (x_hbm, x_v),
        (ee_hbm, ee_v),
        (dep_hbm, dep_v),
        (prec_hbm, prec_v),
        (qc_hbm, qc_v),
        (mf_hbm, mf_v),
        (pi_hbm, pi_v),
    ]
    loads = [pltpu.make_async_copy(a, b, load_sem.at[i]) for i, (a, b) in enumerate(loads)]
    barrier = pltpu.get_barrier_semaphore()

    def greet(s):
        def one(o):
            @pl.when(jnp.logical_not((s == sec) & (o == ob)))
            def _():
                pl.semaphore_signal(
                    barrier,
                    inc=1,
                    device_id={"section": s, "obs": o},
                    device_id_type=pl.DeviceIdType.MESH,
                )

        each(0, O, one)

    lax.fori_loop(0, S, lambda s, c: (greet(s), c)[1], 0)
    for copy in loads:
        copy.start()
    order_in, bc_in, pc_in, x_in, ee_in, dep_in, prec_in, qc_in, mf_in, pi_in = loads

    bc_in.wait()
    line = [bc_v[m : m + 1, :] for m in range(K)]
    if K * NB < 128:
        line.append(jnp.full((1, 128 - K * NB), -1, jnp.int32))
    lists[...] = jnp.concatenate(line, axis=1)
    pc_in.wait()
    for m in range(K):
        pcs[m] = jnp.zeros((NP, C), F32)
        pcs[m, 0:N, :] = pc_v[:, m, :]
        betas[m] = pcs[m]
    def unpack():
        x_in.wait()
        ee_in.wait()
        for b in range(NB):
            for i in range(N):
                xs[b, i * K : (i + 1) * K, :] = x_v[i, :, b * 128 : (b + 1) * 128].astype(F32)
            xs[b, N * K : (N + 1) * K, :] = jnp.ones((K, 128), F32)
            xs[b, (N + 1) * K :, :] = jnp.zeros(((NP - N - 1) * K, 128), F32)

    def products(low, high):
        def one(b):
            lanes = pl.ds(pl.multiple_of(b * 128, 128), 128)
            for m in range(low, high):
                xb = xs[b, pl.ds(m, NP, stride=K), :].astype(BF16)
                xh[m, b] = xb
                both = dot(xb, ee_v[...], TN)
                product = (both[:, 0:TL] * both[:, TL:]).astype(BF16)
                for h in range(TL // 128):
                    pt[m, h, lanes, :] = product[:, 128 * h : 128 * h + 128]

        lax.fori_loop(0, NB, lambda b, c: (one(b), c)[1], 0, unroll=8)

    unpack()

    @pl.when(odd)
    def _():
        products(0, 1)

    @pl.when(jnp.logical_not(odd))
    def _():
        products(0, K // 2)

    pl.semaphore_wait(barrier, S * O - 1)

    def send_lists(s):
        fan(lambda o: lists, bcr.at[sec * O + ob], bc_send, bc_recv.at[sec], s)

    def send_prior(m):
        for j in reversed(range(O // G)):
            o = lax.rem(m + g, G) + G * flipped(ob // G, j, O // G)
            remote(pcs.at[m], pcr.at[m, ob], p_send, p_recv.at[m], 0, o)

    @pl.when(odd)
    def _():
        lax.fori_loop(0, K, lambda m, c: (send_prior(m), c)[1], 0)

    lax.fori_loop(0, S, lambda s, c: (send_lists(s), c)[1], 0)

    cs[...] = jnp.zeros_like(cs)
    coef_v[...] = jnp.zeros_like(coef_v)
    came[...] = jnp.zeros_like(came)

    eye = iota((128, 128), 0) == iota((128, 128), 1)
    upto = iota((128, 128), 0) <= iota((128, 128), 1)
    for m in range(K):
        row = bc_v[m : m + 1, :].astype(F32)
        if NB < 128:
            row = jnp.concatenate([row, jnp.full((1, 128 - NB), -1.0, F32)], axis=1)
        row = jnp.broadcast_to(row, (128, 128))
        col = jnp.sum(jnp.where(eye, row, 0.0), axis=1, keepdims=True)
        range_row = jnp.floor((row + 0.5) * (1.0 / C))
        range_col = jnp.floor((col + 0.5) * (1.0 / C))
        same = range_row == range_col
        rank_row = jnp.sum(jnp.where(same & upto, 1.0, 0.0), axis=0, keepdims=True)
        chcol[m] = jnp.broadcast_to(col[0:NB], (NB, 128))
        slots_v[m : m + 1, :] = jnp.clip((range_row[0:1] * float(SL) + rank_row - 1.0).astype(jnp.int32), 0, Q - 1)
    to_scalars = pltpu.make_async_copy(slots_v, slots_s, slot_sem)
    to_scalars.start()

    @pl.when(odd)
    def _():
        products(1, K)

    @pl.when(jnp.logical_not(odd))
    def _():
        products(K // 2, K)

    dep_in.wait()
    prec_in.wait()
    qc_in.wait()
    to_scalars.wait()

    def split_f32(x):
        return [p.astype(F32) for p in split2(x)]

    def row_entry(m):
        @pl.when(sec == 0)
        def _():
            got(pcr.at[m], p_recv.at[m])
            channel = chcol[m]
            coef = jnp.zeros((NB, N), F32)
            lane = iota((NB, C), 1).astype(F32)
            for o in range(O):
                wide = jnp.broadcast_to(channel[:, 0:1], (NB, C)) - float(o * C)
                hot = jnp.where(lane == wide, 1.0, 0.0).astype(BF16)
                for part in split2(pcr[m, o, 0:N, :]):
                    coef = coef + dot(hot, part, NT)
            coef_v[:, 0:N] = coef

        @pl.when(sec != 0)
        def _():
            got(cr.at[m], c_recv.at[m])
            came[0:Q, :] = cr[m]
            sub = iota((8, 128), 0)
            for q in range(NB // 8):
                tile = jnp.zeros((8, 128), F32)
                for r in range(8):
                    row = jnp.broadcast_to(came[pl.ds(jnp.clip(slots_s[m, 8 * q + r], 0, Q - 1), 1), :], (8, 128))
                    tile = jnp.where(sub == r, row, tile)
                coef_v[8 * q : 8 * q + 8, :] = tile[:, 0:NP]

        pieces = split_f32(coef_v[...])
        sub = iota((8, 128), 0)
        tiles = []
        for q in range(NB // 8):
            stack = jnp.concatenate([p[8 * q : 8 * q + 8] for p in pieces], axis=0).astype(BF16)
            tile = jnp.zeros((8, 128), F32)
            for c in range(4):
                at = (8 * q + 2 * c) * 128
                pair = jnp.concatenate([xh[m, at // 128], xh[m, at // 128 + 1]], axis=1)
                full = dot(stack, pair, NN)
                full = full[0:8] + full[8:16]
                tile = jnp.where(sub == 2 * c, full[:, 0:128], tile)
                tile = jnp.where(sub == 2 * c + 1, full[:, 128:256], tile)
            tiles.append(tile)
        offset = jnp.concatenate(tiles, axis=0)
        rows = pl.ds(m, NB, stride=K)
        residual = dep_v[rows, :] - offset
        precision = prec_v[rows, :]
        passed = qc_v[rows, :].astype(F32)
        weight = passed * precision / (1.0 + precision * residual * residual / HUBER_SQ)
        pull = weight * residual
        total = jnp.sum(jnp.sum(pull * residual, axis=0, keepdims=True), axis=1, keepdims=True)
        count = jnp.sum(jnp.sum(passed, axis=0, keepdims=True), axis=1, keepdims=True)
        slot = iota((Q, 128), 0)
        acc = jnp.zeros((2 * Q, TL), F32)
        for c in range(NB // 2):
            sides = []
            for b in (2 * c, 2 * c + 1):
                hit = slot == slots_s[m, b]
                sides.append(
                    jnp.concatenate(
                        [jnp.where(hit, jnp.broadcast_to(v[b : b + 1], (Q, 128)), 0.0) for v in (weight, pull)], axis=0
                    )
                )
            left = jnp.concatenate(sides, axis=1).astype(BF16)
            right = jnp.concatenate([pt[m, h, 256 * c : 256 * c + 256, :] for h in range(TL // 128)], axis=1)
            acc = acc + dot(left, right, NN)
        out = jnp.where(iota((Q, TL), 1) < T, acc[0:Q], acc[Q:])
        lane = iota((Q, TL), 1)
        out = jnp.where(lane == T + N, total, jnp.where(lane == T + N + 1, count, out))
        ts[m] = out.reshape(O, SL, TL)
        fan(lambda o: ts.at[m, o], tr.at[sec, m, ob], t_send, t_recv.at[sec, m], hub)

    def scale_of(terms):
        row = iota((Q, TL), 0)
        sums = jnp.sum(jnp.where(row % SL == 0, terms, 0.0), axis=0, keepdims=True)
        return (sums[:, T + N + 1 : T + N + 2] + PRIOR_WEIGHT) / (sums[:, T + N : T + N + 1] + PRIOR_WEIGHT)

    def solve():
        H = NP // 8
        sub = iota((8, Q), 0)
        cols = []
        for k in range(N):
            at = k * N - k * (k - 1) // 2 - k
            cols.append([work[at + 8 * h : at + 8 * h + 8, :] for h in range(H)])
        right = [work[T + 8 * h : T + 8 * h + 8, :] for h in range(H)]
        scale = [jnp.ones((8, Q), F32) for _ in range(H)]
        pivot_now = jnp.broadcast_to(cols[0][0][0:1], (8, Q))
        for j in range(N):
            h, r = j // 8, j % 8
            col = cols[j]
            root = lax.rsqrt(pivot_now)
            inverse = root * root
            if j + 1 < N:
                kh, kr = (j + 1) // 8, (j + 1) % 8
                side = jnp.broadcast_to(col[kh][kr : kr + 1], (8, Q))
                pivot_now = jnp.broadcast_to(cols[j + 1][kh][kr : kr + 1], (8, Q)) - side * side * inverse
            factor = [v * inverse for v in col]
            factor[h] = jnp.where(sub == r, 0.0, factor[h])
            scale[h] = jnp.where(sub == r, inverse, scale[h])
            step = jnp.broadcast_to(right[h][r : r + 1], (8, Q))
            right = [right[i] - factor[i] * step for i in range(H)]
            for k in range(j + 1, N):
                kh, kr = k // 8, k % 8
                pivot = jnp.broadcast_to(col[kh][kr : kr + 1], (8, Q))
                for i in range(H):
                    if i >= kh or i < h or (i == h and r > 0):
                        cols[k][i] = cols[k][i] - factor[i] * pivot
                cols[k][h] = jnp.where(sub == r, pivot, cols[k][h])
        return jnp.concatenate([right[i] * scale[i] for i in range(H)], axis=0)

    def base_ready(m):
        for par in range(2):
            after = jnp.minimum(2 * g + par + 1, S - 1)
            base[par, m] = sum(dot(hots[after, m], part, NT) for part in split3(betas[m]))

    def at_slots(w, m):
        return sum(dot(part, hots[w, m], NT) for part in split3(state[m]))

    def full_normal(w, m):
        terms = tr[w, m].reshape(Q, TL)
        return sum(dot(part, hots[w, m], TN) for part in split2(terms))[0:T] * scale_of(terms)

    def finish(m):
        got(state_in.at[m], h_recv.at[m, 0])
        iob[m] = state_in[m] + full_normal(hub, m)

    def change(par, m):
        w = 2 * g + par
        terms = tr[w, m].reshape(Q, TL)
        normal = sum(dot(part, match[par, m], TN) for part in split2(terms)) * scale_of(terms)
        work[0:T, :] = held[par, m] + normal[0:T]
        work[T:TL, :] = normal[T:TL]
        filled = work[0:1, :] > 0.0
        return split2(jnp.where((iota((NP, Q), 0) < N) & filled, solve(), 0.0))

    def hub_entry(par, m):
        w = 2 * g + par
        got(tr.at[w, m], t_recv.at[w, m])

        @pl.when(par == 0)
        def _():
            remote(tr.at[w, m], tr.at[w, m], s_send.at[w], f_recv.at[w, m], sec - 1, ob)

        for q in range(1, G):

            @pl.when(q > g)
            def _():
                remote(tr.at[w, m], tr.at[w, m], f_send.at[par, q], f_recv.at[w, m], 2 * q + 1, ob)

        @pl.when(par == 1)
        def _():
            got(held.at[1, m], h_recv.at[m, 1])

        @pl.when(w + 1 < S)
        def _():
            deltas = change(par, m)
            slots = base[par, m] + sum(dot(follow[par, m], part, NT) for part in deltas)
            later = base[1, m] + sum(dot(follow[2, m], part, NT) for part in deltas)
            fresh = betas[m] + sum(dot(part, first[par, m], NN) for part in deltas)
            cs[par, m, :, :, 0:NP] = slots.reshape(O, SL, NP)
            base[1, m] = later
            betas[m] = fresh
            betas_out[par, m] = fresh
            fan(lambda o: cs.at[par, m, o], cr.at[m, pl.ds(pl.multiple_of(ob * SL, SL), SL)], c_send.at[par], c_recv.at[m], w + 1)

            @pl.when(par == 0)
            def _():
                remote(betas_out.at[0, m], cob.at[m], o_send, o_recv.at[m], sec - 1, ob)

            @pl.when(par == 1)
            def _():
                cob[m] = betas_out[1, m]
                remote(betas_out.at[1, m], beta_in.at[m], b_send, b_recv.at[m], sec + 2, ob)

        @pl.when(w + 1 == S)
        def _():
            got(state_in.at[m], h_recv.at[m, 0])
            iob[m] = state_in[m] + full_normal(hub, m)
            cob[m] = betas[m] + sum(dot(part, first[par, m], NN) for part in change(par, m))

    def streams(body):
        lax.fori_loop(0, K, lambda m, c: (body(m), c)[1], 0)

    def begin():
        pi_in.wait()
        mf_in.wait()
        for m in range(K):
            state[m] = pi_v[:, m, :]
        low = ob * C
        prefix = jnp.where(iota((128, 128), 0) <= iota((128, 128), 1), 1.0, 0.0).astype(BF16)
        rank_of_row = (iota((Q, 128), 0) % SL + 1).astype(F32)
        lane = iota((Q, C), 1).astype(F32)
        for w in range(S):
            got(bcr.at[w * O : (w + 1) * O], bc_recv.at[w])
        owner_lane = iota((Q, 128), 1) // NB

        def window_hots(w):
            channel = jnp.concatenate([jnp.broadcast_to(bcr[w * O + o], (SL, 128)) for o in range(O)], axis=0)
            inside = (channel >= low) & (channel < low + C)
            for m in range(K):
                ours = inside & (owner_lane == m)
                rank = dot(jnp.where(ours, 1.0, 0.0).astype(BF16), prefix, NN)
                hit = ours & (rank == rank_of_row)
                value = jnp.sum(jnp.where(hit, (channel - low + 1).astype(F32), 0.0), axis=1, keepdims=True)
                hots[w, m] = jnp.where(lane == value - 1.0, 1.0, 0.0).astype(BF16)

        each(0, S, window_hots)

    def links():
        earlier_slot = iota((Q, Q), 1) < iota((Q, Q), 0)
        for m in range(K):
            for par in range(2):
                hot = hots[2 * g + par, m]
                same = dot(hot, hot, NT)
                match[par, m] = same.astype(BF16)
                copies = jnp.sum(jnp.where(earlier_slot, same, 0.0), axis=1, keepdims=True)
                first[par, m] = jnp.where(copies == 0.0, hot.astype(F32), 0.0).astype(BF16)
        after = jnp.minimum(2 * g + 2, S - 1)
        for m in range(K):
            follow[0, m] = dot(hots[2 * g + 1, m], first[0, m], NT).astype(BF16)
            follow[1, m] = dot(hots[after, m], first[1, m], NT).astype(BF16)
            follow[2, m] = dot(hots[after, m], first[0, m], NT).astype(BF16)

    def catch_up_one(w, m):
        got(tr.at[w, m], f_recv.at[w, m])

        @pl.when(odd)
        def _():
            remote(tr.at[w, m], tr.at[w, m], s_send.at[w], f_recv.at[w, m], sec - 1, ob)

        state[m] = (state[m] + full_normal(w, m)) * mf_v[...]

    def catch_up(windows):
        lax.fori_loop(0, windows, lambda w, c: (streams(lambda m: catch_up_one(w, m)), c)[1], 0)

    def first_ready():
        @pl.when(g == 0)
        def _():
            for m in range(K):
                base_ready(m)
                held[0, m] = at_slots(2 * g, m)

        def one(i):
            @pl.when(i < K)
            def _():
                m = jnp.minimum(i, K - 1)
                catch_up_one(2 * g - 1, m)
                held[0, m] = at_slots(2 * g, m)

            @pl.when(i >= 2)
            def _():
                m = jnp.maximum(i - 2, 0)
                got(beta_in.at[m], b_recv.at[m])
                betas[m] = beta_in[m]
                base_ready(m)

        @pl.when(g > 0)
        def _():
            lax.fori_loop(0, K + 2, lambda i, c: (one(i), c)[1], 0)

    @pl.when(odd | (g > 0))
    def _():
        begin()

    @pl.when(odd)
    def _():
        links()
        catch_up(2 * g - 1)
        first_ready()
        got(pcr.at[:, 0 : O // G], p_send)
        lax.fori_loop(0, 2 * g, lambda w, c: (got(tr.at[0], s_send.at[w]), c)[1], 0)

    def turn(par):
        @pl.when(par == core)
        def _():
            streams(row_entry)

        @pl.when(odd)
        def _():
            streams(lambda m: hub_entry(par, m))

    got(bcr.at[0 : S * O - 1], bc_send)
    lax.fori_loop(0, 2, lambda par, c: (turn(par), c)[1], 0)

    @pl.when(odd & (g + 1 < G))
    def _():
        streams(finish)

    @pl.when(jnp.logical_not(odd))
    def _():
        @pl.when(g == 0)
        def _():
            begin()

        catch_up(2 * g)

        def update(m):
            got(tr.at[2 * g, m], f_recv.at[2 * g, m])
            post = state[m] + full_normal(2 * g, m)
            iob[m] = post
            state[m] = post * mf_v[...]
            remote(state.at[m], state_in.at[m], h_send.at[0], h_recv.at[m, 0], sec + 1, ob)
            held[1, m] = at_slots(2 * g + 1, m)
            remote(held.at[1, m], held.at[1, m], h_send.at[1], h_recv.at[m, 1], sec + 1, ob)

        streams(update)
        streams(lambda m: got(cob.at[m], o_recv.at[m]))

    order_in.wait()
    for k in range(K):
        m = order_s[k]
        io_out[:, k, :] = iob[m]
        co_out[:, k, :] = cob[m, 0:N, :]

    fanned(ts, t_send, hub)

    @pl.when(odd)
    def _():
        fanned(cr, c_send.at[0], hub)
        got(betas_out.at[0], o_send)
        got(tr.at[0], s_send.at[2 * g])

        @pl.when(g + 1 < G)
        def _():
            fanned(cr, c_send.at[1], hub + 1)
            got(betas_out.at[1], b_send)

        for q in range(1, G):

            @pl.when(q > g)
            def _():
                got(tr.at[0], f_send.at[0, q])
                got(tr.at[0], f_send.at[1, q])

    @pl.when(jnp.logical_not(odd))
    def _():
        got(state, h_send.at[0])
        got(held.at[1], h_send.at[1])


def write_out(coeffs, info, coeffs_out, info_out, sems):
    copies = [
        pltpu.make_async_copy(info, info_out, sems.at[0]),
        pltpu.make_async_copy(coeffs, coeffs_out, sems.at[1]),
    ]
    for copy in copies:
        copy.start()
    for copy in copies:
        copy.wait()


def local(
    predictors,
    departures,
    obs_precision,
    qc_pass,
    block_channel,
    stream_order,
    prior_coeffs,
    prior_info,
    memory_factor,
):
    S, O = lax.axis_size("section"), lax.axis_size("obs")
    K, N, C = prior_coeffs.shape
    T = prior_info.shape[1]
    NB = block_channel.shape[2]
    R = predictors.shape[3]
    width = R // NB
    assert width == 128 and S % 2 == 0 and O % (S // 2) == 0 and K * NB <= 128 and NB % 8 == 0
    NP = round_up(N + 1, 8)
    SL = round_up(max(2 * NB // O, 1), 8)
    TL = round_up(T + NP + 2, 128)
    G, Q = S // 2, O * SL
    pairs = [(i, j) for i in range(N) for j in range(i, N)]
    expand = np.zeros((NP, 2 * TL), np.float32)
    for t, (i, j) in enumerate(pairs):
        expand[i, t] = 1.0
        expand[j, TL + t] = 1.0
    for i in range(N):
        expand[i, T + i] = 1.0
        expand[N, TL + T + i] = 1.0
    cfg = (S, O, K, N, NP, T, C, NB, SL, TL)

    def by_block(array):
        return array[0].reshape(K, NB, width).transpose(1, 0, 2).reshape(NB * K, width)

    vm = pl.BlockSpec(memory_space=pltpu.VMEM)
    hbm = pl.BlockSpec(memory_space=pltpu.HBM)
    dma = pltpu.SemaphoreType.DMA
    coeffs, info = pl.pallas_call(
        functools.partial(kernel, cfg),
        out_shape=(
            jax.ShapeDtypeStruct((N, K, C), F32),
            jax.ShapeDtypeStruct((T, K, C), F32),
        ),
        in_specs=[hbm] * 10,
        out_specs=(vm, vm),
        scratch_shapes=[
            pltpu.SMEM((K,), jnp.int32),
            pltpu.VMEM((N, K, R), BF16),
            pltpu.VMEM((NB * K, 128), F32),
            pltpu.VMEM((NB * K, 128), F32),
            pltpu.VMEM((NB * K, 128), jnp.int32),
            pltpu.VMEM((K, NB), jnp.int32),
            pltpu.VMEM((N, K, C), F32),
            pltpu.VMEM((T, K, C), F32),
            pltpu.VMEM((1, C), F32),
            pltpu.VMEM((NP, 2 * TL), BF16),
            pltpu.VMEM((1, 128), jnp.int32),
            pltpu.VMEM((S * O, 1, 128), jnp.int32),
            pltpu.VMEM((K, NP, C), F32),
            pltpu.VMEM((K, O, NP, C), F32),
            pltpu.VMEM((2, K, O, SL, 128), F32),
            pltpu.VMEM((K, Q, 128), F32),
            pltpu.VMEM((K, O, SL, TL), F32),
            pltpu.VMEM((S, K, O, SL, TL), F32),
            pltpu.VMEM((NB, NP * K, 128), F32),
            pltpu.VMEM((K, NB, NP, 128), BF16),
            pltpu.VMEM((K, TL // 128, R, 128), BF16),
            pltpu.VMEM((K, NB, 128), F32),
            pltpu.VMEM((K, 128), jnp.int32),
            pltpu.SMEM((K, 128), jnp.int32),
            pltpu.VMEM((Q + 8, 128), F32),
            pltpu.VMEM((NB, NP), F32),
            pltpu.VMEM((S, K, Q, C), BF16),
            pltpu.VMEM((K, T, C), F32),
            pltpu.VMEM((K, NP, C), F32),
            pltpu.VMEM((K, NP, C), F32),
            pltpu.VMEM((2, K, NP, C), F32),
            pltpu.VMEM((K, T, C), F32),
            pltpu.VMEM((2, K, Q, NP), F32),
            pltpu.VMEM((2, K, T, Q), F32),
            pltpu.VMEM((2, K, Q, Q), BF16),
            pltpu.VMEM((2, K, Q, C), BF16),
            pltpu.VMEM((3, K, Q, Q), BF16),
            pltpu.VMEM((TL, Q), F32),
            pltpu.VMEM((K, NP, C), F32),
            pltpu.VMEM((K, T, C), F32),
            dma((10,)),
            dma,
            dma,
            dma((S,)),
            dma,
            dma((K,)),
            dma((2,)),
            dma((K,)),
            dma,
            dma((S, K)),
            dma((2, G)),
            dma((S, K)),
            dma,
            dma((K,)),
            dma((S,)),
            dma((2,)),
            dma((K, 2)),
            dma,
            dma((K,)),
        ],
        compiler_params=pltpu.CompilerParams(
            has_side_effects=True, collective_id=0, vmem_limit_bytes=48 * 1024 * 1024
        ),
    )(*(pltpu.with_memory_space_constraint(a, pltpu.HBM) for a in (
        stream_order,
        predictors[0].transpose(1, 0, 2),
        by_block(departures),
        by_block(obs_precision),
        by_block(qc_pass),
        block_channel[0],
        prior_coeffs.transpose(1, 0, 2),
        prior_info.transpose(1, 0, 2),
        memory_factor[None],
        jnp.asarray(expand, BF16),
    )))
    coeffs, info = pl.pallas_call(
        write_out,
        out_shape=(
            jax.ShapeDtypeStruct((N, K, C), F32),
            jax.ShapeDtypeStruct((T, K, C), F32),
        ),
        in_specs=[vm, vm],
        out_specs=(hbm, hbm),
        scratch_shapes=[dma((2,))],
        compiler_params=pltpu.CompilerParams(vmem_limit_bytes=4 * 1024 * 1024),
    )(coeffs, info)
    return coeffs.transpose(1, 0, 2)[None], info.transpose(1, 0, 2)[None]


def solution(mesh):
    in_specs = (
        P("section", None, None, "obs"),
        P("section", None, "obs"),
        P("section", None, "obs"),
        P("section", None, "obs"),
        P("section", None, "obs"),
        P(),
        P(None, None, "obs"),
        P(None, None, "obs"),
        P("obs"),
    )
    out_specs = (P("section", None, None, "obs"), P("section", None, None, "obs"))
    return jax.shard_map(local, mesh=mesh, in_specs=in_specs, out_specs=out_specs, check_vma=False)
```

```python
import functools

import jax
import jax.numpy as jnp
import numpy as np
from jax import lax
from jax.experimental import pallas as pl
from jax.experimental.pallas import tpu as pltpu
from jax.sharding import PartitionSpec as P

HUBER_SQ = 9.0
PRIOR_WEIGHT = 64.0
F32 = jnp.float32
BF16 = jnp.bfloat16
NN = (((1,), (0,)), ((), ()))
NT = (((1,), (1,)), ((), ()))
TN = (((0,), (0,)), ((), ()))


def round_up(n, m):
    return -(-n // m) * m


def split3(x):
    hi = x.astype(BF16)
    rest = x - hi.astype(F32)
    mid = rest.astype(BF16)
    low = (rest - mid.astype(F32)).astype(BF16)
    return hi, mid, low


def split2(x):
    hi = x.astype(BF16)
    return hi, (x - hi.astype(F32)).astype(BF16)


def dot(a, b, dims):
    return lax.dot_general(a, b, dims, preferred_element_type=F32)


def each(low, high, body):
    n = high - low

    def step(i, _):
        body(i)
        return 0

    lax.fori_loop(low, high, step, 0, unroll=n if n <= 8 else 1)


def iota(shape, axis):
    return lax.broadcasted_iota(jnp.int32, shape, axis)


def kernel(
    cfg,
    order_hbm,
    x_hbm,
    dep_hbm,
    prec_hbm,
    qc_hbm,
    bc_hbm,
    pc_hbm,
    pi_hbm,
    mf_hbm,
    ee_hbm,
    co_out,
    io_out,
    order_s,
    x_v,
    dep_v,
    prec_v,
    qc_v,
    bc_v,
    pc_v,
    pi_v,
    mf_v,
    ee_v,
    lists,
    bcr,
    pcs,
    pcr,
    cs,
    cr,
    ts,
    tr,
    xs,
    xh,
    pt,
    chcol,
    slots_v,
    slots_s,
    came,
    coef_v,
    hots,
    state,
    betas,
    beta_in,
    betas_out,
    state_in,
    base,
    held,
    match,
    first,
    follow,
    work,
    cob,
    iob,
    load_sem,
    slot_sem,
    bc_send,
    bc_recv,
    p_send,
    p_recv,
    c_send,
    c_recv,
    t_send,
    t_recv,
    f_send,
    f_recv,
    b_send,
    b_recv,
    s_send,
    h_send,
    h_recv,
    o_send,
    o_recv,
):
    S, O, K, N, NP, T, C, NB, SL, TL = cfg
    G = S // 2
    Q = O * SL
    sec = lax.axis_index("section")
    ob = lax.axis_index("obs")
    core = lax.rem(sec, 2)
    odd = core == 1
    g = sec // 2
    hub = 2 * g + 1

    def remote(src, dst, send_sem, recv_sem, s, o):
        pltpu.make_async_remote_copy(
            src_ref=src,
            dst_ref=dst,
            send_sem=send_sem,
            recv_sem=recv_sem,
            device_id={"section": s, "obs": o},
            device_id_type=pl.DeviceIdType.MESH,
        ).start()

    def got(ref, sem):
        pltpu.make_async_copy(ref, ref, sem).wait()

    def flipped(at, j, n):
        if n & (n - 1):
            return lax.rem(at + j, n)
        o = at
        for bit in range(n.bit_length() - 1):
            if j >> bit & 1:
                step = 1 << bit
                o = o + step - 2 * step * lax.rem(at // step, 2)
        return o

    def partner(j):
        return flipped(ob, j, O)

    def fan(src, dst, send_sem, recv_sem, s):
        for j in range(1, O):
            o = partner(O - j)
            remote(src(o), dst, send_sem, recv_sem, s, o)

        @pl.when(s != sec)
        def _():
            remote(src(ob), dst, send_sem, recv_sem, s, ob)

        @pl.when(s == sec)
        def _():
            pltpu.make_async_copy(src(ob), dst, recv_sem).start()

    def fanned(like, send_sem, s):
        @pl.when(s != sec)
        def _():
            got(like, send_sem)

        @pl.when(s == sec)
        def _():
            got(like.at[:, 0 : like.shape[1] // O * (O - 1)], send_sem)

    loads = [
        (order_hbm, order_s),
        (bc_hbm, bc_v),
        (pc_hbm, pc_v),
        (x_hbm, x_v),
        (ee_hbm, ee_v),
        (dep_hbm, dep_v),
        (prec_hbm, prec_v),
        (qc_hbm, qc_v),
        (mf_hbm, mf_v),
        (pi_hbm, pi_v),
    ]
    loads = [pltpu.make_async_copy(a, b, load_sem.at[i]) for i, (a, b) in enumerate(loads)]
    barrier = pltpu.get_barrier_semaphore()

    def greet(s):
        def one(o):
            @pl.when(jnp.logical_not((s == sec) & (o == ob)))
            def _():
                pl.semaphore_signal(
                    barrier,
                    inc=1,
                    device_id={"section": s, "obs": o},
                    device_id_type=pl.DeviceIdType.MESH,
                )

        each(0, O, one)

    lax.fori_loop(0, S, lambda s, c: (greet(s), c)[1], 0)
    for copy in loads:
        copy.start()
    order_in, bc_in, pc_in, x_in, ee_in, dep_in, prec_in, qc_in, mf_in, pi_in = loads

    bc_in.wait()
    line = [bc_v[m : m + 1, :] for m in range(K)]
    if K * NB < 128:
        line.append(jnp.full((1, 128 - K * NB), -1, jnp.int32))
    lists[...] = jnp.concatenate(line, axis=1)
    pc_in.wait()
    for m in range(K):
        pcs[m] = jnp.zeros((NP, C), F32)
        pcs[m, 0:N, :] = pc_v[:, m, :]
        betas[m] = pcs[m]
    def unpack():
        x_in.wait()
        ee_in.wait()
        for b in range(NB):
            for i in range(N):
                xs[b, i * K : (i + 1) * K, :] = x_v[i, :, b * 128 : (b + 1) * 128].astype(F32)
            xs[b, N * K : (N + 1) * K, :] = jnp.ones((K, 128), F32)
            xs[b, (N + 1) * K :, :] = jnp.zeros(((NP - N - 1) * K, 128), F32)

    def products(low, high):
        def one(b):
            lanes = pl.ds(pl.multiple_of(b * 128, 128), 128)
            for m in range(low, high):
                xb = xs[b, pl.ds(m, NP, stride=K), :].astype(BF16)
                xh[m, b] = xb
                both = dot(xb, ee_v[...], TN)
                product = (both[:, 0:TL] * both[:, TL:]).astype(BF16)
                for h in range(TL // 128):
                    pt[m, h, lanes, :] = product[:, 128 * h : 128 * h + 128]

        lax.fori_loop(0, NB, lambda b, c: (one(b), c)[1], 0, unroll=8)

    unpack()

    @pl.when(odd)
    def _():
        products(0, 1)

    @pl.when(jnp.logical_not(odd))
    def _():
        products(0, K // 2)

    pl.semaphore_wait(barrier, S * O - 1)

    def send_lists(s):
        fan(lambda o: lists, bcr.at[sec * O + ob], bc_send, bc_recv.at[sec], s)

    def send_prior(m):
        for j in reversed(range(O // G)):
            o = lax.rem(m + g, G) + G * flipped(ob // G, j, O // G)
            remote(pcs.at[m], pcr.at[m, ob], p_send, p_recv.at[m], 0, o)

    @pl.when(odd)
    def _():
        lax.fori_loop(0, K, lambda m, c: (send_prior(m), c)[1], 0)

    lax.fori_loop(0, S, lambda s, c: (send_lists(s), c)[1], 0)

    cs[...] = jnp.zeros_like(cs)
    coef_v[...] = jnp.zeros_like(coef_v)
    came[...] = jnp.zeros_like(came)

    eye = iota((128, 128), 0) == iota((128, 128), 1)
    upto = iota((128, 128), 0) <= iota((128, 128), 1)
    for m in range(K):
        row = bc_v[m : m + 1, :].astype(F32)
        if NB < 128:
            row = jnp.concatenate([row, jnp.full((1, 128 - NB), -1.0, F32)], axis=1)
        row = jnp.broadcast_to(row, (128, 128))
        col = jnp.sum(jnp.where(eye, row, 0.0), axis=1, keepdims=True)
        range_row = jnp.floor((row + 0.5) * (1.0 / C))
        range_col = jnp.floor((col + 0.5) * (1.0 / C))
        same = range_row == range_col
        rank_row = jnp.sum(jnp.where(same & upto, 1.0, 0.0), axis=0, keepdims=True)
        chcol[m] = jnp.broadcast_to(col[0:NB], (NB, 128))
        slots_v[m : m + 1, :] = jnp.clip((range_row[0:1] * float(SL) + rank_row - 1.0).astype(jnp.int32), 0, Q - 1)
    to_scalars = pltpu.make_async_copy(slots_v, slots_s, slot_sem)
    to_scalars.start()

    @pl.when(odd)
    def _():
        products(1, K)

    @pl.when(jnp.logical_not(odd))
    def _():
        products(K // 2, K)

    dep_in.wait()
    prec_in.wait()
    qc_in.wait()
    to_scalars.wait()

    def split_f32(x):
        return [p.astype(F32) for p in split2(x)]

    def row_entry(m):
        @pl.when(sec == 0)
        def _():
            wide = jnp.concatenate([chcol[m]] * -(-C // 128), axis=1)[:, 0:C]
            lane = iota((NB, C), 1).astype(F32)
            picks = [jnp.where(lane == wide - float(o * C), 1.0, 0.0).astype(BF16) for o in range(O)]
            got(pcr.at[m], p_recv.at[m])
            coef = jnp.zeros((NB, N), F32)
            for o in range(O):
                for part in split2(pcr[m, o, 0:N, :]):
                    coef = coef + dot(picks[o], part, NT)
            coef_v[:, 0:N] = coef

        @pl.when(sec != 0)
        def _():
            got(cr.at[m], c_recv.at[m])
            came[0:Q, :] = cr[m]
            sub = iota((8, 128), 0)
            for q in range(NB // 8):
                tile = jnp.zeros((8, 128), F32)
                for r in range(8):
                    row = jnp.broadcast_to(came[pl.ds(jnp.clip(slots_s[m, 8 * q + r], 0, Q - 1), 1), :], (8, 128))
                    tile = jnp.where(sub == r, row, tile)
                coef_v[8 * q : 8 * q + 8, :] = tile[:, 0:NP]

        pieces = split_f32(coef_v[...])
        sub = iota((8, 128), 0)
        tiles = []
        for q in range(NB // 8):
            stack = jnp.concatenate([p[8 * q : 8 * q + 8] for p in pieces], axis=0).astype(BF16)
            tile = jnp.zeros((8, 128), F32)
            for c in range(4):
                at = (8 * q + 2 * c) * 128
                pair = jnp.concatenate([xh[m, at // 128], xh[m, at // 128 + 1]], axis=1)
                full = dot(stack, pair, NN)
                full = full[0:8] + full[8:16]
                tile = jnp.where(sub == 2 * c, full[:, 0:128], tile)
                tile = jnp.where(sub == 2 * c + 1, full[:, 128:256], tile)
            tiles.append(tile)
        offset = jnp.concatenate(tiles, axis=0)
        rows = pl.ds(m, NB, stride=K)
        residual = dep_v[rows, :] - offset
        precision = prec_v[rows, :]
        passed = qc_v[rows, :].astype(F32)
        weight = passed * precision / (1.0 + precision * residual * residual / HUBER_SQ)
        pull = weight * residual
        total = jnp.sum(jnp.sum(pull * residual, axis=0, keepdims=True), axis=1, keepdims=True)
        count = jnp.sum(jnp.sum(passed, axis=0, keepdims=True), axis=1, keepdims=True)
        slot = iota((Q, 128), 0)
        acc = jnp.zeros((2 * Q, TL), F32)
        for c in range(NB // 2):
            sides = []
            for b in (2 * c, 2 * c + 1):
                hit = slot == slots_s[m, b]
                sides.append(
                    jnp.concatenate(
                        [jnp.where(hit, jnp.broadcast_to(v[b : b + 1], (Q, 128)), 0.0) for v in (weight, pull)], axis=0
                    )
                )
            left = jnp.concatenate(sides, axis=1).astype(BF16)
            right = jnp.concatenate([pt[m, h, 256 * c : 256 * c + 256, :] for h in range(TL // 128)], axis=1)
            acc = acc + dot(left, right, NN)
        out = jnp.where(iota((Q, TL), 1) < T, acc[0:Q], acc[Q:])
        lane = iota((Q, TL), 1)
        out = jnp.where(lane == T + N, total, jnp.where(lane == T + N + 1, count, out))
        ts[m] = out.reshape(O, SL, TL)
        fan(lambda o: ts.at[m, o], tr.at[sec, m, ob], t_send, t_recv.at[sec, m], hub)

    def scale_of(terms):
        row = iota((Q, TL), 0)
        sums = jnp.sum(jnp.where(row % SL == 0, terms, 0.0), axis=0, keepdims=True)
        return (sums[:, T + N + 1 : T + N + 2] + PRIOR_WEIGHT) / (sums[:, T + N : T + N + 1] + PRIOR_WEIGHT)

    def solve():
        H = NP // 8
        sub = iota((8, Q), 0)
        cols = []
        for k in range(N):
            at = k * N - k * (k - 1) // 2 - k
            cols.append([work[at + 8 * h : at + 8 * h + 8, :] for h in range(H)])
        right = [work[T + 8 * h : T + 8 * h + 8, :] for h in range(H)]
        scale = [jnp.ones((8, Q), F32) for _ in range(H)]
        pivot_now = jnp.broadcast_to(cols[0][0][0:1], (8, Q))
        for j in range(N):
            h, r = j // 8, j % 8
            col = cols[j]
            root = lax.rsqrt(pivot_now)
            inverse = root * root
            if j + 1 < N:
                kh, kr = (j + 1) // 8, (j + 1) % 8
                side = jnp.broadcast_to(col[kh][kr : kr + 1], (8, Q))
                pivot_now = jnp.broadcast_to(cols[j + 1][kh][kr : kr + 1], (8, Q)) - side * side * inverse
            factor = [v * inverse for v in col]
            factor[h] = jnp.where(sub == r, 0.0, factor[h])
            scale[h] = jnp.where(sub == r, inverse, scale[h])
            step = jnp.broadcast_to(right[h][r : r + 1], (8, Q))
            right = [right[i] - factor[i] * step for i in range(H)]
            for k in range(j + 1, N):
                kh, kr = k // 8, k % 8
                pivot = jnp.broadcast_to(col[kh][kr : kr + 1], (8, Q))
                for i in range(H):
                    if i >= kh or i < h or (i == h and r > 0):
                        cols[k][i] = cols[k][i] - factor[i] * pivot
                cols[k][h] = jnp.where(sub == r, pivot, cols[k][h])
        return jnp.concatenate([right[i] * scale[i] for i in range(H)], axis=0)

    def base_ready(m):
        for par in range(2):
            after = jnp.minimum(2 * g + par + 1, S - 1)
            base[par, m] = sum(dot(hots[after, m], part, NT) for part in split3(betas[m]))

    def at_slots(w, m):
        return sum(dot(part, hots[w, m], NT) for part in split3(state[m]))

    def full_normal(w, m):
        terms = tr[w, m].reshape(Q, TL)
        return sum(dot(part, hots[w, m], TN) for part in split2(terms))[0:T] * scale_of(terms)

    def finish(m):
        got(state_in.at[m], h_recv.at[m, 0])
        iob[m] = state_in[m] + full_normal(hub, m)

    def change(par, m):
        w = 2 * g + par
        terms = tr[w, m].reshape(Q, TL)
        normal = sum(dot(part, match[par, m], TN) for part in split2(terms)) * scale_of(terms)
        work[0:T, :] = held[par, m] + normal[0:T]
        work[T:TL, :] = normal[T:TL]
        filled = work[0:1, :] > 0.0
        return split2(jnp.where((iota((NP, Q), 0) < N) & filled, solve(), 0.0))

    def hub_entry(par, m):
        w = 2 * g + par
        got(tr.at[w, m], t_recv.at[w, m])

        @pl.when(par == 0)
        def _():
            remote(tr.at[w, m], tr.at[w, m], s_send.at[w], f_recv.at[w, m], sec - 1, ob)

        for q in range(1, G):

            @pl.when(q > g)
            def _():
                remote(tr.at[w, m], tr.at[w, m], f_send.at[par, q], f_recv.at[w, m], 2 * q + 1, ob)

        @pl.when(par == 1)
        def _():
            got(held.at[1, m], h_recv.at[m, 1])

        @pl.when(w + 1 < S)
        def _():
            deltas = change(par, m)
            slots = base[par, m] + sum(dot(follow[par, m], part, NT) for part in deltas)
            later = base[1, m] + sum(dot(follow[2, m], part, NT) for part in deltas)
            fresh = betas[m] + sum(dot(part, first[par, m], NN) for part in deltas)
            cs[par, m, :, :, 0:NP] = slots.reshape(O, SL, NP)
            base[1, m] = later
            betas[m] = fresh
            betas_out[par, m] = fresh
            fan(lambda o: cs.at[par, m, o], cr.at[m, pl.ds(pl.multiple_of(ob * SL, SL), SL)], c_send.at[par], c_recv.at[m], w + 1)

            @pl.when(par == 0)
            def _():
                remote(betas_out.at[0, m], cob.at[m], o_send, o_recv.at[m], sec - 1, ob)

            @pl.when(par == 1)
            def _():
                cob[m] = betas_out[1, m]
                remote(betas_out.at[1, m], beta_in.at[m], b_send, b_recv.at[m], sec + 2, ob)

        @pl.when(w + 1 == S)
        def _():
            got(state_in.at[m], h_recv.at[m, 0])
            iob[m] = state_in[m] + full_normal(hub, m)
            cob[m] = betas[m] + sum(dot(part, first[par, m], NN) for part in change(par, m))

    def streams(body):
        lax.fori_loop(0, K, lambda m, c: (body(m), c)[1], 0)

    def begin():
        pi_in.wait()
        mf_in.wait()
        for m in range(K):
            state[m] = pi_v[:, m, :]
        low = ob * C
        prefix = jnp.where(iota((128, 128), 0) <= iota((128, 128), 1), 1.0, 0.0).astype(BF16)
        rank_of_row = (iota((Q, 128), 0) % SL + 1).astype(F32)
        lane = iota((Q, C), 1).astype(F32)
        for w in range(S):
            got(bcr.at[w * O : (w + 1) * O], bc_recv.at[w])
        owner_lane = iota((Q, 128), 1) // NB

        def window_hots(w):
            channel = jnp.concatenate([jnp.broadcast_to(bcr[w * O + o], (SL, 128)) for o in range(O)], axis=0)
            inside = (channel >= low) & (channel < low + C)
            for m in range(K):
                ours = inside & (owner_lane == m)
                rank = dot(jnp.where(ours, 1.0, 0.0).astype(BF16), prefix, NN)
                hit = ours & (rank == rank_of_row)
                value = jnp.sum(jnp.where(hit, (channel - low + 1).astype(F32), 0.0), axis=1, keepdims=True)
                hots[w, m] = jnp.where(lane == value - 1.0, 1.0, 0.0).astype(BF16)

        each(0, S, window_hots)

    def links():
        earlier_slot = iota((Q, Q), 1) < iota((Q, Q), 0)
        for m in range(K):
            for par in range(2):
                hot = hots[2 * g + par, m]
                same = dot(hot, hot, NT)
                match[par, m] = same.astype(BF16)
                copies = jnp.sum(jnp.where(earlier_slot, same, 0.0), axis=1, keepdims=True)
                first[par, m] = jnp.where(copies == 0.0, hot.astype(F32), 0.0).astype(BF16)
        after = jnp.minimum(2 * g + 2, S - 1)
        for m in range(K):
            follow[0, m] = dot(hots[2 * g + 1, m], first[0, m], NT).astype(BF16)
            follow[1, m] = dot(hots[after, m], first[1, m], NT).astype(BF16)
            follow[2, m] = dot(hots[after, m], first[0, m], NT).astype(BF16)

    def catch_up_one(w, m):
        got(tr.at[w, m], f_recv.at[w, m])

        @pl.when(odd)
        def _():
            remote(tr.at[w, m], tr.at[w, m], s_send.at[w], f_recv.at[w, m], sec - 1, ob)

        state[m] = (state[m] + full_normal(w, m)) * mf_v[...]

    def catch_up(windows):
        lax.fori_loop(0, windows, lambda w, c: (streams(lambda m: catch_up_one(w, m)), c)[1], 0)

    def first_ready():
        @pl.when(g == 0)
        def _():
            for m in range(K):
                base_ready(m)
                held[0, m] = at_slots(2 * g, m)

        def one(i):
            @pl.when(i < K)
            def _():
                m = jnp.minimum(i, K - 1)
                catch_up_one(2 * g - 1, m)
                held[0, m] = at_slots(2 * g, m)

            @pl.when(i >= 2)
            def _():
                m = jnp.maximum(i - 2, 0)
                got(beta_in.at[m], b_recv.at[m])
                betas[m] = beta_in[m]
                base_ready(m)

        @pl.when(g > 0)
        def _():
            lax.fori_loop(0, K + 2, lambda i, c: (one(i), c)[1], 0)

    @pl.when(odd | (g > 0))
    def _():
        begin()

    @pl.when(odd)
    def _():
        links()
        catch_up(2 * g - 1)
        first_ready()
        got(pcr.at[:, 0 : O // G], p_send)
        lax.fori_loop(0, 2 * g, lambda w, c: (got(tr.at[0], s_send.at[w]), c)[1], 0)

    def turn(par):
        @pl.when(par == core)
        def _():
            streams(row_entry)

        @pl.when(odd)
        def _():
            streams(lambda m: hub_entry(par, m))

    got(bcr.at[0 : S * O - 1], bc_send)
    lax.fori_loop(0, 2, lambda par, c: (turn(par), c)[1], 0)

    @pl.when(odd & (g + 1 < G))
    def _():
        streams(finish)

    @pl.when(jnp.logical_not(odd))
    def _():
        @pl.when(g == 0)
        def _():
            begin()

        catch_up(2 * g)

        def update(m):
            got(tr.at[2 * g, m], f_recv.at[2 * g, m])
            post = state[m] + full_normal(2 * g, m)
            iob[m] = post
            state[m] = post * mf_v[...]
            remote(state.at[m], state_in.at[m], h_send.at[0], h_recv.at[m, 0], sec + 1, ob)
            held[1, m] = at_slots(2 * g + 1, m)
            remote(held.at[1, m], held.at[1, m], h_send.at[1], h_recv.at[m, 1], sec + 1, ob)

        streams(update)
        streams(lambda m: got(cob.at[m], o_recv.at[m]))

    order_in.wait()
    for k in range(K):
        m = order_s[k]
        io_out[:, k, :] = iob[m]
        co_out[:, k, :] = cob[m, 0:N, :]

    fanned(ts, t_send, hub)

    @pl.when(odd)
    def _():
        fanned(cr, c_send.at[0], hub)
        got(betas_out.at[0], o_send)
        got(tr.at[0], s_send.at[2 * g])

        @pl.when(g + 1 < G)
        def _():
            fanned(cr, c_send.at[1], hub + 1)
            got(betas_out.at[1], b_send)

        for q in range(1, G):

            @pl.when(q > g)
            def _():
                got(tr.at[0], f_send.at[0, q])
                got(tr.at[0], f_send.at[1, q])

    @pl.when(jnp.logical_not(odd))
    def _():
        got(state, h_send.at[0])
        got(held.at[1], h_send.at[1])


def write_out(coeffs, info, coeffs_out, info_out, sems):
    copies = [
        pltpu.make_async_copy(info, info_out, sems.at[0]),
        pltpu.make_async_copy(coeffs, coeffs_out, sems.at[1]),
    ]
    for copy in copies:
        copy.start()
    for copy in copies:
        copy.wait()


def local(
    predictors,
    departures,
    obs_precision,
    qc_pass,
    block_channel,
    stream_order,
    prior_coeffs,
    prior_info,
    memory_factor,
):
    S, O = lax.axis_size("section"), lax.axis_size("obs")
    K, N, C = prior_coeffs.shape
    T = prior_info.shape[1]
    NB = block_channel.shape[2]
    R = predictors.shape[3]
    width = R // NB
    assert width == 128 and S % 2 == 0 and O % (S // 2) == 0 and K * NB <= 128 and NB % 8 == 0
    NP = round_up(N + 1, 8)
    SL = round_up(max(2 * NB // O, 1), 8)
    TL = round_up(T + NP + 2, 128)
    G, Q = S // 2, O * SL
    pairs = [(i, j) for i in range(N) for j in range(i, N)]
    expand = np.zeros((NP, 2 * TL), np.float32)
    for t, (i, j) in enumerate(pairs):
        expand[i, t] = 1.0
        expand[j, TL + t] = 1.0
    for i in range(N):
        expand[i, T + i] = 1.0
        expand[N, TL + T + i] = 1.0
    cfg = (S, O, K, N, NP, T, C, NB, SL, TL)

    def by_block(array):
        return array[0].reshape(K, NB, width).transpose(1, 0, 2).reshape(NB * K, width)

    vm = pl.BlockSpec(memory_space=pltpu.VMEM)
    hbm = pl.BlockSpec(memory_space=pltpu.HBM)
    dma = pltpu.SemaphoreType.DMA
    coeffs, info = pl.pallas_call(
        functools.partial(kernel, cfg),
        out_shape=(
            jax.ShapeDtypeStruct((N, K, C), F32),
            jax.ShapeDtypeStruct((T, K, C), F32),
        ),
        in_specs=[hbm] * 10,
        out_specs=(vm, vm),
        scratch_shapes=[
            pltpu.SMEM((K,), jnp.int32),
            pltpu.VMEM((N, K, R), BF16),
            pltpu.VMEM((NB * K, 128), F32),
            pltpu.VMEM((NB * K, 128), F32),
            pltpu.VMEM((NB * K, 128), jnp.int32),
            pltpu.VMEM((K, NB), jnp.int32),
            pltpu.VMEM((N, K, C), F32),
            pltpu.VMEM((T, K, C), F32),
            pltpu.VMEM((1, C), F32),
            pltpu.VMEM((NP, 2 * TL), BF16),
            pltpu.VMEM((1, 128), jnp.int32),
            pltpu.VMEM((S * O, 1, 128), jnp.int32),
            pltpu.VMEM((K, NP, C), F32),
            pltpu.VMEM((K, O, NP, C), F32),
            pltpu.VMEM((2, K, O, SL, 128), F32),
            pltpu.VMEM((K, Q, 128), F32),
            pltpu.VMEM((K, O, SL, TL), F32),
            pltpu.VMEM((S, K, O, SL, TL), F32),
            pltpu.VMEM((NB, NP * K, 128), F32),
            pltpu.VMEM((K, NB, NP, 128), BF16),
            pltpu.VMEM((K, TL // 128, R, 128), BF16),
            pltpu.VMEM((K, NB, 128), F32),
            pltpu.VMEM((K, 128), jnp.int32),
            pltpu.SMEM((K, 128), jnp.int32),
            pltpu.VMEM((Q + 8, 128), F32),
            pltpu.VMEM((NB, NP), F32),
            pltpu.VMEM((S, K, Q, C), BF16),
            pltpu.VMEM((K, T, C), F32),
            pltpu.VMEM((K, NP, C), F32),
            pltpu.VMEM((K, NP, C), F32),
            pltpu.VMEM((2, K, NP, C), F32),
            pltpu.VMEM((K, T, C), F32),
            pltpu.VMEM((2, K, Q, NP), F32),
            pltpu.VMEM((2, K, T, Q), F32),
            pltpu.VMEM((2, K, Q, Q), BF16),
            pltpu.VMEM((2, K, Q, C), BF16),
            pltpu.VMEM((3, K, Q, Q), BF16),
            pltpu.VMEM((TL, Q), F32),
            pltpu.VMEM((K, NP, C), F32),
            pltpu.VMEM((K, T, C), F32),
            dma((10,)),
            dma,
            dma,
            dma((S,)),
            dma,
            dma((K,)),
            dma((2,)),
            dma((K,)),
            dma,
            dma((S, K)),
            dma((2, G)),
            dma((S, K)),
            dma,
            dma((K,)),
            dma((S,)),
            dma((2,)),
            dma((K, 2)),
            dma,
            dma((K,)),
        ],
        compiler_params=pltpu.CompilerParams(
            has_side_effects=True, collective_id=0, vmem_limit_bytes=48 * 1024 * 1024
        ),
    )(*(pltpu.with_memory_space_constraint(a, pltpu.HBM) for a in (
        stream_order,
        predictors[0].transpose(1, 0, 2),
        by_block(departures),
        by_block(obs_precision),
        by_block(qc_pass),
        block_channel[0],
        prior_coeffs.transpose(1, 0, 2),
        prior_info.transpose(1, 0, 2),
        memory_factor[None],
        jnp.asarray(expand, BF16),
    )))
    coeffs, info = pl.pallas_call(
        write_out,
        out_shape=(
            jax.ShapeDtypeStruct((N, K, C), F32),
            jax.ShapeDtypeStruct((T, K, C), F32),
        ),
        in_specs=[vm, vm],
        out_specs=(hbm, hbm),
        scratch_shapes=[dma((2,))],
        compiler_params=pltpu.CompilerParams(vmem_limit_bytes=4 * 1024 * 1024),
    )(coeffs, info)
    return coeffs.transpose(1, 0, 2)[None], info.transpose(1, 0, 2)[None]


def solution(mesh):
    in_specs = (
        P("section", None, None, "obs"),
        P("section", None, "obs"),
        P("section", None, "obs"),
        P("section", None, "obs"),
        P("section", None, "obs"),
        P(),
        P(None, None, "obs"),
        P(None, None, "obs"),
        P("obs"),
    )
    out_specs = (P("section", None, None, "obs"), P("section", None, None, "obs"))
    return jax.shard_map(local, mesh=mesh, in_specs=in_specs, out_specs=out_specs, check_vma=False)
```
